32 devices in a mesh: dp: 8 (over z, y), ctx: 4 (over x, core).
Axes of the slice: x: 2, y: 2, z: 4, core: 2. Of those that a mesh axis runs over, the one named last changes fastest.
Arguments:
- tokens: bfloat16 [16, 1024, 1024], P('dp', 'ctx'), may hold values from -6 to 6
- first_values: bfloat16 [16, 1024, 1024], P('dp', 'ctx'), may hold values from -6 to 6
- cotangent: bfloat16 [16, 1024, 1024], P('dp', 'ctx'), may hold values from -6 to 6
- segment_ids: int32 [16, 1024], P('dp'), may hold values from 0 to 4, as said below
- attn_gain: bfloat16 [1024], P(('dp', 'ctx')), may hold values from 0.5 to 1.5
- w_query: bfloat16 [1024, 1024], P(('dp', 'ctx')), may hold values from -0.1875 to 0.1875
- w_key: bfloat16 [1024, 1024], P(('dp', 'ctx')), may hold values from -0.1875 to 0.1875
- w_value: bfloat16 [1024, 1024], P(('dp', 'ctx')), may hold values from -0.1875 to 0.1875
- w_out: bfloat16 [1024, 1024], P(('dp', 'ctx')), may hold values from -1 to 1
- ffn_gain: bfloat16 [1024], P(('dp', 'ctx')), may hold values from 0.5 to 1.5
- gate_weight: bfloat16 [1024, 2816], P(('dp', 'ctx')), may hold values from -0.1875 to 0.1875
- up_weight: bfloat16 [1024, 2816], P(('dp', 'ctx')), may hold values from -0.1875 to 0.1875
- down_weight: bfloat16 [2816, 1024], P(('dp', 'ctx')), may hold values from -0.21875 to 0.21875
Outputs:
- output: bfloat16 [16, 1024, 1024], P('dp', 'ctx')
- tokens_grad: float32 [16, 1024, 1024], P('dp', 'ctx')
- first_values_grad: float32 [16, 1024, 1024], P('dp', 'ctx')
- attn_gain_grad: float32 [1024], P(('dp', 'ctx'))
- query_grad: float32 [1024, 1024], P(('dp', 'ctx'))
- key_grad: float32 [1024, 1024], P(('dp', 'ctx'))
- value_grad: float32 [1024, 1024], P(('dp', 'ctx'))
- out_grad: float32 [1024, 1024], P(('dp', 'ctx'))
- ffn_gain_grad: float32 [1024], P(('dp', 'ctx'))
- gate_grad: float32 [1024, 2816], P(('dp', 'ctx'))
- up_grad: float32 [1024, 2816], P(('dp', 'ctx'))
- down_grad: float32 [2816, 1024], P(('dp', 'ctx'))
The draws below stay inside these ranges and needn't reach their ends.
Inputs may be any that keep to these rules, and one draw needn't show every extreme that they name: `segment_ids`: along each sequence the ids start at 0 and rise by one where a document begins; every document but a sequence's last holds 60 to 800 tokens, and each sequence holds at least one document of exactly 800 tokens.
All inputs are finite; a program needn't handle non-finite values.
Results may differ from the reference program's by a relative error of at most 0.017.
Values may be sent and summed in bfloat16 or wider, within the bound.
A program may use at most 192 MiB of HBM per device.

```python
import jax
import jax.numpy as jnp
from jax import lax

D = 1024
HEADS = 16
HEAD_DIM = 64
FF = 2816
LENGTH = 1024
DOC_MIN = 60
DOC_MAX = 800
SEQS = 16


def draw_segment_ids(key, part):
    doc_count = LENGTH // DOC_MIN + 2
    key_lengths, key_head, key_pick = jax.random.split(key, 3)
    doc_lengths = jax.random.randint(key_lengths, (SEQS, doc_count), DOC_MIN, DOC_MAX + 1)
    head_length = jax.random.randint(key_head, (SEQS,), DOC_MIN, LENGTH - DOC_MAX + 1)
    picked = jax.random.randint(key_pick, (SEQS,), 0, 2)
    first_doc = jnp.where(picked == 0, DOC_MAX, head_length)
    second_doc = jnp.where(picked == 0, doc_lengths[:, 1], DOC_MAX)
    doc_lengths = jnp.concatenate([first_doc[:, None], second_doc[:, None], doc_lengths[:, 2:]], axis=1)
    leading = (jnp.arange(SEQS, dtype=jnp.int32) == 0)[:, None]
    column = jnp.arange(doc_count, dtype=jnp.int32)[None, :]
    packed_row = jnp.where(column == 0, DOC_MAX, DOC_MIN)
    doc_lengths = jnp.where(leading, packed_row, doc_lengths)
    bounds = jnp.cumsum(doc_lengths, axis=1)
    places = jnp.arange(LENGTH, dtype=jnp.int32)
    return jnp.sum((bounds[:, None, :] <= places[None, :, None]).astype(jnp.int32), axis=2).astype(jnp.int32)


def level_of(own_key, extent, cuts, smallest, top_value):
    level = 1.0
    for axis_at, parts in cuts:
        steps = jax.random.uniform(jax.random.fold_in(jax.random.fold_in(own_key, 6), axis_at), (parts,), jnp.float32, smallest / len(cuts), top_value / len(cuts))
        level = level * jnp.repeat(jnp.exp(steps), extent[axis_at] // parts).reshape((-1,) + (1,) * (len(extent) - 1 - axis_at))
    return level


def scatter_about(rng, shape, width, most, cuts=(), kind=jnp.bfloat16):
    entries = width * jax.random.normal(rng, shape, jnp.float32)
    if cuts:
        entries = entries * level_of(rng, shape, cuts, -0.22, 0.18)
    return jnp.clip(entries, -most, most).astype(kind)


def setup_inputs(seed: int = 0) -> dict:
    splits = jax.random.split(jax.random.key(seed), 14)
    return {
        "tokens": scatter_about(splits[0], (SEQS, LENGTH, D), 1.0, 6.0, ((0, 8), (1, 4))),
        "first_values": scatter_about(splits[1], (SEQS, LENGTH, D), 1.0, 6.0, ((0, 8), (1, 4))),
        "cotangent": scatter_about(splits[2], (SEQS, LENGTH, D), 1.0, 6.0, ((0, 8), (1, 4))),
        "segment_ids": draw_segment_ids(jax.random.fold_in(splits[13], 71), 0),
        "attn_gain": jnp.clip(1.0 + 0.1 * jax.random.normal(splits[4], (D,), jnp.float32), 0.5, 1.5).astype(jnp.bfloat16),
        "w_query": scatter_about(splits[5], (D, D), D ** -0.5, 0.1875, ((0, 32),)),
        "w_key": scatter_about(splits[6], (D, D), D ** -0.5, 0.1875, ((0, 32),)),
        "w_value": scatter_about(splits[7], (D, D), D ** -0.5, 0.1875, ((0, 32),)),
        "w_out": scatter_about(splits[8], (D, D), (D // 32) ** -0.5, 1.0, ((0, 32),)),
        "ffn_gain": jnp.clip(1.0 + 0.1 * jax.random.normal(splits[9], (D,), jnp.float32), 0.5, 1.5).astype(jnp.bfloat16),
        "gate_weight": scatter_about(splits[10], (D, FF), D ** -0.5, 0.1875, ((0, 32),)),
        "up_weight": scatter_about(splits[11], (D, FF), D ** -0.5, 0.1875, ((0, 32),)),
        "down_weight": scatter_about(splits[12], (FF, D), (FF // 4) ** -0.5, 0.21875, ((0, 32),)),
    }


epsilon = 1e-05
rope_base = 10000.0
score_scale = 0.125
masked_score = -1e+30

@jax.custom_vjp
def low(v):
    return lax.optimization_barrier(v.astype(jnp.bfloat16)).astype(jnp.float32)

@jax.custom_vjp
def low_back(v):
    return v

def low_keep(v):
    return (low(v), None)

def low_pass(kept, grad):
    return (grad,)

def back_keep(v):
    return (v, None)

def back_low(kept, grad):
    return (low(grad),)
low.defvjp(low_keep, low_pass)
low_back.defvjp(back_keep, back_low)

def matmul(left, right):
    return jnp.dot(left, right, precision=lax.Precision.HIGHEST, preferred_element_type=jnp.float32)

def doc_positions(segment_row):
    places = jnp.arange(segment_row.shape[0], dtype=jnp.int32)
    doc_edges = jnp.concatenate([jnp.ones((1,), dtype=jnp.bool_), segment_row[1:] != segment_row[:-1]])
    starts = lax.cummax(jnp.where(doc_edges, places, 0), axis=0)
    return places - starts

def rotary_tables(positions):
    frequency = rope_base ** (-jnp.arange(HEAD_DIM // 2, dtype=jnp.float32) * 2.0 / HEAD_DIM)
    angles = positions.astype(jnp.float32)[:, None] * frequency[None, :]
    return (jnp.cos(angles)[:, None, :], jnp.sin(angles)[:, None, :])

def rotate(values, cos_table, sin_table):
    half_width = values.shape[-1] // 2
    first_half = values[..., :half_width]
    second_half = values[..., half_width:]
    return jnp.concatenate([first_half * cos_table - second_half * sin_table, second_half * cos_table + first_half * sin_table], axis=-1)

def swish(values):
    return values * jax.nn.sigmoid(values)

def layer(tokens_row, first_row, segment_row, params):
    attn_gain, w_query, w_key, w_value, w_out, ffn_gain, gate_weight, up_weight, down_weight = params
    length = tokens_row.shape[0]
    places = jnp.arange(length, dtype=jnp.int32)
    cos_table, sin_table = rotary_tables(doc_positions(segment_row))
    scale_one = lax.rsqrt(lax.optimization_barrier(jnp.mean(tokens_row * tokens_row, axis=-1, keepdims=True)) + epsilon)
    normed_one = low(tokens_row * scale_one * attn_gain)
    queries = low_back(matmul(normed_one, w_query))
    keys_lin = low_back(matmul(normed_one, w_key))
    values_lin = low_back(matmul(normed_one, w_value))
    query_rot = low(rotate(queries.reshape(length, HEADS, HEAD_DIM), cos_table, sin_table))
    key_rot = low(rotate(keys_lin.reshape(length, HEADS, HEAD_DIM), cos_table, sin_table))
    values_mixed = low(0.5 * values_lin + 0.5 * first_row).reshape(length, HEADS, HEAD_DIM)
    scores = low_back(jnp.einsum('qhd,khd->hqk', query_rot, key_rot, precision=lax.Precision.HIGHEST) * score_scale)
    allowed = (segment_row[:, None] == segment_row[None, :]) & (places[None, :] <= places[:, None])
    masked = jnp.where(allowed[None], scores, masked_score)
    row_peak = lax.optimization_barrier(jnp.max(masked, axis=-1, keepdims=True))
    exp_terms = jnp.exp(masked - row_peak)
    attn_probs = exp_terms / lax.optimization_barrier(jnp.sum(exp_terms, axis=-1, keepdims=True))
    attended = jnp.einsum('hqk,khd->qhd', low(attn_probs), values_mixed, precision=lax.Precision.HIGHEST)
    context = low(low_back(attended)).reshape(length, D)
    residual = tokens_row + low_back(matmul(context, w_out))
    scale_two = lax.rsqrt(lax.optimization_barrier(jnp.mean(residual * residual, axis=-1, keepdims=True)) + epsilon)
    second_normed = low(residual * scale_two * ffn_gain)
    gate_activation = low_back(matmul(second_normed, gate_weight))
    up_activation = low_back(matmul(second_normed, up_weight))
    hidden_product = low(swish(gate_activation) * up_activation)
    return residual + low_back(matmul(hidden_product, down_weight))

def reference(tokens, first_values, cotangent, segment_ids, attn_gain, w_query, w_key, w_value, w_out, ffn_gain, gate_weight, up_weight, down_weight):
    params = tuple((weight.astype(jnp.float32) for weight in (attn_gain, w_query, w_key, w_value, w_out, ffn_gain, gate_weight, up_weight, down_weight)))
    tokens_float = tokens.astype(jnp.float32)
    first_float = first_values.astype(jnp.float32)
    checked = jax.checkpoint(layer)

    def forward(tokens_all, first_all, params_all):

        def one_sequence(state_unused, inputs):
            return (state_unused, checked(inputs[0], inputs[1], inputs[2], params_all))
        state_final, outputs = lax.scan(one_sequence, jnp.zeros((), jnp.float32), (tokens_all, first_all, segment_ids))
        return outputs
    output, pullback = jax.vjp(forward, tokens_float, first_float, params)
    token_grad, first_grad, param_grads = pullback(cotangent.astype(jnp.float32))
    return (output.astype(jnp.bfloat16), token_grad, first_grad, param_grads[0], param_grads[1], param_grads[2], param_grads[3], param_grads[4], param_grads[5], param_grads[6], param_grads[7], param_grads[8])
```

```python
import functools
import jax
import jax.numpy as jnp
from jax import lax
from jax.experimental import pallas as pl
from jax.experimental.pallas import tpu as pltpu
from jax.sharding import PartitionSpec as P

HEADS = 16
HEAD_DIM = 64
MESH_ID = pl.DeviceIdType.MESH

epsilon = 1e-05
rope_base = 10000.0
score_scale = 0.125
masked_score = -1e30


def inverse_rms(values):
    return lax.rsqrt(jnp.mean(values * values, axis=-1, keepdims=True) + epsilon)


def rotate(values, cos_table, sin_table):
    half_width = values.shape[-1] // 2
    first_half = values[..., :half_width]
    second_half = values[..., half_width:]
    return jnp.concatenate(
        [
            first_half * cos_table - second_half * sin_table,
            second_half * cos_table + first_half * sin_table,
        ],
        axis=-1,
    )


def unrotate(values, cos_table, sin_table):
    half_width = values.shape[-1] // 2
    first_half = values[..., :half_width]
    second_half = values[..., half_width:]
    return jnp.concatenate(
        [
            first_half * cos_table + second_half * sin_table,
            second_half * cos_table - first_half * sin_table,
        ],
        axis=-1,
    )


def swish(values):
    return values * jax.nn.sigmoid(values)


def layout(segments, ctx_rank, row_count):
    length = segments.shape[1]
    places = jnp.arange(length, dtype=jnp.int32)
    doc_edges = jnp.concatenate(
        [jnp.ones((segments.shape[0], 1), dtype=jnp.bool_), segments[:, 1:] != segments[:, :-1]],
        axis=1,
    )
    starts = lax.cummax(jnp.where(doc_edges, places[None, :], 0), axis=1)
    positions = places[None, :] - starts
    first_row = ctx_rank * row_count
    local_places = first_row + jnp.arange(row_count, dtype=jnp.int32)
    local_segments = lax.dynamic_slice_in_dim(segments, first_row, row_count, 1)
    local_positions = lax.dynamic_slice_in_dim(positions, first_row, row_count, 1)
    allowed = (local_segments[:, :, None] == segments[:, None, :]) & (
        places[None, None, :] <= local_places[None, :, None]
    )
    frequency = rope_base ** (-jnp.arange(HEAD_DIM // 2, dtype=jnp.float32) * 2.0 / HEAD_DIM)
    angles = local_positions.astype(jnp.float32)[:, :, None] * frequency
    return (allowed, jnp.cos(angles)[:, :, None, :], jnp.sin(angles)[:, :, None, :])


def position():
    dp = lax.axis_index("dp")
    ct = lax.axis_index("ctx")
    return lax.div(dp, 2), lax.rem(dp, 2), lax.div(ct, 2), lax.rem(ct, 2)


def visit(step, z, planes):
    back = planes - 1 - step
    high = back + jnp.where(back >= z, 1, 0)
    low = planes - 1 - back
    low = low - jnp.where(low <= z, 1, 0)
    other = jnp.where(z < planes // 2, low, high)
    return jnp.where(step == 0, z, other)


def device(z, y, x, c):
    return (z * 2 + y, x * 2 + c)


def halves(shape):
    if shape[0] % 2 == 0:
        cut = shape[0] // 2
        return (pl.ds(0, cut), slice(None), slice(None)), (pl.ds(cut, cut), slice(None), slice(None))
    cut = shape[2] // 2 // 128 * 128
    return (
        (slice(None), slice(None), pl.ds(0, cut)),
        (slice(None), slice(None), pl.ds(cut, shape[2] - cut)),
    )


def entry_barrier(z, y, x, c, planes):
    barrier = pltpu.get_barrier_semaphore()

    def hello(target):
        pl.semaphore_signal(barrier, inc=1, device_id=target, device_id_type=MESH_ID)

    hello(device(z, y, 1 - x, c))
    hello(device(z, 1 - y, x, c))
    hello(device(z, y, x, 1 - c))

    @pl.when(z > 0)
    def _():
        hello(device(z - 1, y, x, c))

    @pl.when(z < planes - 1)
    def _():
        hello(device(z + 1, y, x, c))

    pl.semaphore_wait(barrier, 3 + jnp.where(z > 0, 1, 0) + jnp.where(z < planes - 1, 1, 0))


def gather_kernel(planes, shapes, *refs):
    n = len(shapes)
    ins, outs, sems = refs[:n], refs[n : 2 * n], refs[2 * n :]
    own_sem, z_send, z_recv, x_send, x_recv, y_send, y_recv, d_send, d_recv, c_send, c_recv = sems
    z, y, x, c = position()
    entry_barrier(z, y, x, c, planes)
    local = [
        pltpu.make_async_copy(ins[g], outs[g].at[:, z, y, x, c], own_sem.at[g]) for g in range(n)
    ]
    for copy in local:
        copy.start()

    def push(src, dst, send, recv, target):
        return pltpu.make_async_remote_copy(
            src_ref=src,
            dst_ref=dst,
            send_sem=send,
            recv_sem=recv,
            device_id=target,
            device_id_type=MESH_ID,
        )

    def spot(g, zz, yy, xx):
        return outs[g].at[:, zz, yy, xx, c]

    def z_copy(g, zz, up, own):
        side = 1 if up else 0
        return push(
            ins[g] if own else spot(g, zz, y, x),
            spot(g, zz, y, x),
            z_send.at[g, zz, side],
            z_recv.at[g, zz],
            device(z + 1 if up else z - 1, y, x, c),
        )

    def x_copy(g, zz, own):
        return push(
            ins[g] if own else spot(g, zz, y, x),
            spot(g, zz, y, x),
            x_send.at[g, zz],
            x_recv.at[g, zz],
            device(z, y, 1 - x, c),
        )

    def y_copy(g, zz, own):
        return push(
            ins[g] if own else spot(g, zz, y, x),
            spot(g, zz, y, x),
            y_send.at[g, zz],
            y_recv.at[g, zz],
            device(z, 1 - y, x, c),
        )

    def relay(g, zz, half):
        part = halves(shapes[g])[half]
        if half == 0:
            here, target = spot(g, zz, y, 1 - x), device(z, 1 - y, x, c)
        else:
            here, target = spot(g, zz, 1 - y, x), device(z, y, 1 - x, c)
        here = here.at[part]
        return push(here, here, d_send.at[g, zz, half], d_recv.at[g, zz, half], target)

    def diag_arrival(g, zz, half):
        part = halves(shapes[g])[half]
        here = spot(g, zz, 1 - y, 1 - x).at[part]
        return push(
            here, here, d_send.at[g, zz, half], d_recv.at[g, zz, half], device(z, y, x, 1 - c)
        )

    def core_copy(g, zz, mine):
        here = outs[g].at[:, zz, :, :, c if mine else 1 - c]
        return push(here, here, c_send.at[g, zz], c_recv.at[g, zz], device(z, y, x, 1 - c))

    def spread(g, zz, own):
        if own:

            @pl.when(z > 0)
            def _():
                z_copy(g, zz, False, True).start()

            @pl.when(z < planes - 1)
            def _():
                z_copy(g, zz, True, True).start()

        else:

            @pl.when((zz < z) & (z < planes - 1))
            def _():
                z_copy(g, zz, True, False).start()

            @pl.when((zz > z) & (z > 0))
            def _():
                z_copy(g, zz, False, False).start()

        x_copy(g, zz, own).start()
        y_copy(g, zz, own).start()

    items = [(t, g) for t in range(planes) for g in range(n)]
    lag_plane, lag_core = n, 2 * n

    def stage_plane(t, g):
        zz = visit(t, z, planes)
        x_copy(g, zz, False).wait_recv()
        relay(g, zz, 0).start()
        y_copy(g, zz, False).wait_recv()
        relay(g, zz, 1).start()

    def stage_core(t, g):
        zz = visit(t, z, planes)
        if t == 0:
            local[g].wait()
        diag_arrival(g, zz, 0).wait_recv()
        diag_arrival(g, zz, 1).wait_recv()
        core_copy(g, zz, True).start()

    for i in range(len(items) + lag_core):
        if i < len(items):
            t, g = items[i]
            zz = visit(t, z, planes)
            if t > 0:
                z_copy(g, zz, True, False).wait_recv()
            spread(g, zz, t == 0)
        if 0 <= i - lag_plane < len(items):
            stage_plane(*items[i - lag_plane])
        if 0 <= i - lag_core < len(items):
            stage_core(*items[i - lag_core])
    for t, g in items:
        zz = visit(t, z, planes)
        core_copy(g, zz, False).wait_recv()
        core_copy(g, zz, True).wait_send()
        x_copy(g, zz, t == 0).wait_send()
        y_copy(g, zz, t == 0).wait_send()
        relay(g, zz, 0).wait_send()
        relay(g, zz, 1).wait_send()
        if t == 0:

            @pl.when(z > 0)
            def _():
                z_copy(g, zz, False, True).wait_send()

            @pl.when(z < planes - 1)
            def _():
                z_copy(g, zz, True, True).wait_send()

        else:

            @pl.when((zz < z) & (z < planes - 1))
            def _():
                z_copy(g, zz, True, False).wait_send()

            @pl.when((zz > z) & (z > 0))
            def _():
                z_copy(g, zz, False, False).wait_send()


def gather(planes, blocks):
    n = len(blocks)
    shapes = [b.shape for b in blocks]
    dma = pltpu.SemaphoreType.DMA
    return pl.pallas_call(
        functools.partial(gather_kernel, planes, shapes),
        out_shape=[
            jax.ShapeDtypeStruct((s[0], planes, 2, 2, 2, s[1], s[2]), b.dtype)
            for s, b in zip(shapes, blocks)
        ],
        in_specs=[pl.BlockSpec(memory_space=pl.ANY)] * n,
        out_specs=[pl.BlockSpec(memory_space=pl.ANY)] * n,
        scratch_shapes=[
            dma((n,)),
            dma((n, planes, 2)),
            dma((n, planes)),
            dma((n, planes)),
            dma((n, planes)),
            dma((n, planes)),
            dma((n, planes)),
            dma((n, planes, 2)),
            dma((n, planes, 2)),
            dma((n, planes)),
            dma((n, planes)),
        ],
        compiler_params=pltpu.CompilerParams(collective_id=0, has_side_effects=True),
        name="weight_gather",
    )(*blocks)


def columns(shape, half):
    cut = shape[1] // 2 // 128 * 128
    return pl.ds(0, cut) if half == 0 else pl.ds(cut, shape[1] - cut)


def scatter_kernel(planes, shapes, lags, *refs):
    n = len(shapes)
    parts, outs, refs = refs[:n], refs[n : 2 * n], refs[2 * n :]
    own, from_core, from_dx, from_dy, from_x, from_y, from_z = (
        refs[k * n : (k + 1) * n] for k in range(7)
    )
    own_sem, c_send, c_recv, d_send, d_recv, x_send, x_recv, y_send, y_recv, z_send, z_recv = refs[
        7 * n :
    ]
    z, y, x, c = position()
    entry_barrier(z, y, x, c, planes)
    items = [(planes - 1 - t, g) for t in range(planes) for g in range(n)]

    def push(src, dst, send, recv, target):
        return pltpu.make_async_remote_copy(
            src_ref=src,
            dst_ref=dst,
            send_sem=send,
            recv_sem=recv,
            device_id=target,
            device_id_type=MESH_ID,
        )

    def load(g, zz):
        return pltpu.make_async_copy(
            parts[g].at[zz, :, :, c], own[g].at[zz], own_sem.at[g, zz]
        )

    def core_copy(g, zz):
        return push(
            parts[g].at[zz, :, :, 1 - c],
            from_core[g].at[zz],
            c_send.at[g, zz],
            c_recv.at[g, zz],
            device(z, y, x, 1 - c),
        )

    def diag(g, zz, half):
        part = columns(shapes[g], half)
        box = (from_dx if half == 0 else from_dy)[g].at[zz]
        return push(
            own[g].at[zz, 1 - y, 1 - x, :, part],
            box,
            d_send.at[g, zz, half],
            d_recv.at[g, zz, half],
            device(z, y, 1 - x, c) if half == 0 else device(z, 1 - y, x, c),
        )

    def x_copy(g, zz):
        return push(
            own[g].at[zz, y, 1 - x],
            from_x[g].at[zz],
            x_send.at[g, zz],
            x_recv.at[g, zz],
            device(z, y, 1 - x, c),
        )

    def y_copy(g, zz):
        return push(
            own[g].at[zz, 1 - y, x],
            from_y[g].at[zz],
            y_send.at[g, zz],
            y_recv.at[g, zz],
            device(z, 1 - y, x, c),
        )

    def z_copy(g, zz, up):
        slot = zz if up else jnp.where(zz == z - 1, planes, zz)
        return push(
            own[g].at[zz, y, x],
            from_z[g].at[slot],
            z_send.at[g, zz],
            z_recv.at[g, slot],
            device(z + 1 if up else z - 1, y, x, c),
        )

    def z_arrival(g, slot):
        return push(
            from_z[g].at[slot],
            from_z[g].at[slot],
            z_send.at[g, 0],
            z_recv.at[g, slot],
            device(z, y, x, 1 - c),
        )

    f32 = jnp.float32

    def add(dst, *srcs):
        total = dst[...].astype(f32)
        for src in srcs:
            total = total + src[...].astype(f32)
        dst[...] = total.astype(dst.dtype)

    for t, g in items:
        zz = visit(t, z, planes)
        core_copy(g, zz).start()
        load(g, zz).start()

    def stage_core(t, g):
        zz = visit(t, z, planes)
        load(g, zz).wait()
        core_copy(g, zz).wait_recv()
        add(own[g].at[zz, 1 - y, 1 - x], from_core[g].at[zz, 1 - y, 1 - x])
        diag(g, zz, 0).start()
        diag(g, zz, 1).start()
        add(own[g].at[zz, y, 1 - x], from_core[g].at[zz, y, 1 - x])
        add(own[g].at[zz, 1 - y, x], from_core[g].at[zz, 1 - y, x])
        add(own[g].at[zz, y, x], from_core[g].at[zz, y, x])

    def stage_plane(t, g):
        zz = visit(t, z, planes)
        diag(g, zz, 0).wait_recv()
        add(own[g].at[zz, 1 - y, x, :, columns(shapes[g], 0)], from_dx[g].at[zz])
        y_copy(g, zz).start()
        diag(g, zz, 1).wait_recv()
        add(own[g].at[zz, y, 1 - x, :, columns(shapes[g], 1)], from_dy[g].at[zz])
        x_copy(g, zz).start()

    def stage_line(t, g):
        zz = visit(t, z, planes)
        x_copy(g, zz).wait_recv()
        y_copy(g, zz).wait_recv()
        here = own[g].at[zz, y, x]
        if t > 0:
            add(here, from_x[g].at[zz], from_y[g].at[zz])
            farther = jnp.where(zz > z, z > 0, z < planes - 1)

            @pl.when(farther)
            def _():
                z_arrival(g, zz).wait_recv()
                add(here, from_z[g].at[zz])

            @pl.when(zz > z)
            def _():
                z_copy(g, zz, True).start()

            @pl.when(zz < z)
            def _():
                z_copy(g, zz, False).start()

        else:
            outs[g][...] = (
                here[...].astype(f32)
                + from_x[g][zz].astype(f32)
                + from_y[g][zz].astype(f32)
            )

            @pl.when(z > 0)
            def _():
                z_arrival(g, zz).wait_recv()
                outs[g][...] += from_z[g][zz].astype(f32)

            @pl.when(z < planes - 1)
            def _():
                z_arrival(g, planes).wait_recv()
                outs[g][...] += from_z[g][planes].astype(f32)

    lag_plane, lag_line = lags
    for i in range(len(items) + lag_line):
        if i < len(items):
            stage_core(*items[i])
        if 0 <= i - lag_plane < len(items):
            stage_plane(*items[i - lag_plane])
        if 0 <= i - lag_line < len(items):
            stage_line(*items[i - lag_line])
    for t, g in items:
        zz = visit(t, z, planes)
        core_copy(g, zz).wait_send()
        diag(g, zz, 0).wait_send()
        diag(g, zz, 1).wait_send()
        x_copy(g, zz).wait_send()
        y_copy(g, zz).wait_send()
        if t > 0:
            z_copy(g, zz, True).wait_send()


def scatter_sum(planes, partials, lags, collective_id=1):
    n = len(partials)
    shapes = [p.shape[4:] for p in partials]
    types = [p.dtype for p in partials]
    dma = pltpu.SemaphoreType.DMA

    def boxes(lead, half=None):
        out = []
        for s, d in zip(shapes, types):
            cut = s[1] // 2 // 128 * 128
            width = s[1] if half is None else (cut if half == 0 else s[1] - cut)
            out.append(pltpu.VMEM((*lead, s[0], width), d))
        return out

    return pl.pallas_call(
        functools.partial(scatter_kernel, planes, shapes, lags),
        out_shape=[jax.ShapeDtypeStruct(s, jnp.float32) for s in shapes],
        in_specs=[pl.BlockSpec(memory_space=pl.ANY)] * n,
        out_specs=[pl.BlockSpec(memory_space=pltpu.VMEM)] * n,
        scratch_shapes=[
            *boxes((planes, 2, 2)),
            *boxes((planes, 2, 2)),
            *boxes((planes,), 0),
            *boxes((planes,), 1),
            *boxes((planes,)),
            *boxes((planes,)),
            *boxes((planes + 1,)),
            dma((n, planes)),
            dma((n, planes)),
            dma((n, planes)),
            dma((n, planes, 2)),
            dma((n, planes, 2)),
            dma((n, planes)),
            dma((n, planes)),
            dma((n, planes)),
            dma((n, planes)),
            dma((n, planes)),
            dma((n, planes + 1)),
        ],
        compiler_params=pltpu.CompilerParams(
            collective_id=collective_id, has_side_effects=True, vmem_limit_bytes=62 * 2**20
        ),
        name="gradient_scatter",
    )(*partials)


X_SEND = ((0, 2), (1, 3))
X_BACK = ((2, 0), (3, 1))
CORES = ((0, 1), (1, 0), (2, 3), (3, 2))


def share_keys(pair):
    rank = lax.axis_index("ctx")
    from_x = lax.ppermute(pair, "ctx", X_SEND)
    both = jnp.stack([pair, from_x])
    other = lax.ppermute(both, "ctx", CORES)
    odd = rank % 2 == 1
    high = rank >= 2
    first = jnp.where(odd, other, both)
    second = jnp.where(odd, both, other)
    zero = jnp.zeros_like(first[0])
    tiles = [
        jnp.where(high, first[1], first[0]),
        jnp.where(high, second[1], second[0]),
        jnp.where(high, first[0], zero),
        jnp.where(high, second[0], zero),
    ]
    return jnp.concatenate(tiles, axis=2)


def return_sums(pair):
    rank = lax.axis_index("ctx")
    rows = pair.shape[2] // 4
    odd = rank % 2 == 1
    high = rank >= 2
    tiles = [pair[:, :, i * rows : (i + 1) * rows] for i in range(4)]
    low = pair.dtype
    mine = jnp.stack(
        [jnp.where(odd, tiles[1], tiles[0]), jnp.where(odd, tiles[3], tiles[2])]
    )
    theirs = jnp.stack(
        [jnp.where(odd, tiles[0], tiles[1]), jnp.where(odd, tiles[2], tiles[3])]
    )
    got = lax.ppermute(theirs, "ctx", CORES)
    chip = mine.astype(jnp.float32) + got.astype(jnp.float32)
    back = lax.ppermute(chip[0].astype(low), "ctx", X_BACK)
    return jnp.where(high, chip[1], chip[0]) + back.astype(jnp.float32)


def on_device(
    planes,
    tokens,
    first_values,
    cotangent,
    segment_ids,
    attn_gain,
    w_query,
    w_key,
    w_value,
    w_out,
    ffn_gain,
    gate_weight,
    up_weight,
    down_weight,
):
    f32, bf16 = jnp.float32, jnp.bfloat16
    devices = planes * 8
    seqs, rows, width = tokens.shape
    rank = lax.axis_index("ctx")
    share = attn_gain.shape[0]
    gains = jnp.zeros((1, 16, 128), bf16)
    gains = gains.at[0, 0, :share].set(attn_gain).at[0, 1, :share].set(ffn_gain)
    shards = (gains, w_query, w_key, w_value, w_out, gate_weight, up_weight, down_weight)
    blocks = [s if s.ndim == 3 else s[None] for s in shards]
    gathered = gather(planes, blocks)
    gain_all = gathered[0].reshape(devices, 16, 128)
    attn_gain = gain_all[:, 0, :share].reshape(width)
    ffn_gain = gain_all[:, 1, :share].reshape(width)
    w_query, w_key, w_value, w_out, gate_weight, up_weight, down_weight = (
        g.reshape(devices * b.shape[1], b.shape[2]) for g, b in zip(gathered[1:], blocks[1:])
    )
    allowed, cos_table, sin_table = layout(segment_ids, rank, rows)

    head_shape = (seqs, rows, HEADS, HEAD_DIM)
    mm = functools.partial(jnp.einsum, preferred_element_type=f32)
    tokens_float = tokens.astype(f32)
    scale_one = inverse_rms(tokens_float)
    normed_one = (tokens_float * scale_one * attn_gain.astype(f32)).astype(bf16)
    queries = mm("mrd,de->mre", normed_one, w_query)
    keys_lin = mm("mrd,de->mre", normed_one, w_key)
    values_lin = mm("mrd,de->mre", normed_one, w_value)
    query_rot = rotate(queries.reshape(head_shape), cos_table, sin_table).astype(bf16)
    key_rot = rotate(keys_lin.reshape(head_shape), cos_table, sin_table).astype(bf16)
    values_mixed = (0.5 * values_lin + 0.5 * first_values.astype(f32)).astype(bf16)
    pair = share_keys(jnp.stack([key_rot.reshape(seqs, rows, width), values_mixed]))
    length = pair.shape[2]
    key_heads = pair[0].reshape(seqs, length, HEADS, HEAD_DIM)
    value_heads = pair[1].reshape(seqs, length, HEADS, HEAD_DIM)
    scores = mm("mqhd,mkhd->mhqk", query_rot, key_heads) * score_scale
    masked = jnp.where(allowed[:, None], scores, masked_score)
    row_peak = jnp.max(masked, axis=-1, keepdims=True)
    exp_terms = jnp.exp(masked - row_peak)
    row_total = jnp.sum(exp_terms, axis=-1, keepdims=True)
    attn_probs = exp_terms / row_total
    attended = mm("mhqk,mkhd->mqhd", attn_probs.astype(bf16), value_heads)
    context = attended.astype(bf16).reshape(seqs, rows, width)
    residual = tokens_float + mm("mrd,de->mre", context, w_out)
    scale_two = inverse_rms(residual)
    second_normed = (residual * scale_two * ffn_gain.astype(f32)).astype(bf16)
    gate = mm("ajo,oc->ajc", second_normed, gate_weight)
    up = mm("ajo,oc->ajc", second_normed, up_weight)
    hidden = (swish(gate) * up).astype(bf16)
    output = (residual + mm("biu,ue->bie", hidden, down_weight)).astype(bf16)

    out_float = cotangent.astype(f32)
    d_down = mm("tba,tby->ay", hidden, cotangent).astype(bf16)
    d_hidden = mm("voc,sc->vos", cotangent, down_weight)
    sigmoid_gate = jax.nn.sigmoid(gate)
    d_gate = (d_hidden * up * sigmoid_gate * (1.0 + gate * (1.0 - sigmoid_gate))).astype(bf16)
    d_up = (d_hidden * (gate * sigmoid_gate)).astype(bf16)
    d_gate_weight = mm("noj,noa->ja", second_normed, d_gate).astype(bf16)
    d_up_weight = mm("noj,noa->ja", second_normed, d_up).astype(bf16)
    d_normed_two = mm("pvn,zn->pvz", d_gate, gate_weight) + mm("pvn,zn->pvz", d_up, up_weight)
    d_ffn_gain = jnp.sum(d_normed_two * residual * scale_two, axis=(0, 1))
    weighted_two = d_normed_two * ffn_gain.astype(f32)
    d_residual = (
        out_float
        + scale_two * weighted_two
        - residual
        * (scale_two * scale_two * scale_two)
        * jnp.mean(weighted_two * residual, axis=-1, keepdims=True)
    )
    d_residual_low = d_residual.astype(bf16)
    d_out = mm("mrd,mre->de", context, d_residual_low).astype(bf16)
    d_context = mm("mre,de->mrd", d_residual_low, w_out).astype(bf16).reshape(head_shape)
    d_probs = mm("mqhd,mkhd->mhqk", d_context, value_heads)
    value_part = mm("mhqk,mqhd->mkhd", attn_probs.astype(bf16), d_context)
    d_scores = (
        attn_probs * (d_probs - jnp.sum(d_probs * attn_probs, axis=-1, keepdims=True))
    ).astype(bf16)
    d_query_rot = mm("mhqk,mkhd->mqhd", d_scores, key_heads) * score_scale
    key_part = mm("mhqk,mqhd->mkhd", d_scores, query_rot) * score_scale
    flat = (seqs, length, width)
    d_pair = return_sums(jnp.stack([key_part.reshape(flat), value_part.reshape(flat)]).astype(bf16))
    d_key_rot, d_mixed = d_pair[0], d_pair[1]
    local = (seqs, rows, width)
    d_query = unrotate(d_query_rot, cos_table, sin_table).astype(bf16).reshape(local)
    d_key = (
        unrotate(d_key_rot.reshape(head_shape), cos_table, sin_table).astype(bf16).reshape(local)
    )
    d_value = (0.5 * d_mixed).astype(bf16)
    first_grad = 0.5 * d_mixed
    d_wq = mm("mrd,mre->de", normed_one, d_query).astype(bf16)
    d_wk = mm("mrd,mre->de", normed_one, d_key).astype(bf16)
    d_wv = mm("mrd,mre->de", normed_one, d_value).astype(bf16)
    d_normed_one = (
        mm("mre,de->mrd", d_query, w_query)
        + mm("mre,de->mrd", d_key, w_key)
        + mm("mre,de->mrd", d_value, w_value)
    )
    d_attn_gain = jnp.sum(d_normed_one * tokens_float * scale_one, axis=(0, 1))
    weighted_one = d_normed_one * attn_gain.astype(f32)
    token_grad = (
        d_residual
        + scale_one * weighted_one
        - tokens_float
        * (scale_one * scale_one * scale_one)
        * jnp.mean(weighted_one * tokens_float, axis=-1, keepdims=True)
    )
    d_gains = jnp.stack([d_attn_gain, d_ffn_gain]).reshape(2, devices, share)
    d_gains = jnp.zeros((devices, 8, 256), f32).at[:, :2, :share].set(d_gains.transpose(1, 0, 2))
    partials = [
        g.reshape(planes, 2, 2, 2, g.size // g.shape[-1] // devices, g.shape[-1])
        for g in (d_down, d_gate_weight, d_up_weight, d_out, d_wq, d_wk, d_wv, d_gains)
    ]
    s_down, s_gate, s_up, s_out, s_wq, s_wk, s_wv, s_gains = scatter_sum(planes, partials, (4, 8))
    return (
        output,
        token_grad,
        first_grad,
        s_gains[0, :share],
        s_wq,
        s_wk,
        s_wv,
        s_out,
        s_gains[1, :share],
        s_gate,
        s_up,
        s_down,
    )


def solution(mesh):
    token, weight, vector = P("dp", "ctx", None), P(("dp", "ctx"), None), P(("dp", "ctx"))
    return jax.shard_map(
        functools.partial(on_device, mesh.shape["dp"] // 2),
        mesh=mesh,
        in_specs=(
            token,
            token,
            token,
            P("dp", None),
            vector,
            weight,
            weight,
            weight,
            weight,
            vector,
            weight,
            weight,
            weight,
        ),
        out_specs=(
            token,
            token,
            token,
            vector,
            weight,
            weight,
            weight,
            weight,
            vector,
            weight,
            weight,
            weight,
        ),
        check_vma=False,
    )
```

```python
import functools
import jax
import jax.numpy as jnp
from jax import lax
from jax.experimental import pallas as pl
from jax.experimental.pallas import tpu as pltpu
from jax.sharding import PartitionSpec as P

HEADS = 16
HEAD_DIM = 64
MESH_ID = pl.DeviceIdType.MESH

epsilon = 1e-05
rope_base = 10000.0
score_scale = 0.125
masked_score = -1e30


def inverse_rms(values):
    return lax.rsqrt(jnp.mean(values * values, axis=-1, keepdims=True) + epsilon)


def swish(values):
    return values * jax.nn.sigmoid(values)


def first_half(shape):
    return lax.broadcasted_iota(jnp.int32, shape, len(shape) - 1) % HEAD_DIM < HEAD_DIM // 2


def swap_halves(values):
    return jnp.where(
        first_half(values.shape), pltpu.roll(values, 96, 1), pltpu.roll(values, 32, 1)
    )


def turned(values, cos_table, sin_table, sign):
    return values * cos_table + sign * (swap_halves(values) * sin_table)


def tables(segment_ids, rank, rows):
    seqs, length = segment_ids.shape
    places = jnp.arange(length, dtype=jnp.int32)
    edges = jnp.concatenate(
        [jnp.ones((seqs, 1), dtype=jnp.bool_), segment_ids[:, 1:] != segment_ids[:, :-1]], axis=1
    )
    starts = lax.cummax(jnp.where(edges, places[None, :], 0), axis=1)
    starts = lax.dynamic_slice_in_dim(starts, rank * rows, rows, 1)
    local = rank * rows + jnp.arange(rows, dtype=jnp.int32) - starts
    lane = jnp.arange(128, dtype=jnp.int32)
    half = HEAD_DIM // 2
    frequency = rope_base ** (-(lane % half).astype(jnp.float32) * 2.0 / HEAD_DIM)
    angles = local.astype(jnp.float32).reshape(seqs * rows, 1) * frequency
    sign = jnp.where(lane % HEAD_DIM < half, -1.0, 1.0)
    return starts.reshape(seqs, 1, rows), jnp.cos(angles), jnp.sin(angles) * sign


def project_kernel(tok, first, gain, wq, wk, wv, cos_ref, sin_ref, normed, query, pair):
    f32, bf16 = jnp.float32, jnp.bfloat16

    @pl.when(pl.program_id(0) == 0)
    def _():
        values = tok[...].astype(f32)
        normed[...] = (values * inverse_rms(values) * gain[...].astype(f32)).astype(bf16)

    n1 = normed[...]
    cos_table, sin_table = cos_ref[...], sin_ref[...]
    queries = jnp.dot(n1, wq[...], preferred_element_type=f32)
    keys = jnp.dot(n1, wk[...], preferred_element_type=f32)
    values = jnp.dot(n1, wv[...], preferred_element_type=f32)
    for i in range(queries.shape[1] // 128):
        lanes = slice(i * 128, i * 128 + 128)
        query[:, lanes] = turned(queries[:, lanes], cos_table, sin_table, 1.0).astype(bf16)
        pair[0, :, lanes] = turned(keys[:, lanes], cos_table, sin_table, 1.0).astype(bf16)
    pair[1] = (0.5 * values + 0.5 * first[...].astype(f32)).astype(bf16)


def project(tok, first, gain, wq, wk, wv, cos_table, sin_table):
    rows, width = tok.shape
    tile = 256
    whole = lambda i: (0, 0)
    column = lambda i: (0, i)
    wide = lambda: pl.BlockSpec((width, tile), column)
    return pl.pallas_call(
        project_kernel,
        grid=(width // tile,),
        in_specs=[
            pl.BlockSpec((rows, width), whole),
            pl.BlockSpec((rows, tile), column),
            pl.BlockSpec((1, width), whole),
            wide(),
            wide(),
            wide(),
            pl.BlockSpec((rows, 128), whole),
            pl.BlockSpec((rows, 128), whole),
        ],
        out_specs=[
            pl.BlockSpec((rows, width), whole),
            pl.BlockSpec((rows, tile), column),
            pl.BlockSpec((2, rows, tile), lambda i: (0, 0, i)),
        ],
        out_shape=[
            jax.ShapeDtypeStruct((rows, width), jnp.bfloat16),
            jax.ShapeDtypeStruct((rows, width), jnp.bfloat16),
            jax.ShapeDtypeStruct((2, rows, width), jnp.bfloat16),
        ],
        name="project",
    )(tok, first, gain, wq, wk, wv, cos_table, sin_table)


def two_heads(block, scale):
    lane = lax.broadcasted_iota(jnp.int32, block.shape, 1)
    scaled = block * jnp.asarray(scale, block.dtype)
    zero = jnp.zeros_like(block)
    return jnp.concatenate(
        [jnp.where(lane < HEAD_DIM, scaled, zero), jnp.where(lane < HEAD_DIM, zero, scaled)]
    )


def own_lanes(both):
    rows = both.shape[1] // 2
    lane = lax.broadcasted_iota(jnp.int32, (both.shape[0], rows), 0)
    return jnp.where(lane < HEAD_DIM, both[:, :rows], both[:, rows:]).T


def fill_bias(bias, starts, rank):
    rows = bias.shape[1]
    key = lax.broadcasted_iota(jnp.int32, (rows, rows), 0)
    place = rank * rows + lax.broadcasted_iota(jnp.int32, (rows, rows), 1)
    begin = starts[...]
    for t in range(4):
        x, c = lax.div(rank, 2), lax.rem(rank, 2)
        owner = (1 - x if t >= 2 else x) * 2 + (1 - c if t % 2 else c)
        at = owner * rows + key
        bias[t] = jnp.where((at >= begin) & (at <= place), 0.0, masked_score)


NT = (((1,), (1,)), ((), ()))
TN = (((0,), (0,)), ((), ()))


def attend_step(rank, begin, starts, q, tiles, out, log_total, bias, scores, peak, total, acc):
    f32, bf16 = jnp.float32, jnp.bfloat16

    @pl.when(begin)
    def _():
        fill_bias(bias, starts, rank)

    high = rank >= 2
    stacked = two_heads(q, score_scale)

    def score(t):
        s = lax.dot_general(tiles[t][0][...], stacked, NT, preferred_element_type=f32)
        s = s + jnp.concatenate([bias[t], bias[t]], axis=1)
        scores[t] = s
        return jnp.max(s, axis=0, keepdims=True)

    def gather_values(t, top):
        e = jnp.exp(scores[t] - top)
        part = lax.dot_general(tiles[t][1][...], e.astype(bf16), TN, preferred_element_type=f32)
        return jnp.sum(e, axis=0, keepdims=True), part

    peak[...] = jnp.maximum(score(0), score(1))

    @pl.when(high)
    def _():
        peak[...] = jnp.maximum(peak[...], jnp.maximum(score(2), score(3)))

    top = peak[...]
    sum_a, acc_a = gather_values(0, top)
    sum_b, acc_b = gather_values(1, top)
    total[...] = sum_a + sum_b
    acc[...] = acc_a + acc_b

    @pl.when(high)
    def _():
        top = peak[...]
        sum_a, acc_a = gather_values(2, top)
        sum_b, acc_b = gather_values(3, top)
        total[...] += sum_a + sum_b
        acc[...] += acc_a + acc_b

    out[...] = own_lanes(acc[...] / total[...]).astype(bf16)
    log_total[...] = peak[...] + jnp.log(total[...])


def attend_scratch(rows):
    return [
        pltpu.VMEM((4, rows, rows), jnp.float32),
        pltpu.VMEM((4, rows, 2 * rows), jnp.float32),
        pltpu.VMEM((1, 2 * rows), jnp.float32),
        pltpu.VMEM((1, 2 * rows), jnp.float32),
        pltpu.VMEM((128, 2 * rows), jnp.float32),
    ]


def attend_kernel(starts, q, tile_a, tile_b, tile_c, tile_d, out, log_total, *scratch):
    attend_step(
        lax.axis_index("ctx"),
        pl.program_id(1) == 0,
        starts.at[0],
        q[0],
        [[t.at[0, 0], t.at[1, 0]] for t in (tile_a, tile_b, tile_c, tile_d)],
        out.at[0],
        log_total.at[0, 0],
        *scratch,
    )


def attend(starts, q, tiles):
    seqs, rows, width = q.shape
    pairs = width // 128
    block = lambda: pl.BlockSpec((1, rows, 128), lambda s, p: (s, 0, p))
    tile = lambda: pl.BlockSpec((2, 1, rows, 128), lambda s, p: (0, s, 0, p))
    return pl.pallas_call(
        attend_kernel,
        grid=(seqs, pairs),
        in_specs=[
            pl.BlockSpec((1, 1, rows), lambda s, p: (s, 0, 0)),
            block(),
            tile(),
            tile(),
            tile(),
            tile(),
        ],
        out_specs=[block(), pl.BlockSpec((1, 1, 1, 2 * rows), lambda s, p: (s, p, 0, 0))],
        out_shape=[
            jax.ShapeDtypeStruct(q.shape, jnp.bfloat16),
            jax.ShapeDtypeStruct((seqs, pairs, 1, 2 * rows), jnp.float32),
        ],
        scratch_shapes=attend_scratch(rows),
        name="attend",
    )(starts, q, *tiles)


def attend_back_step(
    rank, begin, starts, q, tiles, context, d_context, log_total, cos_t, sin_t, d_q, d_tiles, bias, acc
):
    f32, bf16 = jnp.float32, jnp.bfloat16

    @pl.when(begin)
    def _():
        fill_bias(bias, starts, rank)

    high = rank >= 2
    stacked = two_heads(q, score_scale)
    stacked_do = two_heads(d_context, 1.0)
    turned_product = (d_context.astype(f32) * context.astype(f32)).T
    delta = jnp.concatenate(
        [
            jnp.sum(turned_product[:HEAD_DIM], axis=0, keepdims=True),
            jnp.sum(turned_product[HEAD_DIM:], axis=0, keepdims=True),
        ],
        axis=1,
    )
    lse = log_total[...]

    def one(t):
        keys, values = tiles[t][0][...], tiles[t][1][...]
        s = lax.dot_general(keys, stacked, NT, preferred_element_type=f32)
        s = s + jnp.concatenate([bias[t], bias[t]], axis=1)
        p = jnp.exp(s - lse)
        dp = lax.dot_general(values, stacked_do, NT, preferred_element_type=f32)
        ds = (p * (dp - delta)).astype(bf16)
        d_tiles[t][1][...] = jnp.dot(p.astype(bf16), stacked_do, preferred_element_type=f32).astype(bf16)
        d_tiles[t][0][...] = jnp.dot(ds, stacked, preferred_element_type=f32).astype(bf16)
        return lax.dot_general(keys, ds, TN, preferred_element_type=f32)

    acc[...] = one(0) + one(1)

    @pl.when(high)
    def _():
        acc[...] += one(2) + one(3)

    d_q[...] = turned(own_lanes(acc[...]) * score_scale, cos_t[...], sin_t[...], -1.0).astype(bf16)


def attend_back_scratch(rows):
    return [pltpu.VMEM((4, rows, rows), jnp.float32), pltpu.VMEM((128, 2 * rows), jnp.float32)]


def attend_back_kernel(starts, q, ta, tb, tc, td, o, do, lse, cos_t, sin_t, dq, da, db, dc, dd, *scratch):
    attend_back_step(
        lax.axis_index("ctx"),
        pl.program_id(1) == 0,
        starts.at[0],
        q[0],
        [[t.at[0, 0], t.at[1, 0]] for t in (ta, tb, tc, td)],
        o[0],
        do[0],
        lse.at[0, 0],
        cos_t.at[0],
        sin_t.at[0],
        dq.at[0],
        [[t.at[0, 0], t.at[1, 0]] for t in (da, db, dc, dd)],
        *scratch,
    )


def attend_back(starts, q, tiles, context, d_context, log_total, cos_table, sin_table):
    seqs, rows, width = q.shape
    pairs = width // 128
    block = lambda: pl.BlockSpec((1, rows, 128), lambda s, p: (s, 0, p))
    tile = lambda: pl.BlockSpec((2, 1, rows, 128), lambda s, p: (0, s, 0, p))
    table = lambda: pl.BlockSpec((1, rows, 128), lambda s, p: (s, 0, 0))
    return pl.pallas_call(
        attend_back_kernel,
        grid=(seqs, pairs),
        in_specs=[
            pl.BlockSpec((1, 1, rows), lambda s, p: (s, 0, 0)),
            block(),
            tile(),
            tile(),
            tile(),
            tile(),
            block(),
            block(),
            pl.BlockSpec((1, 1, 1, 2 * rows), lambda s, p: (s, p, 0, 0)),
            table(),
            table(),
        ],
        out_specs=[block(), tile(), tile(), tile(), tile()],
        out_shape=[jax.ShapeDtypeStruct(q.shape, jnp.bfloat16)]
        + [jax.ShapeDtypeStruct(tiles[0].shape, jnp.bfloat16)] * 4,
        scratch_shapes=attend_back_scratch(rows),
        name="attend_back",
    )(
        starts,
        q,
        *tiles,
        context,
        d_context,
        log_total,
        cos_table.reshape(seqs, rows, 128),
        sin_table.reshape(seqs, rows, 128),
    )


def position():
    dp = lax.axis_index("dp")
    ct = lax.axis_index("ctx")
    return lax.div(dp, 2), lax.rem(dp, 2), lax.div(ct, 2), lax.rem(ct, 2)


def visit(step, z, planes):
    back = planes - 1 - step
    high = back + jnp.where(back >= z, 1, 0)
    low = planes - 1 - back
    low = low - jnp.where(low <= z, 1, 0)
    other = jnp.where(z < planes // 2, low, high)
    return jnp.where(step == 0, z, other)


def device(z, y, x, c):
    return (z * 2 + y, x * 2 + c)


def halves(shape):
    if shape[0] % 2 == 0:
        cut = shape[0] // 2
        return (pl.ds(0, cut), slice(None), slice(None)), (pl.ds(cut, cut), slice(None), slice(None))
    cut = shape[2] // 2 // 128 * 128
    return (
        (slice(None), slice(None), pl.ds(0, cut)),
        (slice(None), slice(None), pl.ds(cut, shape[2] - cut)),
    )


def entry_barrier(z, y, x, c, planes):
    barrier = pltpu.get_barrier_semaphore()

    def hello(target):
        pl.semaphore_signal(barrier, inc=1, device_id=target, device_id_type=MESH_ID)

    hello(device(z, y, 1 - x, c))
    hello(device(z, 1 - y, x, c))
    hello(device(z, y, x, 1 - c))

    @pl.when(z > 0)
    def _():
        hello(device(z - 1, y, x, c))

    @pl.when(z < planes - 1)
    def _():
        hello(device(z + 1, y, x, c))

    pl.semaphore_wait(barrier, 3 + jnp.where(z > 0, 1, 0) + jnp.where(z < planes - 1, 1, 0))


def gather_kernel(planes, shapes, with_pair, *refs):
    n = len(shapes)
    ins, refs = refs[:n], refs[n:]
    if with_pair:
        pair, refs = refs[0], refs[1:]
    outs, refs = refs[:n], refs[n:]
    if with_pair:
        tile_b, tile_c, tile_d = refs[:3]
        refs = refs[3:]
        pair_send, pair_recv = refs[-2:]
        refs = refs[:-2]
    sems = refs
    own_sem, z_send, z_recv, x_send, x_recv, y_send, y_recv, d_send, d_recv, c_send, c_recv = sems
    z, y, x, c = position()
    entry_barrier(z, y, x, c, planes)
    local = [
        pltpu.make_async_copy(ins[g], outs[g].at[:, z, y, x, c], own_sem.at[g]) for g in range(n)
    ]
    for copy in local:
        copy.start()

    def push(src, dst, send, recv, target):
        return pltpu.make_async_remote_copy(
            src_ref=src,
            dst_ref=dst,
            send_sem=send,
            recv_sem=recv,
            device_id=target,
            device_id_type=MESH_ID,
        )

    def spot(g, zz, yy, xx):
        return outs[g].at[:, zz, yy, xx, c]

    def z_copy(g, zz, up, own):
        side = 1 if up else 0
        return push(
            ins[g] if own else spot(g, zz, y, x),
            spot(g, zz, y, x),
            z_send.at[g, zz, side],
            z_recv.at[g, zz],
            device(z + 1 if up else z - 1, y, x, c),
        )

    def x_copy(g, zz, own):
        return push(
            ins[g] if own else spot(g, zz, y, x),
            spot(g, zz, y, x),
            x_send.at[g, zz],
            x_recv.at[g, zz],
            device(z, y, 1 - x, c),
        )

    def y_copy(g, zz, own):
        return push(
            ins[g] if own else spot(g, zz, y, x),
            spot(g, zz, y, x),
            y_send.at[g, zz],
            y_recv.at[g, zz],
            device(z, 1 - y, x, c),
        )

    def relay(g, zz, half):
        part = halves(shapes[g])[half]
        if half == 0:
            here, target = spot(g, zz, y, 1 - x), device(z, 1 - y, x, c)
        else:
            here, target = spot(g, zz, 1 - y, x), device(z, y, 1 - x, c)
        here = here.at[part]
        return push(here, here, d_send.at[g, zz, half], d_recv.at[g, zz, half], target)

    def diag_arrival(g, zz, half):
        part = halves(shapes[g])[half]
        here = spot(g, zz, 1 - y, 1 - x).at[part]
        return push(
            here, here, d_send.at[g, zz, half], d_recv.at[g, zz, half], device(z, y, x, 1 - c)
        )

    def core_copy(g, zz, mine):
        here = outs[g].at[:, zz, :, :, c if mine else 1 - c]
        return push(here, here, c_send.at[g, zz], c_recv.at[g, zz], device(z, y, x, 1 - c))

    def spread(g, zz, own):
        if own:

            @pl.when(z > 0)
            def _():
                z_copy(g, zz, False, True).start()

            @pl.when(z < planes - 1)
            def _():
                z_copy(g, zz, True, True).start()

        else:

            @pl.when((zz < z) & (z < planes - 1))
            def _():
                z_copy(g, zz, True, False).start()

            @pl.when((zz > z) & (z > 0))
            def _():
                z_copy(g, zz, False, False).start()

        x_copy(g, zz, own).start()
        y_copy(g, zz, own).start()

    if with_pair:
        to_partner = push(
            pair, tile_b, pair_send.at[0], pair_recv.at[0], device(z, y, x, 1 - c)
        )
        to_x = push(pair, tile_c, pair_send.at[1], pair_recv.at[1], device(z, y, 1 - x, c))
        passed_on = push(
            tile_c, tile_d, pair_send.at[2], pair_recv.at[2], device(z, y, x, 1 - c)
        )
        to_partner.start()

        @pl.when(x == 0)
        def _():
            to_x.start()

    items = [(t, g) for t in range(planes) for g in range(n)]
    lag_plane, lag_core = n, 2 * n

    def stage_plane(t, g):
        zz = visit(t, z, planes)
        x_copy(g, zz, False).wait_recv()
        relay(g, zz, 0).start()
        y_copy(g, zz, False).wait_recv()
        relay(g, zz, 1).start()

    def stage_core(t, g):
        zz = visit(t, z, planes)
        if t == 0:
            local[g].wait()
        diag_arrival(g, zz, 0).wait_recv()
        diag_arrival(g, zz, 1).wait_recv()
        core_copy(g, zz, True).start()

    for i in range(len(items) + lag_core):
        if i < len(items):
            t, g = items[i]
            zz = visit(t, z, planes)
            if t > 0:
                z_copy(g, zz, True, False).wait_recv()
            spread(g, zz, t == 0)
        if 0 <= i - lag_plane < len(items):
            stage_plane(*items[i - lag_plane])
        if 0 <= i - lag_core < len(items):
            stage_core(*items[i - lag_core])
    if with_pair:

        @pl.when(x == 1)
        def _():
            to_x.wait_recv()
            passed_on.start()

    for t, g in items:
        zz = visit(t, z, planes)
        core_copy(g, zz, False).wait_recv()
        core_copy(g, zz, True).wait_send()
        x_copy(g, zz, t == 0).wait_send()
        y_copy(g, zz, t == 0).wait_send()
        relay(g, zz, 0).wait_send()
        relay(g, zz, 1).wait_send()
        if t == 0:

            @pl.when(z > 0)
            def _():
                z_copy(g, zz, False, True).wait_send()

            @pl.when(z < planes - 1)
            def _():
                z_copy(g, zz, True, True).wait_send()

        else:

            @pl.when((zz < z) & (z < planes - 1))
            def _():
                z_copy(g, zz, True, False).wait_send()

            @pl.when((zz > z) & (z > 0))
            def _():
                z_copy(g, zz, False, False).wait_send()


    if with_pair:
        to_partner.wait()

        @pl.when(x == 0)
        def _():
            to_x.wait_send()

        @pl.when(x == 1)
        def _():
            passed_on.wait()


def gather(planes, blocks, collective_id, pair=None):
    blocks = [b[None] for b in blocks]
    n = len(blocks)
    shapes = [b.shape for b in blocks]
    dma = pltpu.SemaphoreType.DMA
    extra = [] if pair is None else [pair]
    anywhere = pl.BlockSpec(memory_space=pl.ANY)
    got = pl.pallas_call(
        functools.partial(gather_kernel, planes, shapes, pair is not None),
        out_shape=[
            jax.ShapeDtypeStruct((s[0], planes, 2, 2, 2, s[1], s[2]), b.dtype)
            for s, b in zip(shapes, blocks)
        ]
        + [jax.ShapeDtypeStruct(p.shape, p.dtype) for p in extra * 3],
        in_specs=[anywhere] * (n + len(extra)),
        out_specs=[anywhere] * (n + 3 * len(extra)),
        scratch_shapes=[
            dma((n,)),
            dma((n, planes, 2)),
            dma((n, planes)),
            dma((n, planes)),
            dma((n, planes)),
            dma((n, planes)),
            dma((n, planes)),
            dma((n, planes, 2)),
            dma((n, planes, 2)),
            dma((n, planes)),
            dma((n, planes)),
        ]
        + [dma((3,)), dma((3,))] * len(extra),
        compiler_params=pltpu.CompilerParams(collective_id=collective_id, has_side_effects=True),
        name="weight_gather",
    )(*blocks, *extra)
    full = [g.reshape(planes * 8 * s[1], s[2]) for g, s in zip(got, shapes)]
    return full, got[n:]


def columns(shape, half):
    cut = shape[1] // 2 // 128 * 128
    return pl.ds(0, cut) if half == 0 else pl.ds(cut, shape[1] - cut)


def scatter_kernel(planes, shapes, lags, with_tiles, *refs):
    n = len(shapes)
    parts, refs = refs[:n], refs[n:]
    if with_tiles:
        d_a, d_b, d_c, d_d, cos_table, sin_table = refs[:6]
        refs = refs[6:]
    outs, refs = refs[:n], refs[n:]
    if with_tiles:
        d_key, d_value, first_grad = refs[:3]
        refs = refs[3:]
        mine, chip, from_b, from_d, back, load_sem, tile_send, tile_recv = refs[-8:]
        refs = refs[:-8]
    own, from_core, from_dx, from_dy, from_x, from_y, from_z = (
        refs[k * n : (k + 1) * n] for k in range(7)
    )
    own_sem, c_send, c_recv, d_send, d_recv, x_send, x_recv, y_send, y_recv, z_send, z_recv = refs[
        7 * n :
    ]
    z, y, x, c = position()
    entry_barrier(z, y, x, c, planes)
    items = [(planes - 1 - t, g) for t in range(planes) for g in range(n)]

    def push(src, dst, send, recv, target):
        return pltpu.make_async_remote_copy(
            src_ref=src,
            dst_ref=dst,
            send_sem=send,
            recv_sem=recv,
            device_id=target,
            device_id_type=MESH_ID,
        )

    f32 = jnp.float32

    def add(dst, *srcs):
        total = dst[...].astype(f32)
        for src in srcs:
            total = total + src[...].astype(f32)
        dst[...] = total.astype(dst.dtype)

    def load(g, zz):
        return pltpu.make_async_copy(
            parts[g].at[zz, :, :, c], own[g].at[zz], own_sem.at[g, zz]
        )

    def core_copy(g, zz):
        return push(
            parts[g].at[zz, :, :, 1 - c],
            from_core[g].at[zz],
            c_send.at[g, zz],
            c_recv.at[g, zz],
            device(z, y, x, 1 - c),
        )

    def diag(g, zz, half):
        part = columns(shapes[g], half)
        box = (from_dx if half == 0 else from_dy)[g].at[zz]
        return push(
            own[g].at[zz, 1 - y, 1 - x, :, part],
            box,
            d_send.at[g, zz, half],
            d_recv.at[g, zz, half],
            device(z, y, 1 - x, c) if half == 0 else device(z, 1 - y, x, c),
        )

    def x_copy(g, zz):
        return push(
            own[g].at[zz, y, 1 - x],
            from_x[g].at[zz],
            x_send.at[g, zz],
            x_recv.at[g, zz],
            device(z, y, 1 - x, c),
        )

    def y_copy(g, zz):
        return push(
            own[g].at[zz, 1 - y, x],
            from_y[g].at[zz],
            y_send.at[g, zz],
            y_recv.at[g, zz],
            device(z, 1 - y, x, c),
        )

    def z_copy(g, zz, up):
        slot = zz if up else jnp.where(zz == z - 1, planes, zz)
        return push(
            own[g].at[zz, y, x],
            from_z[g].at[slot],
            z_send.at[g, zz],
            z_recv.at[g, slot],
            device(z + 1 if up else z - 1, y, x, c),
        )

    def z_arrival(g, slot):
        return push(
            from_z[g].at[slot],
            from_z[g].at[slot],
            z_send.at[g, 0],
            z_recv.at[g, slot],
            device(z, y, x, 1 - c),
        )

    if with_tiles:
        partner = device(z, y, x, 1 - c)
        load_mine = pltpu.make_async_copy(d_a, mine, load_sem.at[0])
        load_chip = pltpu.make_async_copy(d_c, chip, load_sem.at[1])
        send_b = push(d_b, from_b, tile_send.at[0], tile_recv.at[0], partner)
        send_d = push(d_d, from_d, tile_send.at[1], tile_recv.at[1], partner)
        send_back = push(
            chip, back, tile_send.at[2], tile_recv.at[2], device(z, y, 1 - x, c)
        )
        rows = mine.shape[2]

        @pl.when(x == 1)
        def _():
            send_d.start()
            load_chip.start()

        send_b.start()
        load_mine.start()

        @pl.when(x == 1)
        def _():
            load_chip.wait()
            send_d.wait_recv()

            @pl.loop(0, mine.shape[0] * mine.shape[1] * rows // 32)
            def _(i):
                kind = lax.div(i, mine.shape[1] * rows // 32)
                seq = lax.rem(lax.div(i, rows // 32), mine.shape[1])
                at = pl.ds(pl.multiple_of(lax.rem(i, rows // 32) * 32, 32), 32)
                add(chip.at[kind, seq, at], from_d.at[kind, seq, at])

            send_back.start()

    for t, g in items:
        zz = visit(t, z, planes)
        core_copy(g, zz).start()
        load(g, zz).start()

    def stage_core(t, g):
        zz = visit(t, z, planes)
        load(g, zz).wait()
        core_copy(g, zz).wait_recv()
        add(own[g].at[zz, 1 - y, 1 - x], from_core[g].at[zz, 1 - y, 1 - x])
        diag(g, zz, 0).start()
        diag(g, zz, 1).start()
        add(own[g].at[zz, y, 1 - x], from_core[g].at[zz, y, 1 - x])
        add(own[g].at[zz, 1 - y, x], from_core[g].at[zz, 1 - y, x])
        add(own[g].at[zz, y, x], from_core[g].at[zz, y, x])

    def stage_plane(t, g):
        zz = visit(t, z, planes)
        diag(g, zz, 0).wait_recv()
        add(own[g].at[zz, 1 - y, x, :, columns(shapes[g], 0)], from_dx[g].at[zz])
        y_copy(g, zz).start()
        diag(g, zz, 1).wait_recv()
        add(own[g].at[zz, y, 1 - x, :, columns(shapes[g], 1)], from_dy[g].at[zz])
        x_copy(g, zz).start()

    def stage_line(t, g):
        zz = visit(t, z, planes)
        x_copy(g, zz).wait_recv()
        y_copy(g, zz).wait_recv()
        here = own[g].at[zz, y, x]
        if t > 0:
            add(here, from_x[g].at[zz], from_y[g].at[zz])
            farther = jnp.where(zz > z, z > 0, z < planes - 1)

            @pl.when(farther)
            def _():
                z_arrival(g, zz).wait_recv()
                add(here, from_z[g].at[zz])

            @pl.when(zz > z)
            def _():
                z_copy(g, zz, True).start()

            @pl.when(zz < z)
            def _():
                z_copy(g, zz, False).start()

        else:
            outs[g][...] = (
                here[...].astype(f32)
                + from_x[g][zz].astype(f32)
                + from_y[g][zz].astype(f32)
            )

            @pl.when(z > 0)
            def _():
                z_arrival(g, zz).wait_recv()
                outs[g][...] += from_z[g][zz].astype(f32)

            @pl.when(z < planes - 1)
            def _():
                z_arrival(g, planes).wait_recv()
                outs[g][...] += from_z[g][planes].astype(f32)

    lag_plane, lag_line = lags
    for i in range(len(items) + lag_line):
        if i < len(items):
            stage_core(*items[i])
        if 0 <= i - lag_plane < len(items):
            stage_plane(*items[i - lag_plane])
        if 0 <= i - lag_line < len(items):
            stage_line(*items[i - lag_line])
    for t, g in items:
        zz = visit(t, z, planes)
        core_copy(g, zz).wait_send()
        diag(g, zz, 0).wait_send()
        diag(g, zz, 1).wait_send()
        x_copy(g, zz).wait_send()
        y_copy(g, zz).wait_send()
        if t > 0:
            z_copy(g, zz, True).wait_send()
    if with_tiles:
        load_mine.wait()
        send_b.wait()

        @pl.when(x == 0)
        def _():
            send_back.wait_recv()

        @pl.when(x == 1)
        def _():
            send_d.wait_send()
            send_back.wait_send()

        @pl.when(x == 1)
        def _():
            back[...] = jnp.zeros_like(back)

        @pl.loop(0, mine.shape[1] * rows // 32)
        def _(i):
            seq = lax.div(i, rows // 32)
            at = pl.ds(pl.multiple_of(lax.rem(i, rows // 32) * 32, 32), 32)
            flat = pl.ds(pl.multiple_of(i * 32, 32), 32)
            cos_rows, sin_rows = cos_table[flat, :], sin_table[flat, :]
            for k in range(mine.shape[3] // 128):
                lanes = pl.ds(k * 128, 128)

                def summed(kind):
                    return (
                        mine[kind, seq, at, lanes].astype(f32)
                        + from_b[kind, seq, at, lanes].astype(f32)
                        + back[kind, seq, at, lanes].astype(f32)
                    )

                d_key[flat, lanes] = turned(summed(0), cos_rows, sin_rows, -1.0).astype(jnp.bfloat16)
                half = 0.5 * summed(1)
                d_value[flat, lanes] = half.astype(jnp.bfloat16)
                first_grad[flat, lanes] = half


def scatter_sum(planes, partials, lags, collective_id, tiles=None, angles=None):
    n = len(partials)
    partials = [
        p.reshape(planes, 2, 2, 2, p.shape[0] // (planes * 8), p.shape[1]) for p in partials
    ]
    shapes = [p.shape[4:] for p in partials]
    types = [p.dtype for p in partials]
    dma = pltpu.SemaphoreType.DMA

    def boxes(lead, half=None):
        out = []
        for s, d in zip(shapes, types):
            cut = s[1] // 2 // 128 * 128
            width = s[1] if half is None else (cut if half == 0 else s[1] - cut)
            out.append(pltpu.VMEM((*lead, s[0], width), d))
        return out

    extra, extra_out, extra_scratch = [], [], []
    if tiles is not None:
        extra = [*tiles, *angles]
        box = tiles[0].shape
        flat = (box[1] * box[2], box[3])
        extra_out = [
            jax.ShapeDtypeStruct(flat, jnp.bfloat16),
            jax.ShapeDtypeStruct(flat, jnp.bfloat16),
            jax.ShapeDtypeStruct(flat, jnp.float32),
        ]
        extra_scratch = [pltpu.VMEM(box, jnp.bfloat16)] * 5 + [dma((2,)), dma((3,)), dma((3,))]
    return pl.pallas_call(
        functools.partial(scatter_kernel, planes, shapes, lags, bool(extra)),
        out_shape=[jax.ShapeDtypeStruct(s, jnp.float32) for s in shapes] + extra_out,
        in_specs=[pl.BlockSpec(memory_space=pl.ANY)] * (n + len(extra[:4]))
        + [pl.BlockSpec(memory_space=pltpu.VMEM)] * len(extra[4:]),
        out_specs=[pl.BlockSpec(memory_space=pltpu.VMEM)] * (n + len(extra_out)),
        scratch_shapes=[
            *boxes((planes, 2, 2)),
            *boxes((planes, 2, 2)),
            *boxes((planes,), 0),
            *boxes((planes,), 1),
            *boxes((planes,)),
            *boxes((planes,)),
            *boxes((planes + 1,)),
            dma((n, planes)),
            dma((n, planes)),
            dma((n, planes)),
            dma((n, planes, 2)),
            dma((n, planes, 2)),
            dma((n, planes)),
            dma((n, planes)),
            dma((n, planes)),
            dma((n, planes)),
            dma((n, planes)),
            dma((n, planes + 1)),
            *extra_scratch,
        ],
        compiler_params=pltpu.CompilerParams(
            collective_id=collective_id, has_side_effects=True, vmem_limit_bytes=62 * 2**20
        ),
        name="gradient_scatter",
    )(*partials, *extra)


def on_device(
    planes,
    tokens,
    first_values,
    cotangent,
    segment_ids,
    attn_gain,
    w_query,
    w_key,
    w_value,
    w_out,
    ffn_gain,
    gate_weight,
    up_weight,
    down_weight,
):
    f32, bf16 = jnp.float32, jnp.bfloat16
    devices = planes * 8
    seqs, rows, width = tokens.shape
    rank = lax.axis_index("ctx")
    share = attn_gain.shape[0]
    gains = jnp.zeros((16, 128), bf16)
    gains = gains.at[0, :share].set(attn_gain).at[1, :share].set(ffn_gain)
    (gains, w_query, w_key, w_value), _ = gather(planes, [gains, w_query, w_key, w_value], 0)
    gains = gains.reshape(devices, 16, 128)
    attn_gain = gains[:, 0, :share].reshape(1, width)
    ffn_gain = gains[:, 1, :share].reshape(1, width)
    starts, cos_table, sin_table = tables(segment_ids, rank, rows)
    flat = (seqs * rows, width)
    local = (seqs, rows, width)
    tokens = tokens.reshape(flat)
    mm = functools.partial(jnp.dot, preferred_element_type=f32)
    by_rows = lambda a, b: lax.dot_general(a, b, TN, preferred_element_type=f32).astype(bf16)
    back = lambda a, b: lax.dot_general(a, b, NT, preferred_element_type=f32)
    normed_one, query_rot, pair = project(
        tokens, first_values.reshape(flat), attn_gain, w_query, w_key, w_value, cos_table, sin_table
    )
    query_rot = query_rot.reshape(local)
    pair = pair.reshape(2, *local)
    (w_out, gate_weight, up_weight, down_weight, pair), _ = lax.optimization_barrier(
        ((w_out, gate_weight, up_weight, down_weight, pair), normed_one)
    )
    (w_out, gate_weight, up_weight, down_weight), others = gather(
        planes, [w_out, gate_weight, up_weight, down_weight], 1, pair
    )
    tiles = [pair, *others]
    context3, log_total = attend(starts, query_rot, tiles)
    context = context3.reshape(flat)
    tokens_float = tokens.astype(f32)
    scale_one = inverse_rms(tokens_float)
    cotangent = cotangent.reshape(flat)
    residual = tokens_float + mm(context, w_out)
    scale_two = inverse_rms(residual)
    second_normed = (residual * scale_two * ffn_gain.astype(f32)).astype(bf16)
    gate = mm(second_normed, gate_weight)
    up = mm(second_normed, up_weight)
    hidden = (swish(gate) * up).astype(bf16)
    output = (residual + mm(hidden, down_weight)).astype(bf16)

    out_float = cotangent.astype(f32)
    d_down = by_rows(hidden, cotangent)
    d_hidden = back(cotangent, down_weight)
    sigmoid_gate = jax.nn.sigmoid(gate)
    d_gate = (d_hidden * up * sigmoid_gate * (1.0 + gate * (1.0 - sigmoid_gate))).astype(bf16)
    d_up = (d_hidden * (gate * sigmoid_gate)).astype(bf16)
    d_gate_weight = by_rows(second_normed, d_gate)
    d_up_weight = by_rows(second_normed, d_up)
    d_normed_two = back(d_gate, gate_weight) + back(d_up, up_weight)
    d_ffn_gain = jnp.sum(d_normed_two * residual * scale_two, axis=0)
    weighted_two = d_normed_two * ffn_gain.astype(f32)
    d_residual = (
        out_float
        + scale_two * weighted_two
        - residual
        * (scale_two * scale_two * scale_two)
        * jnp.mean(weighted_two * residual, axis=-1, keepdims=True)
    )
    d_residual_low = d_residual.astype(bf16)
    d_out = by_rows(context, d_residual_low)
    d_context = back(d_residual_low, w_out).astype(bf16).reshape(local)
    d_query, *d_tiles = attend_back(
        starts, query_rot, tiles, context3, d_context, log_total, cos_table, sin_table
    )
    d_query = d_query.reshape(flat)
    s_down, s_gate, s_up, s_out, d_key, d_value, first_grad = scatter_sum(
        planes, [d_down, d_gate_weight, d_up_weight, d_out], (4, 8), 2, d_tiles, (cos_table, sin_table)
    )
    d_wq = by_rows(normed_one, d_query)
    d_wk = by_rows(normed_one, d_key)
    d_wv = by_rows(normed_one, d_value)
    d_normed_one = back(d_query, w_query) + back(d_key, w_key) + back(d_value, w_value)
    d_attn_gain = jnp.sum(d_normed_one * tokens_float * scale_one, axis=0)
    weighted_one = d_normed_one * attn_gain.astype(f32)
    token_grad = (
        d_residual
        + scale_one * weighted_one
        - tokens_float
        * (scale_one * scale_one * scale_one)
        * jnp.mean(weighted_one * tokens_float, axis=-1, keepdims=True)
    )
    d_gains = jnp.stack([d_attn_gain, d_ffn_gain]).reshape(2, devices, share)
    d_gains = jnp.zeros((devices, 8, 256), f32).at[:, :2, :share].set(d_gains.transpose(1, 0, 2))
    s_wq, s_wk, s_wv, s_gains = scatter_sum(
        planes, [d_wq, d_wk, d_wv, d_gains.reshape(devices * 8, 256)], (4, 8), 3
    )
    return (
        output.reshape(local),
        token_grad.reshape(local),
        first_grad.reshape(local),
        s_gains[0, :share],
        s_wq,
        s_wk,
        s_wv,
        s_out,
        s_gains[1, :share],
        s_gate,
        s_up,
        s_down,
    )


def solution(mesh):
    token, weight, vector = P("dp", "ctx", None), P(("dp", "ctx"), None), P(("dp", "ctx"))
    return jax.shard_map(
        functools.partial(on_device, mesh.shape["dp"] // 2),
        mesh=mesh,
        in_specs=(
            token,
            token,
            token,
            P("dp", None),
            vector,
            weight,
            weight,
            weight,
            weight,
            vector,
            weight,
            weight,
            weight,
        ),
        out_specs=(
            token,
            token,
            token,
            vector,
            weight,
            weight,
            weight,
            weight,
            vector,
            weight,
            weight,
            weight,
        ),
        check_vma=False,
    )
```

```python
import functools
import jax
import jax.numpy as jnp
from jax import lax
from jax.experimental import pallas as pl
from jax.experimental.pallas import tpu as pltpu
from jax.sharding import PartitionSpec as P

HEADS = 16
HEAD_DIM = 64
MESH_ID = pl.DeviceIdType.MESH

epsilon = 1e-05
rope_base = 10000.0
score_scale = 0.125
masked_score = -1e30


def inverse_rms(values):
    return lax.rsqrt(jnp.mean(values * values, axis=-1, keepdims=True) + epsilon)


def swish(values):
    return values * jax.nn.sigmoid(values)


def first_half(shape):
    return lax.broadcasted_iota(jnp.int32, shape, len(shape) - 1) % HEAD_DIM < HEAD_DIM // 2


def swap_halves(values):
    return jnp.where(
        first_half(values.shape), pltpu.roll(values, 96, 1), pltpu.roll(values, 32, 1)
    )


def turned(values, cos_table, sin_table, sign):
    return values * cos_table + sign * (swap_halves(values) * sin_table)


def tables(segment_ids, rank, rows):
    seqs, length = segment_ids.shape
    places = jnp.arange(length, dtype=jnp.int32)
    edges = jnp.concatenate(
        [jnp.ones((seqs, 1), dtype=jnp.bool_), segment_ids[:, 1:] != segment_ids[:, :-1]], axis=1
    )
    starts = lax.cummax(jnp.where(edges, places[None, :], 0), axis=1)
    starts = lax.dynamic_slice_in_dim(starts, rank * rows, rows, 1)
    local = rank * rows + jnp.arange(rows, dtype=jnp.int32) - starts
    lane = jnp.arange(128, dtype=jnp.int32)
    half = HEAD_DIM // 2
    frequency = rope_base ** (-(lane % half).astype(jnp.float32) * 2.0 / HEAD_DIM)
    angles = local.astype(jnp.float32).reshape(seqs * rows, 1) * frequency
    sign = jnp.where(lane % HEAD_DIM < half, -1.0, 1.0)
    return starts.reshape(seqs, 1, rows), jnp.cos(angles), jnp.sin(angles) * sign


def project_kernel(tok, first, gain, wq, wk, wv, cos_ref, sin_ref, normed, query, pair):
    f32, bf16 = jnp.float32, jnp.bfloat16

    @pl.when(pl.program_id(0) == 0)
    def _():
        values = tok[...].astype(f32)
        normed[...] = (values * inverse_rms(values) * gain[...].astype(f32)).astype(bf16)

    n1 = normed[...]
    cos_table, sin_table = cos_ref[...], sin_ref[...]
    queries = jnp.dot(n1, wq[...], preferred_element_type=f32)
    keys = jnp.dot(n1, wk[...], preferred_element_type=f32)
    values = jnp.dot(n1, wv[...], preferred_element_type=f32)
    for i in range(queries.shape[1] // 128):
        lanes = slice(i * 128, i * 128 + 128)
        query[:, lanes] = turned(queries[:, lanes], cos_table, sin_table, 1.0).astype(bf16)
        pair[0, :, lanes] = turned(keys[:, lanes], cos_table, sin_table, 1.0).astype(bf16)
    pair[1] = (0.5 * values + 0.5 * first[...].astype(f32)).astype(bf16)


def project(tok, first, gain, wq, wk, wv, cos_table, sin_table):
    rows, width = tok.shape
    tile = 256
    whole = lambda i: (0, 0)
    column = lambda i: (0, i)
    wide = lambda: pl.BlockSpec((width, tile), column)
    return pl.pallas_call(
        project_kernel,
        grid=(width // tile,),
        in_specs=[
            pl.BlockSpec((rows, width), whole),
            pl.BlockSpec((rows, tile), column),
            pl.BlockSpec((1, width), whole),
            wide(),
            wide(),
            wide(),
            pl.BlockSpec((rows, 128), whole),
            pl.BlockSpec((rows, 128), whole),
        ],
        out_specs=[
            pl.BlockSpec((rows, width), whole),
            pl.BlockSpec((rows, tile), column),
            pl.BlockSpec((2, rows, tile), lambda i: (0, 0, i)),
        ],
        out_shape=[
            jax.ShapeDtypeStruct((rows, width), jnp.bfloat16),
            jax.ShapeDtypeStruct((rows, width), jnp.bfloat16),
            jax.ShapeDtypeStruct((2, rows, width), jnp.bfloat16),
        ],
        name="project",
    )(tok, first, gain, wq, wk, wv, cos_table, sin_table)


def two_heads(block, scale):
    lane = lax.broadcasted_iota(jnp.int32, block.shape, 1)
    scaled = block * jnp.asarray(scale, block.dtype)
    zero = jnp.zeros_like(block)
    return jnp.concatenate(
        [jnp.where(lane < HEAD_DIM, scaled, zero), jnp.where(lane < HEAD_DIM, zero, scaled)]
    )


def own_lanes(both):
    rows = both.shape[1] // 2
    lane = lax.broadcasted_iota(jnp.int32, (both.shape[0], rows), 0)
    return jnp.where(lane < HEAD_DIM, both[:, :rows], both[:, rows:]).T


def fill_bias(bias, starts, rank):
    rows = bias.shape[1]
    key = lax.broadcasted_iota(jnp.int32, (rows, rows), 0)
    place = rank * rows + lax.broadcasted_iota(jnp.int32, (rows, rows), 1)
    begin = starts[...]
    for t in range(4):
        x, c = lax.div(rank, 2), lax.rem(rank, 2)
        owner = (1 - x if t >= 2 else x) * 2 + (1 - c if t % 2 else c)
        at = owner * rows + key
        bias[t] = jnp.where((at >= begin) & (at <= place), 0.0, masked_score)


NT = (((1,), (1,)), ((), ()))
TN = (((0,), (0,)), ((), ()))


def attend_step(rank, begin, starts, q, tiles, out, log_total, bias, scores, peak, total, acc):
    f32, bf16 = jnp.float32, jnp.bfloat16

    @pl.when(begin)
    def _():
        fill_bias(bias, starts, rank)

    high = rank >= 2
    stacked = two_heads(q, score_scale)

    def score(t):
        s = lax.dot_general(tiles[t][0][...], stacked, NT, preferred_element_type=f32)
        s = s + jnp.concatenate([bias[t], bias[t]], axis=1)
        scores[t] = s
        return jnp.max(s, axis=0, keepdims=True)

    def gather_values(t, top):
        e = jnp.exp(scores[t] - top)
        part = lax.dot_general(tiles[t][1][...], e.astype(bf16), TN, preferred_element_type=f32)
        return jnp.sum(e, axis=0, keepdims=True), part

    peak[...] = jnp.maximum(score(0), score(1))

    @pl.when(high)
    def _():
        peak[...] = jnp.maximum(peak[...], jnp.maximum(score(2), score(3)))

    top = peak[...]
    sum_a, acc_a = gather_values(0, top)
    sum_b, acc_b = gather_values(1, top)
    total[...] = sum_a + sum_b
    acc[...] = acc_a + acc_b

    @pl.when(high)
    def _():
        top = peak[...]
        sum_a, acc_a = gather_values(2, top)
        sum_b, acc_b = gather_values(3, top)
        total[...] += sum_a + sum_b
        acc[...] += acc_a + acc_b

    out[...] = own_lanes(acc[...] / total[...]).astype(bf16)
    log_total[...] = peak[...] + jnp.log(total[...])


def attend_scratch(rows):
    return [
        pltpu.VMEM((4, rows, rows), jnp.float32),
        pltpu.VMEM((4, rows, 2 * rows), jnp.float32),
        pltpu.VMEM((1, 2 * rows), jnp.float32),
        pltpu.VMEM((1, 2 * rows), jnp.float32),
        pltpu.VMEM((128, 2 * rows), jnp.float32),
    ]


def attend_kernel(starts, q, tile_a, tile_b, tile_c, tile_d, out, log_total, *scratch):
    attend_step(
        lax.axis_index("ctx"),
        pl.program_id(1) == 0,
        starts.at[0],
        q[0],
        [[t.at[0, 0], t.at[1, 0]] for t in (tile_a, tile_b, tile_c, tile_d)],
        out.at[0],
        log_total.at[0, 0],
        *scratch,
    )


def attend(starts, q, tiles):
    seqs, rows, width = q.shape
    pairs = width // 128
    block = lambda: pl.BlockSpec((1, rows, 128), lambda s, p: (s, 0, p))
    tile = lambda: pl.BlockSpec((2, 1, rows, 128), lambda s, p: (0, s, 0, p))
    return pl.pallas_call(
        attend_kernel,
        grid=(seqs, pairs),
        in_specs=[
            pl.BlockSpec((1, 1, rows), lambda s, p: (s, 0, 0)),
            block(),
            tile(),
            tile(),
            tile(),
            tile(),
        ],
        out_specs=[block(), pl.BlockSpec((1, 1, 1, 2 * rows), lambda s, p: (s, p, 0, 0))],
        out_shape=[
            jax.ShapeDtypeStruct(q.shape, jnp.bfloat16),
            jax.ShapeDtypeStruct((seqs, pairs, 1, 2 * rows), jnp.float32),
        ],
        scratch_shapes=attend_scratch(rows),
        name="attend",
    )(starts, q, *tiles)


def attend_back_step(
    rank, begin, starts, q, tiles, context, d_context, log_total, cos_t, sin_t, d_q, d_tiles, bias, acc
):
    f32, bf16 = jnp.float32, jnp.bfloat16

    @pl.when(begin)
    def _():
        fill_bias(bias, starts, rank)

    high = rank >= 2
    stacked = two_heads(q, score_scale)
    stacked_do = two_heads(d_context, 1.0)
    turned_product = (d_context.astype(f32) * context.astype(f32)).T
    delta = jnp.concatenate(
        [
            jnp.sum(turned_product[:HEAD_DIM], axis=0, keepdims=True),
            jnp.sum(turned_product[HEAD_DIM:], axis=0, keepdims=True),
        ],
        axis=1,
    )
    lse = log_total[...]

    def one(t):
        keys, values = tiles[t][0][...], tiles[t][1][...]
        s = lax.dot_general(keys, stacked, NT, preferred_element_type=f32)
        s = s + jnp.concatenate([bias[t], bias[t]], axis=1)
        p = jnp.exp(s - lse)
        dp = lax.dot_general(values, stacked_do, NT, preferred_element_type=f32)
        ds = (p * (dp - delta)).astype(bf16)
        d_tiles[t][1][...] = jnp.dot(p.astype(bf16), stacked_do, preferred_element_type=f32).astype(bf16)
        d_tiles[t][0][...] = jnp.dot(ds, stacked, preferred_element_type=f32).astype(bf16)
        return lax.dot_general(keys, ds, TN, preferred_element_type=f32)

    acc[...] = one(0) + one(1)

    @pl.when(high)
    def _():
        acc[...] += one(2) + one(3)

    d_q[...] = turned(own_lanes(acc[...]) * score_scale, cos_t[...], sin_t[...], -1.0).astype(bf16)


def attend_back_scratch(rows):
    return [pltpu.VMEM((4, rows, rows), jnp.float32), pltpu.VMEM((128, 2 * rows), jnp.float32)]


def position():
    dp = lax.axis_index("dp")
    ct = lax.axis_index("ctx")
    return lax.div(dp, 2), lax.rem(dp, 2), lax.div(ct, 2), lax.rem(ct, 2)


def visit(step, z, planes):
    back = planes - 1 - step
    high = back + jnp.where(back >= z, 1, 0)
    low = planes - 1 - back
    low = low - jnp.where(low <= z, 1, 0)
    other = jnp.where(z < planes // 2, low, high)
    return jnp.where(step == 0, z, other)


def device(z, y, x, c):
    return (z * 2 + y, x * 2 + c)


def halves(shape):
    if shape[0] % 2 == 0:
        cut = shape[0] // 2
        return (pl.ds(0, cut), slice(None), slice(None)), (pl.ds(cut, cut), slice(None), slice(None))
    cut = shape[2] // 2 // 128 * 128
    return (
        (slice(None), slice(None), pl.ds(0, cut)),
        (slice(None), slice(None), pl.ds(cut, shape[2] - cut)),
    )


def entry_barrier(z, y, x, c, planes):
    barrier = pltpu.get_barrier_semaphore()

    def hello(target):
        pl.semaphore_signal(barrier, inc=1, device_id=target, device_id_type=MESH_ID)

    hello(device(z, y, 1 - x, c))
    hello(device(z, 1 - y, x, c))
    hello(device(z, y, x, 1 - c))

    @pl.when(z > 0)
    def _():
        hello(device(z - 1, y, x, c))

    @pl.when(z < planes - 1)
    def _():
        hello(device(z + 1, y, x, c))

    pl.semaphore_wait(barrier, 3 + jnp.where(z > 0, 1, 0) + jnp.where(z < planes - 1, 1, 0))


def gather_kernel(planes, shapes, with_pair, *refs):
    n = len(shapes)
    ins, refs = refs[:n], refs[n:]
    if with_pair:
        pair, refs = refs[0], refs[1:]
    outs, refs = refs[:n], refs[n:]
    if with_pair:
        tile_b, tile_c, tile_d = refs[:3]
        refs = refs[3:]
        pair_send, pair_recv = refs[-2:]
        refs = refs[:-2]
    sems = refs
    own_sem, z_send, z_recv, x_send, x_recv, y_send, y_recv, d_send, d_recv, c_send, c_recv = sems
    z, y, x, c = position()
    entry_barrier(z, y, x, c, planes)
    local = [
        pltpu.make_async_copy(ins[g], outs[g].at[:, z, y, x, c], own_sem.at[g]) for g in range(n)
    ]
    for copy in local:
        copy.start()

    def push(src, dst, send, recv, target):
        return pltpu.make_async_remote_copy(
            src_ref=src,
            dst_ref=dst,
            send_sem=send,
            recv_sem=recv,
            device_id=target,
            device_id_type=MESH_ID,
        )

    def spot(g, zz, yy, xx):
        return outs[g].at[:, zz, yy, xx, c]

    def z_copy(g, zz, up, own):
        side = 1 if up else 0
        return push(
            ins[g] if own else spot(g, zz, y, x),
            spot(g, zz, y, x),
            z_send.at[g, zz, side],
            z_recv.at[g, zz],
            device(z + 1 if up else z - 1, y, x, c),
        )

    def x_copy(g, zz, own):
        return push(
            ins[g] if own else spot(g, zz, y, x),
            spot(g, zz, y, x),
            x_send.at[g, zz],
            x_recv.at[g, zz],
            device(z, y, 1 - x, c),
        )

    def y_copy(g, zz, own):
        return push(
            ins[g] if own else spot(g, zz, y, x),
            spot(g, zz, y, x),
            y_send.at[g, zz],
            y_recv.at[g, zz],
            device(z, 1 - y, x, c),
        )

    def relay(g, zz, half):
        part = halves(shapes[g])[half]
        if half == 0:
            here, target = spot(g, zz, y, 1 - x), device(z, 1 - y, x, c)
        else:
            here, target = spot(g, zz, 1 - y, x), device(z, y, 1 - x, c)
        here = here.at[part]
        return push(here, here, d_send.at[g, zz, half], d_recv.at[g, zz, half], target)

    def diag_arrival(g, zz, half):
        part = halves(shapes[g])[half]
        here = spot(g, zz, 1 - y, 1 - x).at[part]
        return push(
            here, here, d_send.at[g, zz, half], d_recv.at[g, zz, half], device(z, y, x, 1 - c)
        )

    def core_copy(g, zz, mine):
        here = outs[g].at[:, zz, :, :, c if mine else 1 - c]
        return push(here, here, c_send.at[g, zz], c_recv.at[g, zz], device(z, y, x, 1 - c))

    def spread(g, zz, own):
        if own:

            @pl.when(z > 0)
            def _():
                z_copy(g, zz, False, True).start()

            @pl.when(z < planes - 1)
            def _():
                z_copy(g, zz, True, True).start()

        else:

            @pl.when((zz < z) & (z < planes - 1))
            def _():
                z_copy(g, zz, True, False).start()

            @pl.when((zz > z) & (z > 0))
            def _():
                z_copy(g, zz, False, False).start()

        x_copy(g, zz, own).start()
        y_copy(g, zz, own).start()

    if with_pair:
        to_partner = push(
            pair, tile_b, pair_send.at[0], pair_recv.at[0], device(z, y, x, 1 - c)
        )
        to_x = push(pair, tile_c, pair_send.at[1], pair_recv.at[1], device(z, y, 1 - x, c))
        passed_on = push(
            tile_c, tile_d, pair_send.at[2], pair_recv.at[2], device(z, y, x, 1 - c)
        )
        to_partner.start()

        @pl.when(x == 0)
        def _():
            to_x.start()

    items = [(t, g) for t in range(planes) for g in range(n)]
    lag_plane, lag_core = n, 2 * n

    def stage_plane(t, g):
        zz = visit(t, z, planes)
        x_copy(g, zz, False).wait_recv()
        relay(g, zz, 0).start()
        y_copy(g, zz, False).wait_recv()
        relay(g, zz, 1).start()

    def stage_core(t, g):
        zz = visit(t, z, planes)
        if t == 0:
            local[g].wait()
        diag_arrival(g, zz, 0).wait_recv()
        diag_arrival(g, zz, 1).wait_recv()
        core_copy(g, zz, True).start()

    for i in range(len(items) + lag_core):
        if i < len(items):
            t, g = items[i]
            zz = visit(t, z, planes)
            if t > 0:
                z_copy(g, zz, True, False).wait_recv()
            spread(g, zz, t == 0)
        if 0 <= i - lag_plane < len(items):
            stage_plane(*items[i - lag_plane])
        if 0 <= i - lag_core < len(items):
            stage_core(*items[i - lag_core])
    if with_pair:

        @pl.when(x == 1)
        def _():
            to_x.wait_recv()
            passed_on.start()

    for t, g in items:
        zz = visit(t, z, planes)
        core_copy(g, zz, False).wait_recv()
        core_copy(g, zz, True).wait_send()
        x_copy(g, zz, t == 0).wait_send()
        y_copy(g, zz, t == 0).wait_send()
        relay(g, zz, 0).wait_send()
        relay(g, zz, 1).wait_send()
        if t == 0:

            @pl.when(z > 0)
            def _():
                z_copy(g, zz, False, True).wait_send()

            @pl.when(z < planes - 1)
            def _():
                z_copy(g, zz, True, True).wait_send()

        else:

            @pl.when((zz < z) & (z < planes - 1))
            def _():
                z_copy(g, zz, True, False).wait_send()

            @pl.when((zz > z) & (z > 0))
            def _():
                z_copy(g, zz, False, False).wait_send()


    if with_pair:
        to_partner.wait()

        @pl.when(x == 0)
        def _():
            to_x.wait_send()

        @pl.when(x == 1)
        def _():
            passed_on.wait()


def gather(planes, blocks, collective_id, pair=None):
    blocks = [b[None] for b in blocks]
    n = len(blocks)
    shapes = [b.shape for b in blocks]
    dma = pltpu.SemaphoreType.DMA
    extra = [] if pair is None else [pair]
    anywhere = pl.BlockSpec(memory_space=pl.ANY)
    got = pl.pallas_call(
        functools.partial(gather_kernel, planes, shapes, pair is not None),
        out_shape=[
            jax.ShapeDtypeStruct((s[0], planes, 2, 2, 2, s[1], s[2]), b.dtype)
            for s, b in zip(shapes, blocks)
        ]
        + [jax.ShapeDtypeStruct(p.shape, p.dtype) for p in extra * 3],
        in_specs=[anywhere] * (n + len(extra)),
        out_specs=[anywhere] * (n + 3 * len(extra)),
        scratch_shapes=[
            dma((n,)),
            dma((n, planes, 2)),
            dma((n, planes)),
            dma((n, planes)),
            dma((n, planes)),
            dma((n, planes)),
            dma((n, planes)),
            dma((n, planes, 2)),
            dma((n, planes, 2)),
            dma((n, planes)),
            dma((n, planes)),
        ]
        + [dma((3,)), dma((3,))] * len(extra),
        compiler_params=pltpu.CompilerParams(collective_id=collective_id, has_side_effects=True),
        name="weight_gather",
    )(*blocks, *extra)
    full = [g.reshape(planes * 8 * s[1], s[2]) for g, s in zip(got, shapes)]
    return full, got[n:]


def columns(shape, half):
    cut = shape[1] // 2 // 128 * 128
    return pl.ds(0, cut) if half == 0 else pl.ds(cut, shape[1] - cut)


def scatter_kernel(planes, shapes, with_tiles, *refs):
    n = len(shapes)
    parts, refs = refs[:n], refs[n:]
    if with_tiles:
        starts, query, *tiles, context, d_context, log_total, cos_table, sin_table = refs[:11]
        refs = refs[11:]
    outs, refs = refs[:n], refs[n:]
    if with_tiles:
        d_query, d_key, d_value, first_grad = refs[:4]
        refs = refs[4:]
        mine, near, chip, far, from_b, from_d, tile_send, tile_recv, bias, acc = refs[-10:]
        refs = refs[:-10]
    own, from_core, from_dx, from_dy, from_x, from_y, from_z = (
        refs[k * n : (k + 1) * n] for k in range(7)
    )
    own_sem, c_send, c_recv, d_send, d_recv, x_send, x_recv, y_send, y_recv, z_send, z_recv = refs[
        7 * n :
    ]
    z, y, x, c = position()
    entry_barrier(z, y, x, c, planes)

    def push(src, dst, send, recv, target):
        return pltpu.make_async_remote_copy(
            src_ref=src,
            dst_ref=dst,
            send_sem=send,
            recv_sem=recv,
            device_id=target,
            device_id_type=MESH_ID,
        )

    f32 = jnp.float32

    def add(dst, *srcs):
        total = dst[...].astype(f32)
        for src in srcs:
            total = total + src[...].astype(f32)
        dst[...] = total.astype(dst.dtype)

    def load(g, zz):
        return pltpu.make_async_copy(
            parts[g].at[zz, :, :, c], own[g].at[zz], own_sem.at[g, zz]
        )

    def core_copy(g, zz):
        return push(
            parts[g].at[zz, :, :, 1 - c],
            from_core[g].at[zz],
            c_send.at[g, zz],
            c_recv.at[g, zz],
            device(z, y, x, 1 - c),
        )

    def diag_x(g, zz):
        return push(
            own[g].at[zz, 1 - y, 1 - x, :, columns(shapes[g], 0)],
            from_dx[g].at[zz],
            d_send.at[g, zz, 0],
            d_recv.at[g, zz, 0],
            device(z, y, 1 - x, c),
        )

    def diag_y(g, zz, full):
        part = slice(None) if full else columns(shapes[g], 1)
        return push(
            own[g].at[zz, 1 - y, 1 - x, :, part],
            from_dy[g].at[zz, :, part],
            d_send.at[g, zz, 1],
            d_recv.at[g, zz, 1],
            device(z, 1 - y, x, c),
        )

    def x_copy(g, zz):
        return push(
            own[g].at[zz, y, 1 - x],
            from_x[g].at[zz],
            x_send.at[g, zz],
            x_recv.at[g, zz],
            device(z, y, 1 - x, c),
        )

    def y_copy(g, zz):
        return push(
            own[g].at[zz, 1 - y, x],
            from_y[g].at[zz],
            y_send.at[g, zz],
            y_recv.at[g, zz],
            device(z, 1 - y, x, c),
        )

    def z_copy(g, zz, up):
        slot = zz if up else jnp.where(zz == z - 1, planes, zz)
        return push(
            own[g].at[zz, y, x],
            from_z[g].at[slot],
            z_send.at[g, zz],
            z_recv.at[g, slot],
            device(z + 1 if up else z - 1, y, x, c),
        )

    def z_arrival(g, slot):
        return push(
            from_z[g].at[slot],
            from_z[g].at[slot],
            z_send.at[g, 0],
            z_recv.at[g, slot],
            device(z, y, x, 1 - c),
        )

    def lean_or_even(lean, even):
        if not with_tiles:
            even()
            return
        pl.when(x == 0)(even)
        pl.when(x == 1)(lean)

    if with_tiles:
        partner = device(z, y, x, 1 - c)
        seqs, rows = mine.shape[1:3]
        pairs = mine.shape[3] // 128

        def send_b(s):
            return push(
                near.at[:, s], from_b.at[:, s], tile_send.at[0, s], tile_recv.at[0, s], partner
            )

        def send_d(s):
            return push(
                far.at[:, s], from_d.at[:, s], tile_send.at[1, s], tile_recv.at[1, s], partner
            )

        def send_back(s):
            return push(
                chip.at[:, s],
                chip.at[:, s],
                tile_send.at[2, s],
                tile_recv.at[2, s],
                device(z, y, 1 - x, c),
            )

        def unit(u):
            s, p = lax.div(u, pairs), lax.rem(u, pairs)
            lanes = pl.ds(pl.multiple_of(p * 128, 128), 128)
            flat = pl.ds(pl.multiple_of(s * rows, rows), rows)
            two = lambda ref: [ref.at[0, s, :, lanes], ref.at[1, s, :, lanes]]
            attend_back_step(
                lax.axis_index("ctx"),
                p == 0,
                starts.at[s],
                query[s, :, lanes],
                [two(t) for t in tiles],
                context[s, :, lanes],
                d_context[s, :, lanes],
                log_total.at[s, p],
                cos_table.at[flat],
                sin_table.at[flat],
                d_query.at[s, :, lanes],
                [two(t) for t in (mine, near, chip, far)],
                bias,
                acc,
            )

        def work(i):
            each = seqs * pairs // 4

            @pl.when(i < 4)
            def _():
                @pl.loop(0, each)
                def _(j):
                    unit(i * each + j)

            @pl.when((i == 1) | (i == 3))
            def _():
                s = lax.div(i, 2)
                send_b(s).start()

                @pl.when(x == 1)
                def _():
                    send_d(s).start()

            @pl.when(((i == 2) | (i == 4)) & (x == 1))
            def _():
                s = lax.div(i, 2) - 1
                send_d(s).wait_recv()
                for kind in range(2):

                    @pl.loop(0, rows // 32)
                    def _(j):
                        at = pl.ds(pl.multiple_of(j * 32, 32), 32)
                        add(chip.at[kind, s, at], from_d.at[kind, s, at])

                send_back(s).start()

    @pl.loop(0, planes)
    def _(r):
        zz = visit(planes - 1 - r, z, planes)
        for g in range(n):
            core_copy(g, zz).start()
            load(g, zz).start()

    def stage_core(g, t):
        zz = visit(t, z, planes)
        load(g, zz).wait()
        core_copy(g, zz).wait_recv()
        add(own[g].at[zz, 1 - y, 1 - x], from_core[g].at[zz, 1 - y, 1 - x])

        def even():
            diag_x(g, zz).start()
            diag_y(g, zz, False).start()

        lean_or_even(lambda: diag_y(g, zz, True).start(), even)
        add(own[g].at[zz, 1 - y, x], from_core[g].at[zz, 1 - y, x])
        if with_tiles:

            @pl.when(x == 0)
            def _():
                y_copy(g, zz).start()

        add(own[g].at[zz, y, 1 - x], from_core[g].at[zz, y, 1 - x])
        add(own[g].at[zz, y, x], from_core[g].at[zz, y, x])

    def stage_plane(g, t):
        zz = visit(t, z, planes)

        def take_x():
            diag_x(g, zz).wait_recv()
            add(own[g].at[zz, 1 - y, x, :, columns(shapes[g], 0)], from_dx[g].at[zz])
            y_copy(g, zz).start()

        def take_y(full):
            part = slice(None) if full else columns(shapes[g], 1)
            diag_y(g, zz, full).wait_recv()
            add(own[g].at[zz, y, 1 - x, :, part], from_dy[g].at[zz, :, part])
            x_copy(g, zz).start()

        if not with_tiles:
            take_x()
            take_y(False)
            return

        @pl.when(x == 0)
        def _():
            take_y(False)

        @pl.when(x == 1)
        def _():
            take_x()
            take_y(True)

    def stage_line(g, t):
        zz = visit(t, z, planes)
        x_copy(g, zz).wait_recv()
        y_copy(g, zz).wait_recv()
        here = own[g].at[zz, y, x]

        @pl.when(t > 0)
        def _():
            add(here, from_x[g].at[zz], from_y[g].at[zz])
            farther = jnp.where(zz > z, z > 0, z < planes - 1)

            @pl.when(farther)
            def _():
                z_arrival(g, zz).wait_recv()
                add(here, from_z[g].at[zz])

            @pl.when(zz > z)
            def _():
                z_copy(g, zz, True).start()

            @pl.when(zz < z)
            def _():
                z_copy(g, zz, False).start()

        @pl.when(t == 0)
        def _():
            outs[g][...] = (
                here[...].astype(f32)
                + from_x[g][zz].astype(f32)
                + from_y[g][zz].astype(f32)
            )

            @pl.when(z > 0)
            def _():
                z_arrival(g, zz).wait_recv()
                outs[g][...] += from_z[g][zz].astype(f32)

            @pl.when(z < planes - 1)
            def _():
                z_arrival(g, planes).wait_recv()
                outs[g][...] += from_z[g][planes].astype(f32)

    @pl.loop(0, planes + 2)
    def _(r):
        t = planes - 1 - r
        for g in range(n):

            @pl.when(r < planes)
            def _():
                stage_core(g, t)

            @pl.when((r >= 1) & (r < planes + 1))
            def _():
                stage_plane(g, t + 1)

            @pl.when(r >= 2)
            def _():
                stage_line(g, t + 2)

            if with_tiles and g % 2 == 0:
                work(r * 2 + g // 2)

    @pl.loop(0, planes)
    def _(r):
        t = planes - 1 - r
        zz = visit(t, z, planes)
        for g in range(n):
            core_copy(g, zz).wait_send()

            def even():
                diag_x(g, zz).wait_send()
                diag_y(g, zz, False).wait_send()

            lean_or_even(lambda: diag_y(g, zz, True).wait_send(), even)
            x_copy(g, zz).wait_send()
            y_copy(g, zz).wait_send()

            @pl.when(t > 0)
            def _():
                z_copy(g, zz, True).wait_send()

    if with_tiles:
        for s in range(seqs):
            send_b(s).wait()

            @pl.when(x == 0)
            def _():
                send_back(s).wait_recv()

            @pl.when(x == 1)
            def _():
                send_d(s).wait_send()
                send_back(s).wait_send()

        @pl.when(x == 1)
        def _():
            chip[...] = jnp.zeros_like(chip)

        @pl.loop(0, seqs * rows // 32)
        def _(i):
            seq = lax.div(i, rows // 32)
            at = pl.ds(pl.multiple_of(lax.rem(i, rows // 32) * 32, 32), 32)
            flat = pl.ds(pl.multiple_of(i * 32, 32), 32)
            cos_rows, sin_rows = cos_table[flat, :], sin_table[flat, :]
            for k in range(pairs):
                lanes = pl.ds(k * 128, 128)

                def summed(kind):
                    return (
                        mine[kind, seq, at, lanes].astype(f32)
                        + from_b[kind, seq, at, lanes].astype(f32)
                        + chip[kind, seq, at, lanes].astype(f32)
                    )

                d_key[flat, lanes] = turned(summed(0), cos_rows, sin_rows, -1.0).astype(jnp.bfloat16)
                half = 0.5 * summed(1)
                d_value[flat, lanes] = half.astype(jnp.bfloat16)
                first_grad[flat, lanes] = half


def scatter_sum(planes, partials, collective_id, attention=None):
    n = len(partials)
    partials = [
        p.reshape(planes, 2, 2, 2, p.shape[0] // (planes * 8), p.shape[1]) for p in partials
    ]
    shapes = [p.shape[4:] for p in partials]
    types = [p.dtype for p in partials]
    dma = pltpu.SemaphoreType.DMA

    def boxes(lead, narrow=False):
        out = []
        for s, d in zip(shapes, types):
            width = s[1] // 2 // 128 * 128 if narrow else s[1]
            out.append(pltpu.VMEM((*lead, s[0], width), d))
        return out

    extra, extra_out, extra_scratch = [], [], []
    if attention is not None:
        extra = list(attention)
        box = attention[2].shape
        seqs, rows, width = box[1:]
        flat = (seqs * rows, width)
        extra_out = [
            jax.ShapeDtypeStruct(box[1:], jnp.bfloat16),
            jax.ShapeDtypeStruct(flat, jnp.bfloat16),
            jax.ShapeDtypeStruct(flat, jnp.bfloat16),
            jax.ShapeDtypeStruct(flat, jnp.float32),
        ]
        extra_scratch = [
            *[pltpu.VMEM(box, jnp.bfloat16)] * 6,
            dma((3, seqs)),
            dma((3, seqs)),
            *attend_back_scratch(rows),
        ]
    return pl.pallas_call(
        functools.partial(scatter_kernel, planes, shapes, bool(extra)),
        out_shape=[jax.ShapeDtypeStruct(s, jnp.float32) for s in shapes] + extra_out,
        in_specs=[pl.BlockSpec(memory_space=pl.ANY)] * n
        + [pl.BlockSpec(memory_space=pltpu.VMEM)] * len(extra),
        out_specs=[pl.BlockSpec(memory_space=pltpu.VMEM)] * (n + len(extra_out)),
        scratch_shapes=[
            *boxes((planes, 2, 2)),
            *boxes((planes, 2, 2)),
            *boxes((planes,), True),
            *boxes((planes,)),
            *boxes((planes,)),
            *boxes((planes,)),
            *boxes((planes + 1,)),
            dma((n, planes)),
            dma((n, planes)),
            dma((n, planes)),
            dma((n, planes, 2)),
            dma((n, planes, 2)),
            dma((n, planes)),
            dma((n, planes)),
            dma((n, planes)),
            dma((n, planes)),
            dma((n, planes)),
            dma((n, planes + 1)),
            *extra_scratch,
        ],
        compiler_params=pltpu.CompilerParams(
            collective_id=collective_id, has_side_effects=True, vmem_limit_bytes=67043328
        ),
        name="gradient_scatter",
    )(*partials, *extra)


def on_device(
    planes,
    tokens,
    first_values,
    cotangent,
    segment_ids,
    attn_gain,
    w_query,
    w_key,
    w_value,
    w_out,
    ffn_gain,
    gate_weight,
    up_weight,
    down_weight,
):
    f32, bf16 = jnp.float32, jnp.bfloat16
    devices = planes * 8
    seqs, rows, width = tokens.shape
    rank = lax.axis_index("ctx")
    share = attn_gain.shape[0]
    gains = jnp.zeros((16, 128), bf16)
    gains = gains.at[0, :share].set(attn_gain).at[1, :share].set(ffn_gain)
    (gains, w_query, w_key, w_value), _ = gather(planes, [gains, w_query, w_key, w_value], 0)
    gains = gains.reshape(devices, 16, 128)
    attn_gain = gains[:, 0, :share].reshape(1, width)
    ffn_gain = gains[:, 1, :share].reshape(1, width)
    starts, cos_table, sin_table = tables(segment_ids, rank, rows)
    flat = (seqs * rows, width)
    local = (seqs, rows, width)
    tokens = tokens.reshape(flat)
    mm = functools.partial(jnp.dot, preferred_element_type=f32)
    by_rows = lambda a, b: lax.dot_general(a, b, TN, preferred_element_type=f32).astype(bf16)
    back = lambda a, b: lax.dot_general(a, b, NT, preferred_element_type=f32)
    normed_one, query_rot, pair = project(
        tokens, first_values.reshape(flat), attn_gain, w_query, w_key, w_value, cos_table, sin_table
    )
    query_rot = query_rot.reshape(local)
    pair = pair.reshape(2, *local)
    (w_out, gate_weight, up_weight, down_weight, pair), _ = lax.optimization_barrier(
        ((w_out, gate_weight, up_weight, down_weight, pair), normed_one)
    )
    (w_out, gate_weight, up_weight, down_weight), others = gather(
        planes, [w_out, gate_weight, up_weight, down_weight], 1, pair
    )
    tiles = [pair, *others]
    context3, log_total = attend(starts, query_rot, tiles)
    context = context3.reshape(flat)
    tokens_float = tokens.astype(f32)
    scale_one = inverse_rms(tokens_float)
    cotangent = cotangent.reshape(flat)
    residual = tokens_float + mm(context, w_out)
    scale_two = inverse_rms(residual)
    second_normed = (residual * scale_two * ffn_gain.astype(f32)).astype(bf16)
    gate = mm(second_normed, gate_weight)
    up = mm(second_normed, up_weight)
    hidden = (swish(gate) * up).astype(bf16)
    output = (residual + mm(hidden, down_weight)).astype(bf16)

    out_float = cotangent.astype(f32)
    d_down = by_rows(hidden, cotangent)
    d_hidden = back(cotangent, down_weight)
    sigmoid_gate = jax.nn.sigmoid(gate)
    d_gate = (d_hidden * up * sigmoid_gate * (1.0 + gate * (1.0 - sigmoid_gate))).astype(bf16)
    d_up = (d_hidden * (gate * sigmoid_gate)).astype(bf16)
    d_gate_weight = by_rows(second_normed, d_gate)
    d_up_weight = by_rows(second_normed, d_up)
    d_normed_two = back(d_gate, gate_weight) + back(d_up, up_weight)
    d_ffn_gain = jnp.sum(d_normed_two * residual * scale_two, axis=0)
    weighted_two = d_normed_two * ffn_gain.astype(f32)
    d_residual = (
        out_float
        + scale_two * weighted_two
        - residual
        * (scale_two * scale_two * scale_two)
        * jnp.mean(weighted_two * residual, axis=-1, keepdims=True)
    )
    d_residual_low = d_residual.astype(bf16)
    d_out = by_rows(context, d_residual_low)
    d_context = back(d_residual_low, w_out).astype(bf16).reshape(local)
    s_down, s_gate, s_up, s_out, d_query, d_key, d_value, first_grad = scatter_sum(
        planes,
        [d_down, d_gate_weight, d_up_weight, d_out],
        2,
        [starts, query_rot, *tiles, context3, d_context, log_total, cos_table, sin_table],
    )
    d_query = d_query.reshape(flat)
    d_wq = by_rows(normed_one, d_query)
    d_wk = by_rows(normed_one, d_key)
    d_wv = by_rows(normed_one, d_value)
    d_normed_one = back(d_query, w_query) + back(d_key, w_key) + back(d_value, w_value)
    d_attn_gain = jnp.sum(d_normed_one * tokens_float * scale_one, axis=0)
    weighted_one = d_normed_one * attn_gain.astype(f32)
    token_grad = (
        d_residual
        + scale_one * weighted_one
        - tokens_float
        * (scale_one * scale_one * scale_one)
        * jnp.mean(weighted_one * tokens_float, axis=-1, keepdims=True)
    )
    d_gains = jnp.stack([d_attn_gain, d_ffn_gain]).reshape(2, devices, share)
    d_gains = jnp.zeros((devices, 8, 256), f32).at[:, :2, :share].set(d_gains.transpose(1, 0, 2))
    s_wq, s_wk, s_wv, s_gains = scatter_sum(
        planes, [d_wq, d_wk, d_wv, d_gains.reshape(devices * 8, 256)], 3
    )
    return (
        output.reshape(local),
        token_grad.reshape(local),
        first_grad.reshape(local),
        s_gains[0, :share],
        s_wq,
        s_wk,
        s_wv,
        s_out,
        s_gains[1, :share],
        s_gate,
        s_up,
        s_down,
    )


def solution(mesh):
    token, weight, vector = P("dp", "ctx", None), P(("dp", "ctx"), None), P(("dp", "ctx"))
    return jax.shard_map(
        functools.partial(on_device, mesh.shape["dp"] // 2),
        mesh=mesh,
        in_specs=(
            token,
            token,
            token,
            P("dp", None),
            vector,
            weight,
            weight,
            weight,
            weight,
            vector,
            weight,
            weight,
            weight,
        ),
        out_specs=(
            token,
            token,
            token,
            vector,
            weight,
            weight,
            weight,
            weight,
            vector,
            weight,
            weight,
            weight,
        ),
        check_vma=False,
    )
```

```python
import functools
import jax
import jax.numpy as jnp
from jax import lax
from jax.experimental import pallas as pl
from jax.experimental.pallas import tpu as pltpu
from jax.sharding import PartitionSpec as P

HEADS = 16
HEAD_DIM = 64
MESH_ID = pl.DeviceIdType.MESH

epsilon = 1e-05
rope_base = 10000.0
score_scale = 0.125
masked_score = -1e30


def inverse_rms(values):
    return lax.rsqrt(jnp.mean(values * values, axis=-1, keepdims=True) + epsilon)


def swish(values):
    return values * jax.nn.sigmoid(values)


def first_half(shape):
    return lax.broadcasted_iota(jnp.int32, shape, len(shape) - 1) % HEAD_DIM < HEAD_DIM // 2


def swap_halves(values):
    return jnp.where(
        first_half(values.shape), pltpu.roll(values, 96, 1), pltpu.roll(values, 32, 1)
    )


def turned(values, cos_table, sin_table, sign):
    return values * cos_table + sign * (swap_halves(values) * sin_table)


def tables(segment_ids, rank, rows):
    seqs, length = segment_ids.shape
    places = jnp.arange(length, dtype=jnp.int32)
    edges = jnp.concatenate(
        [jnp.ones((seqs, 1), dtype=jnp.bool_), segment_ids[:, 1:] != segment_ids[:, :-1]], axis=1
    )
    starts = lax.cummax(jnp.where(edges, places[None, :], 0), axis=1)
    starts = lax.dynamic_slice_in_dim(starts, rank * rows, rows, 1)
    local = rank * rows + jnp.arange(rows, dtype=jnp.int32) - starts
    lane = jnp.arange(128, dtype=jnp.int32)
    half = HEAD_DIM // 2
    frequency = rope_base ** (-(lane % half).astype(jnp.float32) * 2.0 / HEAD_DIM)
    angles = local.astype(jnp.float32).reshape(seqs * rows, 1) * frequency
    sign = jnp.where(lane % HEAD_DIM < half, -1.0, 1.0)
    return starts.reshape(seqs, 1, rows), jnp.cos(angles), jnp.sin(angles) * sign


def normalise(tok, gain, normed):
    rows = tok.shape[0]

    @pl.loop(0, rows // 64)
    def _(i):
        at = pl.ds(pl.multiple_of(i * 64, 64), 64)
        values = tok[at, :].astype(jnp.float32)
        normed[at, :] = (values * inverse_rms(values) * gain).astype(jnp.bfloat16)


def columns_of(weight, lanes):
    block = weight[:, :, lanes]
    if block.shape[1] % 16:
        block = block.astype(jnp.float32)
    return block.reshape(block.shape[0] * block.shape[1], block.shape[2]).astype(jnp.bfloat16)


def project(normed, first, wq, wk, wv, cos_ref, sin_ref, query, pair):
    f32, bf16 = jnp.float32, jnp.bfloat16
    seqs, rows, width = query.shape

    @pl.loop(0, width // 256)
    def _(i):
        lanes = pl.ds(pl.multiple_of(i * 256, 256), 256)
        n1 = normed[...]
        cos_table, sin_table = cos_ref[...], sin_ref[...]
        queries = jnp.dot(n1, columns_of(wq, lanes), preferred_element_type=f32)
        keys = jnp.dot(n1, columns_of(wk, lanes), preferred_element_type=f32)
        values = jnp.dot(n1, columns_of(wv, lanes), preferred_element_type=f32)
        mixed = (0.5 * values + 0.5 * first[:, lanes].astype(f32)).astype(bf16)
        for half in range(2):
            part = slice(half * 128, half * 128 + 128)
            at = pl.ds(pl.multiple_of(i * 256 + half * 128, 128), 128)
            q = turned(queries[:, part], cos_table, sin_table, 1.0).astype(bf16)
            k = turned(keys[:, part], cos_table, sin_table, 1.0).astype(bf16)
            for s in range(seqs):
                query[s, :, at] = q[s * rows : (s + 1) * rows]
                pair[0, s, :, at] = k[s * rows : (s + 1) * rows]
                pair[1, s, :, at] = mixed[s * rows : (s + 1) * rows, part]


def two_heads(block, scale):
    lane = lax.broadcasted_iota(jnp.int32, block.shape, 1)
    scaled = block * jnp.asarray(scale, block.dtype)
    zero = jnp.zeros_like(block)
    return jnp.concatenate(
        [jnp.where(lane < HEAD_DIM, scaled, zero), jnp.where(lane < HEAD_DIM, zero, scaled)]
    )


def own_lanes(both):
    rows = both.shape[1] // 2
    lane = lax.broadcasted_iota(jnp.int32, (both.shape[0], rows), 0)
    return jnp.where(lane < HEAD_DIM, both[:, :rows], both[:, rows:]).T


def fill_bias(bias, starts, rank):
    rows = bias.shape[1]
    key = lax.broadcasted_iota(jnp.int32, (rows, rows), 0)
    place = rank * rows + lax.broadcasted_iota(jnp.int32, (rows, rows), 1)
    begin = starts[...]
    for t in range(4):
        x, c = lax.div(rank, 2), lax.rem(rank, 2)
        owner = (1 - x if t >= 2 else x) * 2 + (1 - c if t % 2 else c)
        at = owner * rows + key
        bias[t] = jnp.where((at >= begin) & (at <= place), 0.0, masked_score)


NT = (((1,), (1,)), ((), ()))
TN = (((0,), (0,)), ((), ()))


def attend_step(rank, begin, starts, q, tiles, out, log_total, bias, scores, peak, total, acc):
    f32, bf16 = jnp.float32, jnp.bfloat16

    @pl.when(begin)
    def _():
        fill_bias(bias, starts, rank)

    high = rank >= 2
    stacked = two_heads(q, score_scale)

    def score(t):
        s = lax.dot_general(tiles[t][0][...], stacked, NT, preferred_element_type=f32)
        s = s + jnp.concatenate([bias[t], bias[t]], axis=1)
        scores[t] = s
        return jnp.max(s, axis=0, keepdims=True)

    def gather_values(t, top):
        e = jnp.exp(scores[t] - top)
        part = lax.dot_general(tiles[t][1][...], e.astype(bf16), TN, preferred_element_type=f32)
        return jnp.sum(e, axis=0, keepdims=True), part

    peak[...] = jnp.maximum(score(0), score(1))

    @pl.when(high)
    def _():
        peak[...] = jnp.maximum(peak[...], jnp.maximum(score(2), score(3)))

    top = peak[...]
    sum_a, acc_a = gather_values(0, top)
    sum_b, acc_b = gather_values(1, top)
    total[...] = sum_a + sum_b
    acc[...] = acc_a + acc_b

    @pl.when(high)
    def _():
        top = peak[...]
        sum_a, acc_a = gather_values(2, top)
        sum_b, acc_b = gather_values(3, top)
        total[...] += sum_a + sum_b
        acc[...] += acc_a + acc_b

    out[...] = own_lanes(acc[...] / total[...]).astype(bf16)
    log_total[...] = peak[...] + jnp.log(total[...])


def attend_scratch(rows):
    return [
        pltpu.VMEM((4, rows, rows), jnp.float32),
        pltpu.VMEM((4, rows, 2 * rows), jnp.float32),
        pltpu.VMEM((1, 2 * rows), jnp.float32),
        pltpu.VMEM((1, 2 * rows), jnp.float32),
        pltpu.VMEM((128, 2 * rows), jnp.float32),
    ]


def attend_back_step(
    rank, begin, starts, q, tiles, context, d_context, log_total, cos_t, sin_t, d_q, d_tiles, bias, acc
):
    f32, bf16 = jnp.float32, jnp.bfloat16

    @pl.when(begin)
    def _():
        fill_bias(bias, starts, rank)

    high = rank >= 2
    stacked = two_heads(q, score_scale)
    stacked_do = two_heads(d_context, 1.0)
    turned_product = (d_context.astype(f32) * context.astype(f32)).T
    delta = jnp.concatenate(
        [
            jnp.sum(turned_product[:HEAD_DIM], axis=0, keepdims=True),
            jnp.sum(turned_product[HEAD_DIM:], axis=0, keepdims=True),
        ],
        axis=1,
    )
    lse = log_total[...]

    def one(t):
        keys, values = tiles[t][0][...], tiles[t][1][...]
        s = lax.dot_general(keys, stacked, NT, preferred_element_type=f32)
        s = s + jnp.concatenate([bias[t], bias[t]], axis=1)
        p = jnp.exp(s - lse)
        dp = lax.dot_general(values, stacked_do, NT, preferred_element_type=f32)
        ds = (p * (dp - delta)).astype(bf16)
        d_tiles[t][1][...] = jnp.dot(p.astype(bf16), stacked_do, preferred_element_type=f32).astype(bf16)
        d_tiles[t][0][...] = jnp.dot(ds, stacked, preferred_element_type=f32).astype(bf16)
        return lax.dot_general(keys, ds, TN, preferred_element_type=f32)

    acc[...] = one(0) + one(1)

    @pl.when(high)
    def _():
        acc[...] += one(2) + one(3)

    d_q[...] = turned(own_lanes(acc[...]) * score_scale, cos_t[...], sin_t[...], -1.0).astype(bf16)


def attend_back_scratch(rows):
    return [pltpu.VMEM((4, rows, rows), jnp.float32), pltpu.VMEM((128, 2 * rows), jnp.float32)]


def position():
    dp = lax.axis_index("dp")
    ct = lax.axis_index("ctx")
    return lax.div(dp, 2), lax.rem(dp, 2), lax.div(ct, 2), lax.rem(ct, 2)


def visit(step, z, planes):
    back = planes - 1 - step
    high = back + jnp.where(back >= z, 1, 0)
    low = planes - 1 - back
    low = low - jnp.where(low <= z, 1, 0)
    other = jnp.where(z < planes // 2, low, high)
    return jnp.where(step == 0, z, other)


def device(z, y, x, c):
    return (z * 2 + y, x * 2 + c)


def halves(shape):
    if shape[0] % 2 == 0:
        cut = shape[0] // 2
        return (pl.ds(0, cut), slice(None), slice(None)), (pl.ds(cut, cut), slice(None), slice(None))
    cut = shape[2] // 2 // 128 * 128
    return (
        (slice(None), slice(None), pl.ds(0, cut)),
        (slice(None), slice(None), pl.ds(cut, shape[2] - cut)),
    )


def entry_barrier(z, y, x, c, planes):
    barrier = pltpu.get_barrier_semaphore()

    def hello(target):
        pl.semaphore_signal(barrier, inc=1, device_id=target, device_id_type=MESH_ID)

    hello(device(z, y, 1 - x, c))
    hello(device(z, 1 - y, x, c))
    hello(device(z, y, x, 1 - c))

    @pl.when(z > 0)
    def _():
        hello(device(z - 1, y, x, c))

    @pl.when(z < planes - 1)
    def _():
        hello(device(z + 1, y, x, c))

    pl.semaphore_wait(barrier, 3 + jnp.where(z > 0, 1, 0) + jnp.where(z < planes - 1, 1, 0))


def forward_kernel(planes, shapes, first_group, *refs):
    n = len(shapes)
    ins, refs = refs[:n], refs[n:]
    tok, first, starts, cos_table, sin_table = refs[:5]
    outs, refs = refs[5 : 5 + n], refs[5 + n :]
    normed, query, mine, near, chip, far, context, log_total = refs[:8]
    sems, refs = refs[8:19], refs[19:]
    own_sem, z_send, z_recv, x_send, x_recv, y_send, y_recv, d_send, d_recv, c_send, c_recv = sems
    tile_send, tile_recv, load_sem, gains, *weights = refs[: 4 + first_group - 1]
    scratch = refs[4 + first_group - 1 :]
    z, y, x, c = position()
    entry_barrier(z, y, x, c, planes)
    local = [
        pltpu.make_async_copy(ins[g], outs[g].at[:, z, y, x, c], own_sem.at[g]) for g in range(n)
    ]
    for copy in local:
        copy.start()

    def push(src, dst, send, recv, target):
        return pltpu.make_async_remote_copy(
            src_ref=src,
            dst_ref=dst,
            send_sem=send,
            recv_sem=recv,
            device_id=target,
            device_id_type=MESH_ID,
        )

    def spot(g, zz, yy, xx):
        return outs[g].at[:, zz, yy, xx, c]

    def z_copy(g, zz, up, own):
        side = 1 if up else 0
        return push(
            ins[g] if own else spot(g, zz, y, x),
            spot(g, zz, y, x),
            z_send.at[g, zz, side],
            z_recv.at[g, zz],
            device(z + 1 if up else z - 1, y, x, c),
        )

    def x_copy(g, zz, own):
        return push(
            ins[g] if own else spot(g, zz, y, x),
            spot(g, zz, y, x),
            x_send.at[g, zz],
            x_recv.at[g, zz],
            device(z, y, 1 - x, c),
        )

    def y_copy(g, zz, own):
        return push(
            ins[g] if own else spot(g, zz, y, x),
            spot(g, zz, y, x),
            y_send.at[g, zz],
            y_recv.at[g, zz],
            device(z, 1 - y, x, c),
        )

    def relay(g, zz, half, by_y):
        here = spot(g, zz, y, 1 - x) if by_y else spot(g, zz, 1 - y, x)
        here = here.at[halves(shapes[g])[half]]
        return push(
            here,
            here,
            d_send.at[g, zz, 2 * half if by_y else 1],
            d_recv.at[g, zz, half],
            device(z, 1 - y, x, c) if by_y else device(z, y, 1 - x, c),
        )

    def diag_arrival(g, zz, half):
        here = spot(g, zz, 1 - y, 1 - x).at[halves(shapes[g])[half]]
        return push(
            here, here, d_send.at[g, zz, half], d_recv.at[g, zz, half], device(z, y, x, 1 - c)
        )

    def core_copy(g, zz, mine):
        here = outs[g].at[:, zz, :, :, c if mine else 1 - c]
        return push(here, here, c_send.at[g, zz], c_recv.at[g, zz], device(z, y, x, 1 - c))

    def on_links(g, t, act):
        zz = visit(t, z, planes)

        def both(own):
            up = (z < planes - 1) if own else (zz < z) & (z < planes - 1)
            down = (z > 0) if own else (zz > z) & (z > 0)
            pl.when(down)(lambda: act(z_copy(g, zz, False, own)))
            pl.when(up)(lambda: act(z_copy(g, zz, True, own)))
            act(x_copy(g, zz, own))
            act(y_copy(g, zz, own))

        pl.when(t == 0)(lambda: both(True))
        pl.when(t > 0)(lambda: both(False))

    def on_relays(g, t, act, between=lambda: None):
        zz = visit(t, z, planes)
        act(relay(g, zz, 0, True))
        if g < first_group:
            between()
            act(relay(g, zz, 1, False))
            return
        lean = t > 0
        pl.when(lean & (x == 1))(lambda: act(relay(g, zz, 1, True)))
        between()
        pl.when((x == 1) | jnp.logical_not(lean))(lambda: act(relay(g, zz, 1, False)))

    def start(copy):
        copy.start()

    def wait_send(copy):
        copy.wait_send()

    def stage_line(g, t):
        @pl.when(t > 0)
        def _():
            z_copy(g, visit(t, z, planes), True, False).wait_recv()

        on_links(g, t, start)

    def stage_plane(g, t):
        zz = visit(t, z, planes)
        x_copy(g, zz, False).wait_recv()
        on_relays(g, t, start, lambda: y_copy(g, zz, False).wait_recv())

    def stage_core(g, t):
        zz = visit(t, z, planes)
        pl.when(t == 0)(lambda: local[g].wait())
        diag_arrival(g, zz, 0).wait_recv()
        diag_arrival(g, zz, 1).wait_recv()
        core_copy(g, zz, True).start()

    seqs, rows, width = query.shape
    pairs = width // 128
    partner = device(z, y, x, 1 - c)

    def to_partner(s):
        return push(
            mine.at[:, s], near.at[:, s], tile_send.at[0, s], tile_recv.at[0, s], partner
        )

    def to_x(s):
        return push(
            mine.at[:, s],
            chip.at[:, s],
            tile_send.at[1, s],
            tile_recv.at[1, s],
            device(z, y, 1 - x, c),
        )

    def passed_on(s):
        return push(
            chip.at[:, s], far.at[:, s], tile_send.at[2, s], tile_recv.at[2, s], partner
        )

    def send_tiles(s):
        to_partner(s).start()
        pl.when(x == 0)(lambda: to_x(s).start())

    def projection():
        @pl.loop(0, planes)
        def _(t):
            for g in range(first_group):
                core_copy(g, visit(t, z, planes), False).wait_recv()

        loads = [
            pltpu.make_async_copy(outs[g].at[0], buf, load_sem.at[g])
            for g, buf in enumerate([gains, *weights])
        ]
        for copy in loads:
            copy.start()
        loads[0].wait()
        flat_gains = [gains[i, j, k, m] for i in range(planes) for j in (0, 1) for k in (0, 1) for m in (0, 1)]
        per = len(flat_gains) * 128 // width
        gain = jnp.concatenate(
            [
                sum(b[:1].astype(jnp.float32) for b in flat_gains[i * per : (i + 1) * per])
                for i in range(width // 128)
            ],
            axis=1,
        )
        normalise(tok, gain, normed)
        for copy in loads[1:]:
            copy.wait()
        as_blocks = lambda w: w.reshape((planes * 8, *w.shape[4:]))
        project(
            normed, first, *[as_blocks(w) for w in weights], cos_table, sin_table, query, mine
        )
        send_tiles(0)

    def unit(u):
        s, p = lax.div(u, pairs), lax.rem(u, pairs)
        lanes = pl.ds(pl.multiple_of(p * 128, 128), 128)
        attend_step(
            lax.axis_index("ctx"),
            p == 0,
            starts.at[s],
            query[s, :, lanes],
            [[w.at[0, s, :, lanes], w.at[1, s, :, lanes]] for w in (mine, near, chip, far)],
            context.at[s, :, lanes],
            log_total.at[s, p],
            *scratch,
        )

    def work(i):
        pl.when(i == 1)(projection)

        @pl.when(i == 3)
        def _():
            for s in range(1, seqs):
                send_tiles(s)

        @pl.when((i == 4) | (i == 6))
        def _():
            s = lax.div(i, 2) - 2
            to_partner(s).wait_recv()

            @pl.when(x == 1)
            def _():
                to_x(s).wait_recv()
                passed_on(s).start()
                passed_on(s).wait_recv()

        @pl.when((i >= 4) & (i < 8))
        def _():
            each = seqs * pairs // 4

            @pl.loop(0, each)
            def _(j):
                unit((i - 4) * each + j)

    groups = (range(first_group), range(first_group, n))

    @pl.loop(0, max(2 * planes + 2, planes + 5))
    def _(r):
        for k, group in enumerate(groups):
            t = r - k * planes
            for g in group:
                pl.when((t >= 0) & (t < planes))(lambda: stage_line(g, t))
                pl.when((t >= 1) & (t < planes + 1))(lambda: stage_plane(g, t - 1))
                pl.when((t >= 2) & (t < planes + 2))(lambda: stage_core(g, t - 2))
                if k == 1 and (g - first_group) % 2 == 1:
                    work((r - planes - 1) * 2 + (g - first_group) // 2)

    @pl.loop(0, planes)
    def _(t):
        zz = visit(t, z, planes)
        for g in range(n):
            if g >= first_group:
                core_copy(g, zz, False).wait_recv()
            core_copy(g, zz, True).wait_send()
            on_links(g, t, wait_send)
            on_relays(g, t, wait_send)

    for s in range(seqs):
        to_partner(s).wait_send()
        pl.when(x == 0)(lambda: to_x(s).wait_send())
        pl.when(x == 1)(lambda: passed_on(s).wait_send())


def forward(planes, first_group, blocks, tok, first, starts, cos_table, sin_table):
    blocks = [b[None] for b in blocks]
    n = len(blocks)
    shapes = [b.shape for b in blocks]
    seqs, _, rows = starts.shape
    width = tok.shape[1]
    bf16 = jnp.bfloat16
    dma = pltpu.SemaphoreType.DMA
    anywhere = pl.BlockSpec(memory_space=pl.ANY)
    vmem = pl.BlockSpec(memory_space=pltpu.VMEM)
    local = jax.ShapeDtypeStruct((seqs, rows, width), bf16)
    tile = jax.ShapeDtypeStruct((2, seqs, rows, width), bf16)
    got = pl.pallas_call(
        functools.partial(forward_kernel, planes, shapes, first_group),
        out_shape=[
            jax.ShapeDtypeStruct((s[0], planes, 2, 2, 2, s[1], s[2]), b.dtype)
            for s, b in zip(shapes, blocks)
        ]
        + [jax.ShapeDtypeStruct(tok.shape, bf16), local, *[tile] * 4, local]
        + [jax.ShapeDtypeStruct((seqs, width // 128, 1, 2 * rows), jnp.float32)],
        in_specs=[anywhere] * n + [vmem] * 5,
        out_specs=[anywhere] * n + [vmem] * 8,
        scratch_shapes=[
            dma((n,)),
            dma((n, planes, 2)),
            dma((n, planes)),
            dma((n, planes)),
            dma((n, planes)),
            dma((n, planes)),
            dma((n, planes)),
            dma((n, planes, 3)),
            dma((n, planes, 2)),
            dma((n, planes)),
            dma((n, planes)),
            dma((3, seqs)),
            dma((3, seqs)),
            dma((first_group,)),
            *[pltpu.VMEM((planes, 2, 2, 2, *s[1:]), bf16) for s in shapes[:first_group]],
            *attend_scratch(rows),
        ],
        compiler_params=pltpu.CompilerParams(
            collective_id=0, has_side_effects=True, vmem_limit_bytes=48 * 2**20
        ),
        name="forward",
    )(*blocks, tok, first, starts, cos_table, sin_table)
    full = [g.reshape(planes * 8 * s[1], s[2]) for g, s in zip(got, shapes)]
    return full, got[n:]


def columns(shape, half):
    cut = shape[1] // 2 // 128 * 128
    return pl.ds(0, cut) if half == 0 else pl.ds(cut, shape[1] - cut)


def scatter_kernel(planes, shapes, with_tiles, *refs):
    n = len(shapes)
    parts, refs = refs[:n], refs[n:]
    if with_tiles:
        starts, query, *tiles, context, d_context, log_total, cos_table, sin_table = refs[:11]
        refs = refs[11:]
    outs, refs = refs[:n], refs[n:]
    if with_tiles:
        d_query, d_key, d_value, first_grad = refs[:4]
        refs = refs[4:]
        mine, near, chip, far, from_b, from_d, tile_send, tile_recv, bias, acc = refs[-10:]
        refs = refs[:-10]
    own, from_core, from_dx, from_dy, from_x, from_y, from_z = (
        refs[k * n : (k + 1) * n] for k in range(7)
    )
    own_sem, c_send, c_recv, d_send, d_recv, x_send, x_recv, y_send, y_recv, z_send, z_recv = refs[
        7 * n :
    ]
    z, y, x, c = position()
    entry_barrier(z, y, x, c, planes)

    def push(src, dst, send, recv, target):
        return pltpu.make_async_remote_copy(
            src_ref=src,
            dst_ref=dst,
            send_sem=send,
            recv_sem=recv,
            device_id=target,
            device_id_type=MESH_ID,
        )

    f32 = jnp.float32

    def add(dst, *srcs):
        total = dst[...].astype(f32)
        for src in srcs:
            total = total + src[...].astype(f32)
        dst[...] = total.astype(dst.dtype)

    def load(g, zz):
        return pltpu.make_async_copy(
            parts[g].at[zz, :, :, c], own[g].at[zz], own_sem.at[g, zz]
        )

    def core_copy(g, zz):
        return push(
            parts[g].at[zz, :, :, 1 - c],
            from_core[g].at[zz],
            c_send.at[g, zz],
            c_recv.at[g, zz],
            device(z, y, x, 1 - c),
        )

    def diag_x(g, zz):
        return push(
            own[g].at[zz, 1 - y, 1 - x, :, columns(shapes[g], 0)],
            from_dx[g].at[zz],
            d_send.at[g, zz, 0],
            d_recv.at[g, zz, 0],
            device(z, y, 1 - x, c),
        )

    def diag_y(g, zz, full):
        part = slice(None) if full else columns(shapes[g], 1)
        return push(
            own[g].at[zz, 1 - y, 1 - x, :, part],
            from_dy[g].at[zz, :, part],
            d_send.at[g, zz, 1],
            d_recv.at[g, zz, 1],
            device(z, 1 - y, x, c),
        )

    def x_copy(g, zz):
        return push(
            own[g].at[zz, y, 1 - x],
            from_x[g].at[zz],
            x_send.at[g, zz],
            x_recv.at[g, zz],
            device(z, y, 1 - x, c),
        )

    def y_copy(g, zz):
        return push(
            own[g].at[zz, 1 - y, x],
            from_y[g].at[zz],
            y_send.at[g, zz],
            y_recv.at[g, zz],
            device(z, 1 - y, x, c),
        )

    def z_copy(g, zz, up):
        slot = zz if up else jnp.where(zz == z - 1, planes, zz)
        return push(
            own[g].at[zz, y, x],
            from_z[g].at[slot],
            z_send.at[g, zz],
            z_recv.at[g, slot],
            device(z + 1 if up else z - 1, y, x, c),
        )

    def z_arrival(g, slot):
        return push(
            from_z[g].at[slot],
            from_z[g].at[slot],
            z_send.at[g, 0],
            z_recv.at[g, slot],
            device(z, y, x, 1 - c),
        )

    def lean_or_even(lean, even):
        if not with_tiles:
            even()
            return
        pl.when(x == 0)(even)
        pl.when(x == 1)(lean)

    if with_tiles:
        partner = device(z, y, x, 1 - c)
        seqs, rows = mine.shape[1:3]
        pairs = mine.shape[3] // 128

        def send_b(s):
            return push(
                near.at[:, s], from_b.at[:, s], tile_send.at[0, s], tile_recv.at[0, s], partner
            )

        def send_d(s):
            return push(
                far.at[:, s], from_d.at[:, s], tile_send.at[1, s], tile_recv.at[1, s], partner
            )

        def send_back(s):
            return push(
                chip.at[:, s],
                chip.at[:, s],
                tile_send.at[2, s],
                tile_recv.at[2, s],
                device(z, y, 1 - x, c),
            )

        def unit(u):
            s, p = lax.div(u, pairs), lax.rem(u, pairs)
            lanes = pl.ds(pl.multiple_of(p * 128, 128), 128)
            flat = pl.ds(pl.multiple_of(s * rows, rows), rows)
            two = lambda ref: [ref.at[0, s, :, lanes], ref.at[1, s, :, lanes]]
            attend_back_step(
                lax.axis_index("ctx"),
                p == 0,
                starts.at[s],
                query[s, :, lanes],
                [two(t) for t in tiles],
                context[s, :, lanes],
                d_context[s, :, lanes],
                log_total.at[s, p],
                cos_table.at[flat],
                sin_table.at[flat],
                d_query.at[s, :, lanes],
                [two(t) for t in (mine, near, chip, far)],
                bias,
                acc,
            )

        def work(i):
            each = seqs * pairs // 4

            @pl.when(i < 4)
            def _():
                @pl.loop(0, each)
                def _(j):
                    unit(i * each + j)

            @pl.when((i == 1) | (i == 3))
            def _():
                s = lax.div(i, 2)
                send_b(s).start()

                @pl.when(x == 1)
                def _():
                    send_d(s).start()

            @pl.when(((i == 2) | (i == 4)) & (x == 1))
            def _():
                s = lax.div(i, 2) - 1
                send_d(s).wait_recv()
                for kind in range(2):

                    @pl.loop(0, rows // 32)
                    def _(j):
                        at = pl.ds(pl.multiple_of(j * 32, 32), 32)
                        add(chip.at[kind, s, at], from_d.at[kind, s, at])

                send_back(s).start()

    @pl.loop(0, planes)
    def _(r):
        zz = visit(planes - 1 - r, z, planes)
        for g in range(n):
            core_copy(g, zz).start()
            load(g, zz).start()

    def stage_core(g, t):
        zz = visit(t, z, planes)
        load(g, zz).wait()
        core_copy(g, zz).wait_recv()
        add(own[g].at[zz, 1 - y, 1 - x], from_core[g].at[zz, 1 - y, 1 - x])

        def even():
            diag_x(g, zz).start()
            diag_y(g, zz, False).start()

        lean_or_even(lambda: diag_y(g, zz, True).start(), even)
        add(own[g].at[zz, 1 - y, x], from_core[g].at[zz, 1 - y, x])
        if with_tiles:

            @pl.when(x == 0)
            def _():
                y_copy(g, zz).start()

        add(own[g].at[zz, y, 1 - x], from_core[g].at[zz, y, 1 - x])
        add(own[g].at[zz, y, x], from_core[g].at[zz, y, x])

    def stage_plane(g, t):
        zz = visit(t, z, planes)

        def take_x():
            diag_x(g, zz).wait_recv()
            add(own[g].at[zz, 1 - y, x, :, columns(shapes[g], 0)], from_dx[g].at[zz])
            y_copy(g, zz).start()

        def take_y(full):
            part = slice(None) if full else columns(shapes[g], 1)
            diag_y(g, zz, full).wait_recv()
            add(own[g].at[zz, y, 1 - x, :, part], from_dy[g].at[zz, :, part])
            x_copy(g, zz).start()

        if not with_tiles:
            take_x()
            take_y(False)
            return

        @pl.when(x == 0)
        def _():
            take_y(False)

        @pl.when(x == 1)
        def _():
            take_x()
            take_y(True)

    def stage_line(g, t):
        zz = visit(t, z, planes)
        x_copy(g, zz).wait_recv()
        y_copy(g, zz).wait_recv()
        here = own[g].at[zz, y, x]

        @pl.when(t > 0)
        def _():
            add(here, from_x[g].at[zz], from_y[g].at[zz])
            farther = jnp.where(zz > z, z > 0, z < planes - 1)

            @pl.when(farther)
            def _():
                z_arrival(g, zz).wait_recv()
                add(here, from_z[g].at[zz])

            @pl.when(zz > z)
            def _():
                z_copy(g, zz, True).start()

            @pl.when(zz < z)
            def _():
                z_copy(g, zz, False).start()

        @pl.when(t == 0)
        def _():
            outs[g][...] = (
                here[...].astype(f32)
                + from_x[g][zz].astype(f32)
                + from_y[g][zz].astype(f32)
            )

            @pl.when(z > 0)
            def _():
                z_arrival(g, zz).wait_recv()
                outs[g][...] += from_z[g][zz].astype(f32)

            @pl.when(z < planes - 1)
            def _():
                z_arrival(g, planes).wait_recv()
                outs[g][...] += from_z[g][planes].astype(f32)

    @pl.loop(0, planes + 2)
    def _(r):
        t = planes - 1 - r
        for g in range(n):

            @pl.when(r < planes)
            def _():
                stage_core(g, t)

            @pl.when((r >= 1) & (r < planes + 1))
            def _():
                stage_plane(g, t + 1)

            @pl.when(r >= 2)
            def _():
                stage_line(g, t + 2)

            if with_tiles and g % 2 == 0:
                work(r * 2 + g // 2)

    @pl.loop(0, planes)
    def _(r):
        t = planes - 1 - r
        zz = visit(t, z, planes)
        for g in range(n):
            core_copy(g, zz).wait_send()

            def even():
                diag_x(g, zz).wait_send()
                diag_y(g, zz, False).wait_send()

            lean_or_even(lambda: diag_y(g, zz, True).wait_send(), even)
            x_copy(g, zz).wait_send()
            y_copy(g, zz).wait_send()

            @pl.when(t > 0)
            def _():
                z_copy(g, zz, True).wait_send()

    if with_tiles:
        for s in range(seqs):
            send_b(s).wait()

            @pl.when(x == 0)
            def _():
                send_back(s).wait_recv()

            @pl.when(x == 1)
            def _():
                send_d(s).wait_send()
                send_back(s).wait_send()

        @pl.when(x == 1)
        def _():
            chip[...] = jnp.zeros_like(chip)

        @pl.loop(0, seqs * rows // 32)
        def _(i):
            seq = lax.div(i, rows // 32)
            at = pl.ds(pl.multiple_of(lax.rem(i, rows // 32) * 32, 32), 32)
            flat = pl.ds(pl.multiple_of(i * 32, 32), 32)
            cos_rows, sin_rows = cos_table[flat, :], sin_table[flat, :]
            for k in range(pairs):
                lanes = pl.ds(k * 128, 128)

                def summed(kind):
                    return (
                        mine[kind, seq, at, lanes].astype(f32)
                        + from_b[kind, seq, at, lanes].astype(f32)
                        + chip[kind, seq, at, lanes].astype(f32)
                    )

                d_key[flat, lanes] = turned(summed(0), cos_rows, sin_rows, -1.0).astype(jnp.bfloat16)
                half = 0.5 * summed(1)
                d_value[flat, lanes] = half.astype(jnp.bfloat16)
                first_grad[flat, lanes] = half


def scatter_sum(planes, partials, collective_id, attention=None):
    n = len(partials)
    partials = [
        p.reshape(planes, 2, 2, 2, p.shape[0] // (planes * 8), p.shape[1]) for p in partials
    ]
    shapes = [p.shape[4:] for p in partials]
    types = [p.dtype for p in partials]
    dma = pltpu.SemaphoreType.DMA

    def boxes(lead, narrow=False):
        out = []
        for s, d in zip(shapes, types):
            width = s[1] // 2 // 128 * 128 if narrow else s[1]
            out.append(pltpu.VMEM((*lead, s[0], width), d))
        return out

    extra, extra_out, extra_scratch = [], [], []
    if attention is not None:
        extra = list(attention)
        box = attention[2].shape
        seqs, rows, width = box[1:]
        flat = (seqs * rows, width)
        extra_out = [
            jax.ShapeDtypeStruct(box[1:], jnp.bfloat16),
            jax.ShapeDtypeStruct(flat, jnp.bfloat16),
            jax.ShapeDtypeStruct(flat, jnp.bfloat16),
            jax.ShapeDtypeStruct(flat, jnp.float32),
        ]
        extra_scratch = [
            *[pltpu.VMEM(box, jnp.bfloat16)] * 6,
            dma((3, seqs)),
            dma((3, seqs)),
            *attend_back_scratch(rows),
        ]
    return pl.pallas_call(
        functools.partial(scatter_kernel, planes, shapes, bool(extra)),
        out_shape=[jax.ShapeDtypeStruct(s, jnp.float32) for s in shapes] + extra_out,
        in_specs=[pl.BlockSpec(memory_space=pl.ANY)] * n
        + [pl.BlockSpec(memory_space=pltpu.VMEM)] * len(extra),
        out_specs=[pl.BlockSpec(memory_space=pltpu.VMEM)] * (n + len(extra_out)),
        scratch_shapes=[
            *boxes((planes, 2, 2)),
            *boxes((planes, 2, 2)),
            *boxes((planes,), True),
            *boxes((planes,)),
            *boxes((planes,)),
            *boxes((planes,)),
            *boxes((planes + 1,)),
            dma((n, planes)),
            dma((n, planes)),
            dma((n, planes)),
            dma((n, planes, 2)),
            dma((n, planes, 2)),
            dma((n, planes)),
            dma((n, planes)),
            dma((n, planes)),
            dma((n, planes)),
            dma((n, planes)),
            dma((n, planes + 1)),
            *extra_scratch,
        ],
        compiler_params=pltpu.CompilerParams(
            collective_id=collective_id, has_side_effects=True, vmem_limit_bytes=67043328
        ),
        name="gradient_scatter",
    )(*partials, *extra)


def on_device(
    planes,
    tokens,
    first_values,
    cotangent,
    segment_ids,
    attn_gain,
    w_query,
    w_key,
    w_value,
    w_out,
    ffn_gain,
    gate_weight,
    up_weight,
    down_weight,
):
    f32, bf16 = jnp.float32, jnp.bfloat16
    devices = planes * 8
    seqs, rows, width = tokens.shape
    rank = lax.axis_index("ctx")
    share = attn_gain.shape[0]
    per = 128 // share
    place = lax.rem(lax.axis_index("dp") * lax.axis_size("ctx") + rank, per)
    here = jnp.arange(128, dtype=jnp.int32) // share == place
    spread = lambda gain: jnp.where(here, jnp.tile(gain, per), jnp.zeros((), bf16))
    gains = jnp.zeros((16, 128), bf16).at[0].set(spread(attn_gain)).at[1].set(spread(ffn_gain))
    starts, cos_table, sin_table = tables(segment_ids, rank, rows)
    flat = (seqs * rows, width)
    local = (seqs, rows, width)
    tokens = tokens.reshape(flat)
    mm = functools.partial(jnp.dot, preferred_element_type=f32)
    by_rows = lambda a, b: lax.dot_general(a, b, TN, preferred_element_type=f32).astype(bf16)
    back = lambda a, b: lax.dot_general(a, b, NT, preferred_element_type=f32)
    (gains, w_query, w_key, w_value, w_out, gate_weight, up_weight, down_weight), (
        normed_one,
        query_rot,
        *tiles,
        context3,
        log_total,
    ) = forward(
        planes,
        4,
        [gains, w_query, w_key, w_value, w_out, gate_weight, up_weight, down_weight],
        tokens,
        first_values.reshape(flat),
        starts,
        cos_table,
        sin_table,
    )
    gains = jnp.sum(gains.reshape(width // 128, per, 16, 128), axis=1)
    attn_gain = gains[:, 0].reshape(1, width)
    ffn_gain = gains[:, 1].reshape(1, width)
    context = context3.reshape(flat)
    tokens_float = tokens.astype(f32)
    scale_one = inverse_rms(tokens_float)
    cotangent = cotangent.reshape(flat)
    residual = tokens_float + mm(context, w_out)
    scale_two = inverse_rms(residual)
    second_normed = (residual * scale_two * ffn_gain.astype(f32)).astype(bf16)
    gate = mm(second_normed, gate_weight)
    up = mm(second_normed, up_weight)
    hidden = (swish(gate) * up).astype(bf16)
    output = (residual + mm(hidden, down_weight)).astype(bf16)

    out_float = cotangent.astype(f32)
    d_down = by_rows(hidden, cotangent)
    d_hidden = back(cotangent, down_weight)
    sigmoid_gate = jax.nn.sigmoid(gate)
    d_gate = (d_hidden * up * sigmoid_gate * (1.0 + gate * (1.0 - sigmoid_gate))).astype(bf16)
    d_up = (d_hidden * (gate * sigmoid_gate)).astype(bf16)
    d_gate_weight = by_rows(second_normed, d_gate)
    d_up_weight = by_rows(second_normed, d_up)
    d_normed_two = back(d_gate, gate_weight) + back(d_up, up_weight)
    d_ffn_gain = jnp.sum(d_normed_two * residual * scale_two, axis=0)
    weighted_two = d_normed_two * ffn_gain.astype(f32)
    d_residual = (
        out_float
        + scale_two * weighted_two
        - residual
        * (scale_two * scale_two * scale_two)
        * jnp.mean(weighted_two * residual, axis=-1, keepdims=True)
    )
    d_residual_low = d_residual.astype(bf16)
    d_out = by_rows(context, d_residual_low)
    d_context = back(d_residual_low, w_out).astype(bf16).reshape(local)
    s_down, s_gate, s_up, s_out, d_query, d_key, d_value, first_grad = scatter_sum(
        planes,
        [d_down, d_gate_weight, d_up_weight, d_out],
        2,
        [starts, query_rot, *tiles, context3, d_context, log_total, cos_table, sin_table],
    )
    d_query = d_query.reshape(flat)
    d_wq = by_rows(normed_one, d_query)
    d_wk = by_rows(normed_one, d_key)
    d_wv = by_rows(normed_one, d_value)
    d_normed_one = back(d_query, w_query) + back(d_key, w_key) + back(d_value, w_value)
    d_attn_gain = jnp.sum(d_normed_one * tokens_float * scale_one, axis=0)
    weighted_one = d_normed_one * attn_gain.astype(f32)
    token_grad = (
        d_residual
        + scale_one * weighted_one
        - tokens_float
        * (scale_one * scale_one * scale_one)
        * jnp.mean(weighted_one * tokens_float, axis=-1, keepdims=True)
    )
    d_gains = jnp.stack([d_attn_gain, d_ffn_gain]).reshape(2, devices, share)
    d_gains = jnp.zeros((devices, 8, 256), f32).at[:, :2, :share].set(d_gains.transpose(1, 0, 2))
    s_wq, s_wk, s_wv, s_gains = scatter_sum(
        planes, [d_wq, d_wk, d_wv, d_gains.reshape(devices * 8, 256)], 3
    )
    return (
        output.reshape(local),
        token_grad.reshape(local),
        first_grad.reshape(local),
        s_gains[0, :share],
        s_wq,
        s_wk,
        s_wv,
        s_out,
        s_gains[1, :share],
        s_gate,
        s_up,
        s_down,
    )


def solution(mesh):
    token, weight, vector = P("dp", "ctx", None), P(("dp", "ctx"), None), P(("dp", "ctx"))
    return jax.shard_map(
        functools.partial(on_device, mesh.shape["dp"] // 2),
        mesh=mesh,
        in_specs=(
            token,
            token,
            token,
            P("dp", None),
            vector,
            weight,
            weight,
            weight,
            weight,
            vector,
            weight,
            weight,
            weight,
        ),
        out_specs=(
            token,
            token,
            token,
            vector,
            weight,
            weight,
            weight,
            weight,
            vector,
            weight,
            weight,
            weight,
        ),
        check_vma=False,
    )
```

```python
import functools
import jax
import jax.numpy as jnp
from jax import lax
from jax.experimental import pallas as pl
from jax.experimental.pallas import tpu as pltpu
from jax.sharding import PartitionSpec as P

HEADS = 16
HEAD_DIM = 64
MESH_ID = pl.DeviceIdType.MESH

epsilon = 1e-05
rope_base = 10000.0
score_scale = 0.125
masked_score = -1e30


def inverse_rms(values):
    return lax.rsqrt(jnp.mean(values * values, axis=-1, keepdims=True) + epsilon)


def swish(values):
    return values * jax.nn.sigmoid(values)


def first_half(shape):
    return lax.broadcasted_iota(jnp.int32, shape, len(shape) - 1) % HEAD_DIM < HEAD_DIM // 2


def swap_halves(values):
    return jnp.where(
        first_half(values.shape), pltpu.roll(values, 96, 1), pltpu.roll(values, 32, 1)
    )


def turned(values, cos_table, sin_table, sign):
    return values * cos_table + sign * (swap_halves(values) * sin_table)


def tables(segment_ids, rank, rows):
    seqs, length = segment_ids.shape
    places = jnp.arange(length, dtype=jnp.int32)
    edges = jnp.concatenate(
        [jnp.ones((seqs, 1), dtype=jnp.bool_), segment_ids[:, 1:] != segment_ids[:, :-1]], axis=1
    )
    starts = lax.cummax(jnp.where(edges, places[None, :], 0), axis=1)
    starts = lax.dynamic_slice_in_dim(starts, rank * rows, rows, 1)
    local = rank * rows + jnp.arange(rows, dtype=jnp.int32) - starts
    lane = jnp.arange(128, dtype=jnp.int32)
    half = HEAD_DIM // 2
    frequency = rope_base ** (-(lane % half).astype(jnp.float32) * 2.0 / HEAD_DIM)
    angles = local.astype(jnp.float32).reshape(seqs * rows, 1) * frequency
    sign = jnp.where(lane % HEAD_DIM < half, -1.0, 1.0)
    return starts.reshape(seqs, 1, rows), jnp.cos(angles), jnp.sin(angles) * sign


def normalise(tok, gain, normed):
    rows = tok.shape[0]

    @pl.loop(0, rows // 64)
    def _(i):
        at = pl.ds(pl.multiple_of(i * 64, 64), 64)
        values = tok[at, :].astype(jnp.float32)
        normed[at, :] = (values * inverse_rms(values) * gain).astype(jnp.bfloat16)


def columns_of(weight, lanes):
    block = weight[:, :, lanes]
    if block.shape[1] % 16:
        block = block.astype(jnp.float32)
    return block.reshape(block.shape[0] * block.shape[1], block.shape[2]).astype(jnp.bfloat16)


def project(normed, first, wq, wk, wv, cos_ref, sin_ref, query, pair):
    f32, bf16 = jnp.float32, jnp.bfloat16
    seqs, rows, width = query.shape

    @pl.loop(0, width // 256)
    def _(i):
        lanes = pl.ds(pl.multiple_of(i * 256, 256), 256)
        n1 = normed[...]
        cos_table, sin_table = cos_ref[...], sin_ref[...]
        queries = jnp.dot(n1, columns_of(wq, lanes), preferred_element_type=f32)
        keys = jnp.dot(n1, columns_of(wk, lanes), preferred_element_type=f32)
        values = jnp.dot(n1, columns_of(wv, lanes), preferred_element_type=f32)
        mixed = (0.5 * values + 0.5 * first[:, lanes].astype(f32)).astype(bf16)
        for half in range(2):
            part = slice(half * 128, half * 128 + 128)
            at = pl.ds(pl.multiple_of(i * 256 + half * 128, 128), 128)
            q = turned(queries[:, part], cos_table, sin_table, 1.0).astype(bf16)
            k = turned(keys[:, part], cos_table, sin_table, 1.0).astype(bf16)
            for s in range(seqs):
                query[s, :, at] = q[s * rows : (s + 1) * rows]
                pair[0, s, :, at] = k[s * rows : (s + 1) * rows]
                pair[1, s, :, at] = mixed[s * rows : (s + 1) * rows, part]


def two_heads(block, scale):
    lane = lax.broadcasted_iota(jnp.int32, block.shape, 1)
    scaled = block * jnp.asarray(scale, block.dtype)
    zero = jnp.zeros_like(block)
    return jnp.concatenate(
        [jnp.where(lane < HEAD_DIM, scaled, zero), jnp.where(lane < HEAD_DIM, zero, scaled)]
    )


def own_lanes(both):
    rows = both.shape[1] // 2
    lane = lax.broadcasted_iota(jnp.int32, (both.shape[0], rows), 0)
    return jnp.where(lane < HEAD_DIM, both[:, :rows], both[:, rows:]).T


def fill_bias(bias, starts, rank):
    rows = bias.shape[1]
    key = lax.broadcasted_iota(jnp.int32, (rows, rows), 0)
    place = rank * rows + lax.broadcasted_iota(jnp.int32, (rows, rows), 1)
    begin = starts[...]
    for t in range(4):
        x, c = lax.div(rank, 2), lax.rem(rank, 2)
        owner = (1 - x if t >= 2 else x) * 2 + (1 - c if t % 2 else c)
        at = owner * rows + key
        bias[t] = jnp.where((at >= begin) & (at <= place), 0.0, masked_score)


NT = (((1,), (1,)), ((), ()))
TN = (((0,), (0,)), ((), ()))


def attend_step(rank, begin, starts, q, tiles, out, log_total, bias, scores, peak, total, acc):
    f32, bf16 = jnp.float32, jnp.bfloat16

    @pl.when(begin)
    def _():
        fill_bias(bias, starts, rank)

    high = rank >= 2
    stacked = two_heads(q, score_scale)

    def score(t):
        s = lax.dot_general(tiles[t][0][...], stacked, NT, preferred_element_type=f32)
        s = s + jnp.concatenate([bias[t], bias[t]], axis=1)
        scores[t] = s
        return jnp.max(s, axis=0, keepdims=True)

    def gather_values(t, top):
        e = jnp.exp(scores[t] - top)
        part = lax.dot_general(tiles[t][1][...], e.astype(bf16), TN, preferred_element_type=f32)
        return jnp.sum(e, axis=0, keepdims=True), part

    peak[...] = jnp.maximum(score(0), score(1))

    @pl.when(high)
    def _():
        peak[...] = jnp.maximum(peak[...], jnp.maximum(score(2), score(3)))

    top = peak[...]
    sum_a, acc_a = gather_values(0, top)
    sum_b, acc_b = gather_values(1, top)
    total[...] = sum_a + sum_b
    acc[...] = acc_a + acc_b

    @pl.when(high)
    def _():
        top = peak[...]
        sum_a, acc_a = gather_values(2, top)
        sum_b, acc_b = gather_values(3, top)
        total[...] += sum_a + sum_b
        acc[...] += acc_a + acc_b

    out[...] = own_lanes(acc[...] / total[...]).astype(bf16)
    log_total[...] = peak[...] + jnp.log(total[...])


def attend_scratch(rows):
    return [
        pltpu.VMEM((4, rows, rows), jnp.float32),
        pltpu.VMEM((4, rows, 2 * rows), jnp.float32),
        pltpu.VMEM((1, 2 * rows), jnp.float32),
        pltpu.VMEM((1, 2 * rows), jnp.float32),
        pltpu.VMEM((128, 2 * rows), jnp.float32),
    ]


def attend_back_step(
    rank, begin, starts, q, tiles, context, d_context, log_total, cos_t, sin_t, d_q, d_tiles, bias, acc
):
    f32, bf16 = jnp.float32, jnp.bfloat16

    @pl.when(begin)
    def _():
        fill_bias(bias, starts, rank)

    high = rank >= 2
    stacked = two_heads(q, score_scale)
    stacked_do = two_heads(d_context, 1.0)
    turned_product = (d_context.astype(f32) * context.astype(f32)).T
    delta = jnp.concatenate(
        [
            jnp.sum(turned_product[:HEAD_DIM], axis=0, keepdims=True),
            jnp.sum(turned_product[HEAD_DIM:], axis=0, keepdims=True),
        ],
        axis=1,
    )
    lse = log_total[...]

    def one(t):
        keys, values = tiles[t][0][...], tiles[t][1][...]
        s = lax.dot_general(keys, stacked, NT, preferred_element_type=f32)
        s = s + jnp.concatenate([bias[t], bias[t]], axis=1)
        p = jnp.exp(s - lse)
        dp = lax.dot_general(values, stacked_do, NT, preferred_element_type=f32)
        ds = (p * (dp - delta)).astype(bf16)
        d_tiles[t][1][...] = jnp.dot(p.astype(bf16), stacked_do, preferred_element_type=f32).astype(bf16)
        d_tiles[t][0][...] = jnp.dot(ds, stacked, preferred_element_type=f32).astype(bf16)
        return lax.dot_general(keys, ds, TN, preferred_element_type=f32)

    acc[...] = one(0) + one(1)

    @pl.when(high)
    def _():
        acc[...] += one(2) + one(3)

    d_q[...] = turned(own_lanes(acc[...]) * score_scale, cos_t[...], sin_t[...], -1.0).astype(bf16)


def attend_back_scratch(rows):
    return [pltpu.VMEM((4, rows, rows), jnp.float32), pltpu.VMEM((128, 2 * rows), jnp.float32)]


def position():
    dp = lax.axis_index("dp")
    ct = lax.axis_index("ctx")
    return lax.div(dp, 2), lax.rem(dp, 2), lax.div(ct, 2), lax.rem(ct, 2)


def visit(step, z, planes):
    back = planes - 1 - step
    high = back + jnp.where(back >= z, 1, 0)
    low = planes - 1 - back
    low = low - jnp.where(low <= z, 1, 0)
    other = jnp.where(z < planes // 2, low, high)
    return jnp.where(step == 0, z, other)


def device(z, y, x, c):
    return (z * 2 + y, x * 2 + c)


def halves(shape):
    if shape[0] % 2 == 0:
        cut = shape[0] // 2
        return (pl.ds(0, cut), slice(None), slice(None)), (pl.ds(cut, cut), slice(None), slice(None))
    cut = shape[2] // 2 // 128 * 128
    return (
        (slice(None), slice(None), pl.ds(0, cut)),
        (slice(None), slice(None), pl.ds(cut, shape[2] - cut)),
    )


def entry_barrier(z, y, x, c, planes):
    barrier = pltpu.get_barrier_semaphore()

    def hello(target):
        pl.semaphore_signal(barrier, inc=1, device_id=target, device_id_type=MESH_ID)

    hello(device(z, y, 1 - x, c))
    hello(device(z, 1 - y, x, c))
    hello(device(z, y, x, 1 - c))

    @pl.when(z > 0)
    def _():
        hello(device(z - 1, y, x, c))

    @pl.when(z < planes - 1)
    def _():
        hello(device(z + 1, y, x, c))

    pl.semaphore_wait(barrier, 3 + jnp.where(z > 0, 1, 0) + jnp.where(z < planes - 1, 1, 0))


def forward_kernel(planes, shapes, first_group, *refs):
    n = len(shapes)
    ins, refs = refs[:n], refs[n:]
    tok, first, starts, cos_table, sin_table = refs[:5]
    outs, refs = refs[5 : 5 + n], refs[5 + n :]
    normed, query, mine, near, chip, far, context, log_total = refs[:8]
    sems, refs = refs[8:19], refs[19:]
    own_sem, z_send, z_recv, x_send, x_recv, y_send, y_recv, d_send, d_recv, c_send, c_recv = sems
    tile_send, tile_recv, load_sem, gains, *weights = refs[: 4 + first_group - 1]
    scratch = refs[4 + first_group - 1 :]
    z, y, x, c = position()
    entry_barrier(z, y, x, c, planes)
    local = [
        pltpu.make_async_copy(ins[g], outs[g].at[:, z, y, x, c], own_sem.at[g]) for g in range(n)
    ]
    for copy in local:
        copy.start()

    def push(src, dst, send, recv, target):
        return pltpu.make_async_remote_copy(
            src_ref=src,
            dst_ref=dst,
            send_sem=send,
            recv_sem=recv,
            device_id=target,
            device_id_type=MESH_ID,
        )

    def spot(g, zz, yy, xx):
        return outs[g].at[:, zz, yy, xx, c]

    def z_copy(g, zz, up, own):
        side = 1 if up else 0
        return push(
            ins[g] if own else spot(g, zz, y, x),
            spot(g, zz, y, x),
            z_send.at[g, zz, side],
            z_recv.at[g, zz],
            device(z + 1 if up else z - 1, y, x, c),
        )

    def x_copy(g, zz, own):
        return push(
            ins[g] if own else spot(g, zz, y, x),
            spot(g, zz, y, x),
            x_send.at[g, zz],
            x_recv.at[g, zz],
            device(z, y, 1 - x, c),
        )

    def y_copy(g, zz, own):
        return push(
            ins[g] if own else spot(g, zz, y, x),
            spot(g, zz, y, x),
            y_send.at[g, zz],
            y_recv.at[g, zz],
            device(z, 1 - y, x, c),
        )

    def relay(g, zz, half, by_y):
        here = spot(g, zz, y, 1 - x) if by_y else spot(g, zz, 1 - y, x)
        here = here.at[halves(shapes[g])[half]]
        return push(
            here,
            here,
            d_send.at[g, zz, 2 * half if by_y else 1],
            d_recv.at[g, zz, half],
            device(z, 1 - y, x, c) if by_y else device(z, y, 1 - x, c),
        )

    def diag_arrival(g, zz, half):
        here = spot(g, zz, 1 - y, 1 - x).at[halves(shapes[g])[half]]
        return push(
            here, here, d_send.at[g, zz, half], d_recv.at[g, zz, half], device(z, y, x, 1 - c)
        )

    def core_copy(g, zz, mine):
        here = outs[g].at[:, zz, :, :, c if mine else 1 - c]
        return push(here, here, c_send.at[g, zz], c_recv.at[g, zz], device(z, y, x, 1 - c))

    def on_links(g, t, act):
        zz = visit(t, z, planes)

        def both(own):
            up = (z < planes - 1) if own else (zz < z) & (z < planes - 1)
            down = (z > 0) if own else (zz > z) & (z > 0)
            pl.when(down)(lambda: act(z_copy(g, zz, False, own)))
            pl.when(up)(lambda: act(z_copy(g, zz, True, own)))
            act(x_copy(g, zz, own))
            act(y_copy(g, zz, own))

        pl.when(t == 0)(lambda: both(True))
        pl.when(t > 0)(lambda: both(False))

    def on_relays(g, t, act, between=lambda: None):
        zz = visit(t, z, planes)
        act(relay(g, zz, 0, True))
        if g < first_group:
            between()
            act(relay(g, zz, 1, False))
            return
        lean = t > 0
        pl.when(lean & (x == 1))(lambda: act(relay(g, zz, 1, True)))
        between()
        pl.when((x == 1) | jnp.logical_not(lean))(lambda: act(relay(g, zz, 1, False)))

    def start(copy):
        copy.start()

    def wait_send(copy):
        copy.wait_send()

    def stage_line(g, t):
        @pl.when(t > 0)
        def _():
            z_copy(g, visit(t, z, planes), True, False).wait_recv()

        on_links(g, t, start)

    def stage_plane(g, t):
        zz = visit(t, z, planes)
        x_copy(g, zz, False).wait_recv()
        on_relays(g, t, start, lambda: y_copy(g, zz, False).wait_recv())

    def stage_core(g, t):
        zz = visit(t, z, planes)
        pl.when(t == 0)(lambda: local[g].wait())
        diag_arrival(g, zz, 0).wait_recv()
        diag_arrival(g, zz, 1).wait_recv()
        core_copy(g, zz, True).start()

    seqs, rows, width = query.shape
    pairs = width // 128
    partner = device(z, y, x, 1 - c)

    def to_partner(s):
        return push(
            mine.at[:, s], near.at[:, s], tile_send.at[0, s], tile_recv.at[0, s], partner
        )

    def to_x(s):
        return push(
            mine.at[:, s],
            chip.at[:, s],
            tile_send.at[1, s],
            tile_recv.at[1, s],
            device(z, y, 1 - x, c),
        )

    def passed_on(s):
        return push(
            chip.at[:, s], far.at[:, s], tile_send.at[2, s], tile_recv.at[2, s], partner
        )

    def send_tiles(s):
        to_partner(s).start()
        pl.when(x == 0)(lambda: to_x(s).start())

    def projection():
        @pl.loop(0, planes)
        def _(t):
            for g in range(first_group):
                core_copy(g, visit(t, z, planes), False).wait_recv()

        loads = [
            pltpu.make_async_copy(outs[g].at[0], buf, load_sem.at[g])
            for g, buf in enumerate([gains, *weights])
        ]
        for copy in loads:
            copy.start()
        loads[0].wait()
        flat_gains = [gains[i, j, k, m] for i in range(planes) for j in (0, 1) for k in (0, 1) for m in (0, 1)]
        per = len(flat_gains) * 128 // width
        gain = jnp.concatenate(
            [
                sum(b[:1].astype(jnp.float32) for b in flat_gains[i * per : (i + 1) * per])
                for i in range(width // 128)
            ],
            axis=1,
        )
        normalise(tok, gain, normed)
        for copy in loads[1:]:
            copy.wait()
        as_blocks = lambda w: w.reshape((planes * 8, *w.shape[4:]))
        project(
            normed, first, *[as_blocks(w) for w in weights], cos_table, sin_table, query, mine
        )
        for s in range(seqs):
            send_tiles(s)

    def unit(s, p):
        lanes = pl.ds(pl.multiple_of(p * 128, 128), 128)
        attend_step(
            lax.axis_index("ctx"),
            p == 0,
            starts.at[s],
            query[s, :, lanes],
            [[w.at[0, s, :, lanes], w.at[1, s, :, lanes]] for w in (mine, near, chip, far)],
            context.at[s, :, lanes],
            log_total.at[s, p],
            *scratch,
        )

    def attention():
        @pl.loop(0, seqs)
        def _(s):
            to_partner(s).wait_recv()

            @pl.when(x == 1)
            def _():
                to_x(s).wait_recv()
                passed_on(s).start()
                passed_on(s).wait_recv()

            @pl.loop(0, pairs)
            def _(p):
                unit(s, p)

    groups = (range(first_group), range(first_group, n))

    @pl.loop(0, 2 * planes + 2)
    def _(r):
        for stage, lag in ((stage_line, 0), (stage_plane, 1), (stage_core, 2)):
            for k, group in enumerate(groups):
                t = r - k * planes - lag
                for g in group:
                    pl.when((t >= 0) & (t < planes))(lambda: stage(g, t))
            if lag == 0:
                pl.when(r == planes + 3)(attention)
        pl.when(r == planes + 1)(projection)

    @pl.loop(0, planes)
    def _(t):
        zz = visit(t, z, planes)
        for g in range(n):
            if g >= first_group:
                core_copy(g, zz, False).wait_recv()
            core_copy(g, zz, True).wait_send()
            on_links(g, t, wait_send)
            on_relays(g, t, wait_send)

    for s in range(seqs):
        to_partner(s).wait_send()
        pl.when(x == 0)(lambda: to_x(s).wait_send())
        pl.when(x == 1)(lambda: passed_on(s).wait_send())


def forward(planes, first_group, blocks, tok, first, starts, cos_table, sin_table):
    blocks = [b[None] for b in blocks]
    n = len(blocks)
    shapes = [b.shape for b in blocks]
    seqs, _, rows = starts.shape
    width = tok.shape[1]
    bf16 = jnp.bfloat16
    dma = pltpu.SemaphoreType.DMA
    anywhere = pl.BlockSpec(memory_space=pl.ANY)
    vmem = pl.BlockSpec(memory_space=pltpu.VMEM)
    local = jax.ShapeDtypeStruct((seqs, rows, width), bf16)
    tile = jax.ShapeDtypeStruct((2, seqs, rows, width), bf16)
    got = pl.pallas_call(
        functools.partial(forward_kernel, planes, shapes, first_group),
        out_shape=[
            jax.ShapeDtypeStruct((s[0], planes, 2, 2, 2, s[1], s[2]), b.dtype)
            for s, b in zip(shapes, blocks)
        ]
        + [jax.ShapeDtypeStruct(tok.shape, bf16), local, *[tile] * 4, local]
        + [jax.ShapeDtypeStruct((seqs, width // 128, 1, 2 * rows), jnp.float32)],
        in_specs=[anywhere] * n + [vmem] * 5,
        out_specs=[anywhere] * n + [vmem] * 8,
        scratch_shapes=[
            dma((n,)),
            dma((n, planes, 2)),
            dma((n, planes)),
            dma((n, planes)),
            dma((n, planes)),
            dma((n, planes)),
            dma((n, planes)),
            dma((n, planes, 3)),
            dma((n, planes, 2)),
            dma((n, planes)),
            dma((n, planes)),
            dma((3, seqs)),
            dma((3, seqs)),
            dma((first_group,)),
            *[pltpu.VMEM((planes, 2, 2, 2, *s[1:]), bf16) for s in shapes[:first_group]],
            *attend_scratch(rows),
        ],
        compiler_params=pltpu.CompilerParams(
            collective_id=0, has_side_effects=True, vmem_limit_bytes=67043328
        ),
        name="forward",
    )(*blocks, tok, first, starts, cos_table, sin_table)
    full = [g.reshape(planes * 8 * s[1], s[2]) for g, s in zip(got, shapes)]
    return full, got[n:]


def columns(shape, half):
    cut = shape[1] // 2 // 128 * 128
    return pl.ds(0, cut) if half == 0 else pl.ds(cut, shape[1] - cut)


class Reduction:
    def __init__(self, **steps):
        self.__dict__.update(steps)


def reduction(planes, shapes, routed, own_at, away_at, before_core, boxes, sems, outs):
    n = len(shapes)
    from_core, from_dx, from_dy, from_x, from_y, from_z = (
        boxes[k * n : (k + 1) * n] for k in range(6)
    )
    c_send, c_recv, d_send, d_recv, x_send, x_recv, y_send, y_recv, z_send, z_recv = sems
    z, y, x, c = position()

    def push(src, dst, send, recv, target):
        return pltpu.make_async_remote_copy(
            src_ref=src,
            dst_ref=dst,
            send_sem=send,
            recv_sem=recv,
            device_id=target,
            device_id_type=MESH_ID,
        )

    f32 = jnp.float32

    def add(dst, *srcs):
        total = dst[...].astype(f32)
        for src in srcs:
            total = total + src[...].astype(f32)
        dst[...] = total.astype(dst.dtype)

    def core_copy(g, zz):
        return push(
            away_at(g, zz),
            from_core[g].at[zz],
            c_send.at[g, zz],
            c_recv.at[g, zz],
            device(z, y, x, 1 - c),
        )

    def diag_x(g, zz):
        return push(
            own_at(g, zz, 1 - y, 1 - x).at[:, columns(shapes[g], 0)],
            from_dx[g].at[zz],
            d_send.at[g, zz, 0],
            d_recv.at[g, zz, 0],
            device(z, y, 1 - x, c),
        )

    def diag_y(g, zz, full):
        part = slice(None) if full else columns(shapes[g], 1)
        return push(
            own_at(g, zz, 1 - y, 1 - x).at[:, part],
            from_dy[g].at[zz, :, part],
            d_send.at[g, zz, 1],
            d_recv.at[g, zz, 1],
            device(z, 1 - y, x, c),
        )

    def x_copy(g, zz):
        return push(
            own_at(g, zz, y, 1 - x),
            from_x[g].at[zz],
            x_send.at[g, zz],
            x_recv.at[g, zz],
            device(z, y, 1 - x, c),
        )

    def y_copy(g, zz):
        return push(
            own_at(g, zz, 1 - y, x),
            from_y[g].at[zz],
            y_send.at[g, zz],
            y_recv.at[g, zz],
            device(z, 1 - y, x, c),
        )

    def z_copy(g, zz, up):
        slot = zz if up else jnp.where(zz == z - 1, planes, zz)
        return push(
            own_at(g, zz, y, x),
            from_z[g].at[slot],
            z_send.at[g, zz],
            z_recv.at[g, slot],
            device(z + 1 if up else z - 1, y, x, c),
        )

    def z_arrival(g, slot):
        return push(
            from_z[g].at[slot],
            from_z[g].at[slot],
            z_send.at[g, 0],
            z_recv.at[g, slot],
            device(z, y, x, 1 - c),
        )

    def lean_or_even(t, lean, even):
        if not routed:
            even()
            return
        is_lean = (x == 1) & (t < planes - 2)
        pl.when(jnp.logical_not(is_lean))(even)
        pl.when(is_lean)(lean)

    def stage_core(g, t):
        zz = visit(t, z, planes)
        before_core(g, zz)
        core_copy(g, zz).wait_recv()
        add(own_at(g, zz, 1 - y, 1 - x), from_core[g].at[zz, 1 - y, 1 - x])

        def even():
            diag_x(g, zz).start()
            diag_y(g, zz, False).start()

        lean_or_even(t, lambda: diag_y(g, zz, True).start(), even)
        add(own_at(g, zz, 1 - y, x), from_core[g].at[zz, 1 - y, x])
        if routed:

            @pl.when((x == 0) & (t < planes - 2))
            def _():
                y_copy(g, zz).start()

        add(own_at(g, zz, y, 1 - x), from_core[g].at[zz, y, 1 - x])
        add(own_at(g, zz, y, x), from_core[g].at[zz, y, x])

    def stage_plane(g, t):
        zz = visit(t, z, planes)

        def take_x():
            diag_x(g, zz).wait_recv()
            add(own_at(g, zz, 1 - y, x).at[:, columns(shapes[g], 0)], from_dx[g].at[zz])
            y_copy(g, zz).start()

        def take_y(full):
            part = slice(None) if full else columns(shapes[g], 1)
            diag_y(g, zz, full).wait_recv()
            add(own_at(g, zz, y, 1 - x).at[:, part], from_dy[g].at[zz, :, part])
            x_copy(g, zz).start()

        if not routed:
            take_x()
            take_y(False)
            return
        lean = t < planes - 2
        pl.when((x == 1) | jnp.logical_not(lean))(take_x)
        pl.when((x == 1) & lean)(lambda: take_y(True))
        pl.when((x == 0) | jnp.logical_not(lean))(lambda: take_y(False))

    def stage_line(g, t):
        zz = visit(t, z, planes)
        x_copy(g, zz).wait_recv()
        y_copy(g, zz).wait_recv()
        here = own_at(g, zz, y, x)

        @pl.when(t > 0)
        def _():
            add(here, from_x[g].at[zz], from_y[g].at[zz])
            farther = jnp.where(zz > z, z > 0, z < planes - 1)

            @pl.when(farther)
            def _():
                z_arrival(g, zz).wait_recv()
                add(here, from_z[g].at[zz])

            @pl.when(zz > z)
            def _():
                z_copy(g, zz, True).start()

            @pl.when(zz < z)
            def _():
                z_copy(g, zz, False).start()

        @pl.when(t == 0)
        def _():
            outs[g][...] = (
                here[...].astype(f32)
                + from_x[g][zz].astype(f32)
                + from_y[g][zz].astype(f32)
            )

            @pl.when(z > 0)
            def _():
                z_arrival(g, zz).wait_recv()
                outs[g][...] += from_z[g][zz].astype(f32)

            @pl.when(z < planes - 1)
            def _():
                z_arrival(g, planes).wait_recv()
                outs[g][...] += from_z[g][planes].astype(f32)

    def stage_end(g, t):
        zz = visit(t, z, planes)
        core_copy(g, zz).wait_send()

        def even():
            diag_x(g, zz).wait_send()
            diag_y(g, zz, False).wait_send()

        lean_or_even(t, lambda: diag_y(g, zz, True).wait_send(), even)
        x_copy(g, zz).wait_send()
        y_copy(g, zz).wait_send()

        @pl.when(t > 0)
        def _():
            z_copy(g, zz, True).wait_send()

    return Reduction(
        core_copy=core_copy, core=stage_core, plane=stage_plane, line=stage_line, end=stage_end
    )


def remote(src, dst, send, recv, target):
    return pltpu.make_async_remote_copy(
        src_ref=src,
        dst_ref=dst,
        send_sem=send,
        recv_sem=recv,
        device_id=target,
        device_id_type=MESH_ID,
    )


def scatter_kernel(planes, shapes, *refs):
    n = len(shapes)
    parts, refs = refs[:n], refs[n:]
    starts, query, *tiles, context, d_context, log_total, cos_table, sin_table = refs[:11]
    refs = refs[11:]
    outs, refs = refs[:n], refs[n:]
    d_query, d_key, d_value, first_grad = refs[:4]
    refs = refs[4:]
    mine, near, chip, far, from_b, from_d, tile_send, tile_recv, bias, acc = refs[-10:]
    own, boxes, own_sem, sems = refs[:n], refs[n : 7 * n], refs[7 * n], refs[7 * n + 1 : -10]
    z, y, x, c = position()
    entry_barrier(z, y, x, c, planes)
    f32 = jnp.float32
    push = remote

    def add(dst, src):
        dst[...] = (dst[...].astype(f32) + src[...].astype(f32)).astype(dst.dtype)

    def load(g, zz):
        return pltpu.make_async_copy(
            parts[g].at[zz, :, :, c], own[g].at[zz], own_sem.at[g, zz]
        )

    steps = reduction(
        planes,
        shapes,
        True,
        lambda g, zz, yy, xx: own[g].at[zz, yy, xx],
        lambda g, zz: parts[g].at[zz, :, :, 1 - c],
        lambda g, zz: load(g, zz).wait(),
        boxes,
        sems,
        outs,
    )

    partner = device(z, y, x, 1 - c)
    seqs, rows = mine.shape[1:3]
    pairs = mine.shape[3] // 128

    def send_b(s):
        return push(
            near.at[:, s], from_b.at[:, s], tile_send.at[0, s], tile_recv.at[0, s], partner
        )

    def send_d(s):
        return push(
            far.at[:, s], from_d.at[:, s], tile_send.at[1, s], tile_recv.at[1, s], partner
        )

    def send_back(s):
        return push(
            chip.at[:, s],
            chip.at[:, s],
            tile_send.at[2, s],
            tile_recv.at[2, s],
            device(z, y, 1 - x, c),
        )

    def unit(s, p):
        lanes = pl.ds(pl.multiple_of(p * 128, 128), 128)
        flat = pl.ds(pl.multiple_of(s * rows, rows), rows)
        two = lambda ref: [ref.at[0, s, :, lanes], ref.at[1, s, :, lanes]]
        attend_back_step(
            lax.axis_index("ctx"),
            p == 0,
            starts.at[s],
            query[s, :, lanes],
            [two(t) for t in tiles],
            context[s, :, lanes],
            d_context[s, :, lanes],
            log_total.at[s, p],
            cos_table.at[flat],
            sin_table.at[flat],
            d_query.at[s, :, lanes],
            [two(t) for t in (mine, near, chip, far)],
            bias,
            acc,
        )

    def work(i):
        @pl.when((i >= 2) & (i <= 2 * seqs) & (lax.rem(i, 2) == 0) & (x == 1))
        def _():
            s = lax.div(i, 2) - 1
            send_d(s).wait_recv()

            @pl.loop(0, 2 * rows // 32)
            def _(j):
                kind = lax.div(j, rows // 32)
                at = pl.ds(pl.multiple_of(lax.rem(j, rows // 32) * 32, 32), 32)
                add(chip.at[kind, s, at], from_d.at[kind, s, at])

            send_back(s).start()

        @pl.when((i >= 0) & (i < 2 * seqs))
        def _():
            s = lax.div(i, 2)

            @pl.loop(0, pairs // 2)
            def _(p):
                unit(s, lax.rem(i, 2) * (pairs // 2) + p)

            @pl.when(lax.rem(i, 2) == 1)
            def _():
                send_b(s).start()
                pl.when(x == 1)(lambda: send_d(s).start())

    @pl.loop(0, planes)
    def _(r):
        zz = visit(planes - 1 - r, z, planes)
        for g in range(n):
            steps.core_copy(g, zz).start()
            load(g, zz).start()

    @pl.loop(0, planes + 2)
    def _(r):
        t = planes - 1 - r
        for g in range(n):
            pl.when(r < planes)(lambda: steps.core(g, t))
        for g in range(n):
            if g == 0:
                work(2 * r - 2)
            pl.when((r >= 1) & (r < planes + 1))(lambda: steps.plane(g, t + 1))
        work(2 * r - 1)
        for g in range(n):
            pl.when(r >= 2)(lambda: steps.line(g, t + 2))

    @pl.loop(0, planes)
    def _(t):
        for g in range(n):
            steps.end(g, t)

    for s in range(seqs):
        send_b(s).wait()

        @pl.when(x == 0)
        def _():
            send_back(s).wait_recv()

        @pl.when(x == 1)
        def _():
            send_d(s).wait_send()
            send_back(s).wait_send()

    @pl.when(x == 1)
    def _():
        chip[...] = jnp.zeros_like(chip)

    @pl.loop(0, seqs * rows // 32)
    def _(i):
        seq = lax.div(i, rows // 32)
        at = pl.ds(pl.multiple_of(lax.rem(i, rows // 32) * 32, 32), 32)
        flat = pl.ds(pl.multiple_of(i * 32, 32), 32)
        cos_rows, sin_rows = cos_table[flat, :], sin_table[flat, :]
        for k in range(pairs):
            lanes = pl.ds(k * 128, 128)

            def summed(kind):
                return (
                    mine[kind, seq, at, lanes].astype(f32)
                    + from_b[kind, seq, at, lanes].astype(f32)
                    + chip[kind, seq, at, lanes].astype(f32)
                )

            d_key[flat, lanes] = turned(summed(0), cos_rows, sin_rows, -1.0).astype(jnp.bfloat16)
            half = 0.5 * summed(1)
            d_value[flat, lanes] = half.astype(jnp.bfloat16)
            first_grad[flat, lanes] = half


def boxes_of(planes, shapes, types):
    def boxes(lead, narrow=False):
        out = []
        for s, d in zip(shapes, types):
            width = s[1] // 2 // 128 * 128 if narrow else s[1]
            out.append(pltpu.VMEM((*lead, s[0], width), d))
        return out

    return [
        *boxes((planes, 2, 2)),
        *boxes((planes,), True),
        *boxes((planes,)),
        *boxes((planes,)),
        *boxes((planes,)),
        *boxes((planes + 1,)),
    ]


def sems_of(planes, n):
    dma = pltpu.SemaphoreType.DMA
    return [
        dma((n, planes)),
        dma((n, planes)),
        dma((n, planes, 2)),
        dma((n, planes, 2)),
        dma((n, planes)),
        dma((n, planes)),
        dma((n, planes)),
        dma((n, planes)),
        dma((n, planes)),
        dma((n, planes + 1)),
    ]


def scatter_sum(planes, partials, attention):
    n = len(partials)
    partials = [
        p.reshape(planes, 2, 2, 2, p.shape[0] // (planes * 8), p.shape[1]) for p in partials
    ]
    shapes = [p.shape[4:] for p in partials]
    bf16 = jnp.bfloat16
    dma = pltpu.SemaphoreType.DMA
    box = attention[2].shape
    seqs, rows, width = box[1:]
    flat = (seqs * rows, width)
    vmem = pl.BlockSpec(memory_space=pltpu.VMEM)
    return pl.pallas_call(
        functools.partial(scatter_kernel, planes, shapes),
        out_shape=[jax.ShapeDtypeStruct(s, jnp.float32) for s in shapes]
        + [
            jax.ShapeDtypeStruct(box[1:], bf16),
            jax.ShapeDtypeStruct(flat, bf16),
            jax.ShapeDtypeStruct(flat, bf16),
            jax.ShapeDtypeStruct(flat, jnp.float32),
        ],
        in_specs=[pl.BlockSpec(memory_space=pl.ANY)] * n + [vmem] * len(attention),
        out_specs=[vmem] * (n + 4),
        scratch_shapes=[
            *[pltpu.VMEM((planes, 2, 2, *s), bf16) for s in shapes],
            *boxes_of(planes, shapes, [bf16] * n),
            dma((n, planes)),
            *sems_of(planes, n),
            *[pltpu.VMEM(box, bf16)] * 6,
            dma((3, seqs)),
            dma((3, seqs)),
            *attend_back_scratch(rows),
        ],
        compiler_params=pltpu.CompilerParams(
            collective_id=1, has_side_effects=True, vmem_limit_bytes=67043328
        ),
        name="gradient_scatter",
    )(*partials, *attention)


def last_kernel(planes, shapes, *refs):
    f32, bf16 = jnp.float32, jnp.bfloat16
    n = len(shapes)
    normed, *d_proj = refs[:4]
    w_in, tok_in, d_residual_in, attn_gain, d_ffn_gain = refs[4:7], *refs[7:11]
    outs, token_grad = refs[11 : 11 + n], refs[11 + n]
    refs = refs[12 + n :]
    weights, tok, d_residual, gain_sum = refs[:3], *refs[3:6]
    parts, boxes, sems, load_sem = refs[6 : 6 + n], refs[6 + n : 6 + 7 * n], refs[6 + 7 * n : -1], refs[-1]
    z, y, x, c = position()
    loads = [
        pltpu.make_async_copy(src, dst, load_sem.at[i])
        for i, (src, dst) in enumerate(zip([*w_in, tok_in, d_residual_in], [*weights, tok, d_residual]))
    ]
    for copy in loads:
        copy.start()
    entry_barrier(z, y, x, c, planes)
    rows, width = tok.shape
    steps = reduction(
        planes,
        shapes,
        False,
        lambda g, zz, yy, xx: parts[g].at[zz, yy, xx, c],
        lambda g, zz: parts[g].at[zz, :, :, 1 - c],
        lambda g, zz: None,
        boxes,
        sems,
        outs,
    )
    at_once = planes * 256 // width

    def weight_grads(j):
        lanes = pl.ds(pl.multiple_of(j * 256, 256), 256)
        for g in range(3):
            part = lax.dot_general(normed[:, lanes], d_proj[g][...], TN, preferred_element_type=f32)
            shape = (at_once, 2, 2, 2, *shapes[g])
            parts[g][pl.ds(j * at_once, at_once)] = part.reshape(shape).astype(bf16)

    def normed_grad():
        for copy in loads:
            copy.wait()

        @pl.loop(0, width // 256)
        def _(j):
            at = pl.ds(pl.multiple_of(j * 256, 256), 256)
            total = 0.0
            for g in range(3):
                total = total + lax.dot_general(
                    d_proj[g][...], weights[g][at, :], NT, preferred_element_type=f32
                )
            token_grad[:, at] = total

    def token_gradient():
        gain_sum[...] = jnp.zeros_like(gain_sum)

        @pl.loop(0, rows // 64)
        def _(i):
            at = pl.ds(pl.multiple_of(i * 64, 64), 64)
            values = tok[at, :].astype(f32)
            scale = inverse_rms(values)
            d_normed = token_grad[at, :]
            products = d_normed * values * scale
            gain_sum[...] += jnp.sum(products.reshape(8, 8, width), axis=0)
            weighted = d_normed * attn_gain[...]
            token_grad[at, :] = (
                d_residual[at, :]
                + scale * weighted
                - values * (scale * scale * scale) * jnp.mean(weighted * values, axis=-1, keepdims=True)
            )

        both = jnp.concatenate(
            [jnp.sum(gain_sum[...], axis=0, keepdims=True), d_ffn_gain[...], jnp.zeros((6, width), f32)]
        )
        per = planes * 8 * 256 // width
        for i in range(planes * 8):
            at = i // per * 256
            parts[3][i // 8, i // 4 % 2, i // 2 % 2, i % 2] = both[:, at : at + 256]

    def send_cores(g, t):
        steps.core_copy(g, visit(t, z, planes)).start()

    if at_once > 1:
        pl.loop(0, width // 256)(weight_grads)
    lag = 2

    @pl.loop(0, planes + 3 + lag)
    def _(r):
        t = planes - 1 - r

        @pl.when(r < planes)
        def _():
            if at_once == 1:
                weight_grads(visit(t, z, planes))
            for g in range(3):
                send_cores(g, t)

        for group, late in ((range(3), 0), ((3,), lag)):
            for step, behind in ((steps.core, 1), (steps.plane, 2), (steps.line, 3)):
                behind += late
                for g in group:
                    pl.when((r >= behind) & (r < planes + behind))(lambda: step(g, t + behind))

        @pl.when(r == 1)
        def _():
            normed_grad()

        @pl.when(r == 2)
        def _():
            token_gradient()

            @pl.loop(0, planes)
            def _(i):
                send_cores(3, i)

    @pl.loop(0, planes)
    def _(t):
        for g in range(n):
            steps.end(g, t)


def last(planes, normed, d_proj, weights, tok, d_residual, attn_gain, d_ffn_gain):
    f32, bf16 = jnp.float32, jnp.bfloat16
    width = tok.shape[1]
    shapes = [(width // (planes * 8), width)] * 3 + [(8, 256)]
    types = [bf16] * 3 + [f32]
    n = len(shapes)
    vmem, anywhere = pl.BlockSpec(memory_space=pltpu.VMEM), pl.BlockSpec(memory_space=pl.ANY)
    return pl.pallas_call(
        functools.partial(last_kernel, planes, shapes),
        out_shape=[jax.ShapeDtypeStruct(s, f32) for s in [*shapes, tok.shape]],
        in_specs=[vmem] * 4 + [anywhere] * 5 + [vmem] * 2,
        out_specs=[vmem] * (n + 1),
        scratch_shapes=[
            *[pltpu.VMEM((width, width), bf16)] * 3,
            pltpu.VMEM(tok.shape, bf16),
            pltpu.VMEM(tok.shape, f32),
            pltpu.VMEM((8, width), f32),
            *[pltpu.VMEM((planes, 2, 2, 2, *s), d) for s, d in zip(shapes, types)],
            *boxes_of(planes, shapes, types),
            *sems_of(planes, n),
            pltpu.SemaphoreType.DMA((5,)),
        ],
        compiler_params=pltpu.CompilerParams(
            collective_id=2, has_side_effects=True, vmem_limit_bytes=67043328
        ),
        name="last",
    )(normed, *d_proj, *weights, tok, d_residual, attn_gain, d_ffn_gain)


def on_device(
    planes,
    tokens,
    first_values,
    cotangent,
    segment_ids,
    attn_gain,
    w_query,
    w_key,
    w_value,
    w_out,
    ffn_gain,
    gate_weight,
    up_weight,
    down_weight,
):
    f32, bf16 = jnp.float32, jnp.bfloat16
    seqs, rows, width = tokens.shape
    rank = lax.axis_index("ctx")
    share = attn_gain.shape[0]
    per = 128 // share
    index = lax.axis_index("dp") * lax.axis_size("ctx") + rank
    place = lax.rem(index, per)
    here = jnp.arange(128, dtype=jnp.int32) // share == place
    spread = lambda gain: jnp.where(here, jnp.tile(gain, per), jnp.zeros((), bf16))
    gains = jnp.zeros((16, 128), bf16).at[0].set(spread(attn_gain)).at[1].set(spread(ffn_gain))
    starts, cos_table, sin_table = tables(segment_ids, rank, rows)
    flat = (seqs * rows, width)
    local = (seqs, rows, width)
    tokens = tokens.reshape(flat)
    mm = functools.partial(jnp.dot, preferred_element_type=f32)
    by_rows = lambda a, b: lax.dot_general(a, b, TN, preferred_element_type=f32).astype(bf16)
    back = lambda a, b: lax.dot_general(a, b, NT, preferred_element_type=f32)
    (gains, w_query, w_key, w_value, w_out, gate_weight, up_weight, down_weight), (
        normed_one,
        query_rot,
        *tiles,
        context3,
        log_total,
    ) = forward(
        planes,
        4,
        [gains, w_query, w_key, w_value, w_out, gate_weight, up_weight, down_weight],
        tokens,
        first_values.reshape(flat),
        starts,
        cos_table,
        sin_table,
    )
    gains = jnp.sum(gains.reshape(width // 128, per, 16, 128), axis=1)
    attn_gain = gains[:, 0].reshape(1, width)
    ffn_gain = gains[:, 1].reshape(1, width)
    context = context3.reshape(flat)
    tokens_float = tokens.astype(f32)
    cotangent = cotangent.reshape(flat)
    residual = tokens_float + mm(context, w_out)
    scale_two = inverse_rms(residual)
    second_normed = (residual * scale_two * ffn_gain.astype(f32)).astype(bf16)
    gate = mm(second_normed, gate_weight)
    up = mm(second_normed, up_weight)
    hidden = (swish(gate) * up).astype(bf16)
    output = (residual + mm(hidden, down_weight)).astype(bf16)

    out_float = cotangent.astype(f32)
    d_down = by_rows(hidden, cotangent)
    d_hidden = back(cotangent, down_weight)
    sigmoid_gate = jax.nn.sigmoid(gate)
    d_gate = (d_hidden * up * sigmoid_gate * (1.0 + gate * (1.0 - sigmoid_gate))).astype(bf16)
    d_up = (d_hidden * (gate * sigmoid_gate)).astype(bf16)
    d_gate_weight = by_rows(second_normed, d_gate)
    d_up_weight = by_rows(second_normed, d_up)
    d_normed_two = back(d_gate, gate_weight) + back(d_up, up_weight)
    d_ffn_gain = jnp.sum(d_normed_two * residual * scale_two, axis=0)
    weighted_two = d_normed_two * ffn_gain.astype(f32)
    d_residual = (
        out_float
        + scale_two * weighted_two
        - residual
        * (scale_two * scale_two * scale_two)
        * jnp.mean(weighted_two * residual, axis=-1, keepdims=True)
    )
    d_residual_low = d_residual.astype(bf16)
    d_out = by_rows(context, d_residual_low)
    d_context = back(d_residual_low, w_out).astype(bf16).reshape(local)
    s_down, s_gate, s_up, s_out, d_query, d_key, d_value, first_grad = scatter_sum(
        planes,
        [d_down, d_gate_weight, d_up_weight, d_out],
        [starts, query_rot, *tiles, context3, d_context, log_total, cos_table, sin_table],
    )
    d_query = d_query.reshape(flat)
    s_wq, s_wk, s_wv, s_gains, token_grad = last(
        planes,
        normed_one,
        [d_query, d_key, d_value],
        [w_query, w_key, w_value],
        tokens,
        d_residual,
        attn_gain.astype(f32),
        d_ffn_gain[None],
    )
    slot = lax.rem(index, 256 // share) * share
    s_gains = lax.dynamic_slice_in_dim(s_gains[:2], slot, share, 1)
    return (
        output.reshape(local),
        token_grad.reshape(local),
        first_grad.reshape(local),
        s_gains[0],
        s_wq,
        s_wk,
        s_wv,
        s_out,
        s_gains[1],
        s_gate,
        s_up,
        s_down,
    )


def solution(mesh):
    token, weight, vector = P("dp", "ctx", None), P(("dp", "ctx"), None), P(("dp", "ctx"))
    return jax.shard_map(
        functools.partial(on_device, mesh.shape["dp"] // 2),
        mesh=mesh,
        in_specs=(
            token,
            token,
            token,
            P("dp", None),
            vector,
            weight,
            weight,
            weight,
            weight,
            vector,
            weight,
            weight,
            weight,
        ),
        out_specs=(
            token,
            token,
            token,
            vector,
            weight,
            weight,
            weight,
            weight,
            vector,
            weight,
            weight,
            weight,
        ),
        check_vma=False,
    )
```

```python
import functools
import jax
import jax.numpy as jnp
from jax import lax
from jax.experimental import pallas as pl
from jax.experimental.pallas import tpu as pltpu
from jax.sharding import PartitionSpec as P

HEADS = 16
HEAD_DIM = 64
MESH_ID = pl.DeviceIdType.MESH

epsilon = 1e-05
rope_base = 10000.0
score_scale = 0.125
masked_score = -1e30


def inverse_rms(values):
    return lax.rsqrt(jnp.mean(values * values, axis=-1, keepdims=True) + epsilon)


def swish(values):
    return values * jax.nn.sigmoid(values)


def first_half(shape):
    return lax.broadcasted_iota(jnp.int32, shape, len(shape) - 1) % HEAD_DIM < HEAD_DIM // 2


def swap_halves(values):
    return jnp.where(
        first_half(values.shape), pltpu.roll(values, 96, 1), pltpu.roll(values, 32, 1)
    )


def turned(values, cos_table, sin_table, sign):
    return values * cos_table + sign * (swap_halves(values) * sin_table)


def tables(segment_ids, rank, rows):
    seqs = segment_ids.shape[0]
    own_ids = lax.dynamic_slice_in_dim(segment_ids, rank * rows, rows, 1)
    earlier = segment_ids[:, :, None] < own_ids[:, None, :]
    starts = jnp.sum(earlier.astype(jnp.int32), axis=1)
    local = rank * rows + jnp.arange(rows, dtype=jnp.int32) - starts
    lane = jnp.arange(128, dtype=jnp.int32)
    half = HEAD_DIM // 2
    frequency = rope_base ** (-(lane % half).astype(jnp.float32) * 2.0 / HEAD_DIM)
    angles = local.astype(jnp.float32).reshape(seqs * rows, 1) * frequency
    sign = jnp.where(lane % HEAD_DIM < half, -1.0, 1.0)
    return starts.reshape(seqs, 1, rows), jnp.cos(angles), jnp.sin(angles) * sign


def normalise(tok, gain, normed):
    rows = tok.shape[0]

    @pl.loop(0, rows // 64)
    def _(i):
        at = pl.ds(pl.multiple_of(i * 64, 64), 64)
        values = tok[at, :].astype(jnp.float32)
        normed[at, :] = (values * inverse_rms(values) * gain).astype(jnp.bfloat16)


def columns_of(weight, lanes):
    block = weight[:, :, lanes]
    if block.shape[1] % 16:
        block = block.astype(jnp.float32)
    return block.reshape(block.shape[0] * block.shape[1], block.shape[2]).astype(jnp.bfloat16)


def project(normed, first, wq, wk, wv, cos_ref, sin_ref, query, pair):
    f32, bf16 = jnp.float32, jnp.bfloat16
    seqs, rows, width = query.shape

    @pl.loop(0, width // 256)
    def _(i):
        lanes = pl.ds(pl.multiple_of(i * 256, 256), 256)
        n1 = normed[...]
        cos_table, sin_table = cos_ref[...], sin_ref[...]
        queries = jnp.dot(n1, columns_of(wq, lanes), preferred_element_type=f32)
        keys = jnp.dot(n1, columns_of(wk, lanes), preferred_element_type=f32)
        values = jnp.dot(n1, columns_of(wv, lanes), preferred_element_type=f32)
        mixed = (0.5 * values + 0.5 * first[:, lanes].astype(f32)).astype(bf16)
        for half in range(2):
            part = slice(half * 128, half * 128 + 128)
            at = pl.ds(pl.multiple_of(i * 256 + half * 128, 128), 128)
            q = turned(queries[:, part], cos_table, sin_table, 1.0).astype(bf16)
            k = turned(keys[:, part], cos_table, sin_table, 1.0).astype(bf16)
            for s in range(seqs):
                query[s, :, at] = q[s * rows : (s + 1) * rows]
                pair[0, s, :, at] = k[s * rows : (s + 1) * rows]
                pair[1, s, :, at] = mixed[s * rows : (s + 1) * rows, part]


def two_heads(block, scale):
    lane = lax.broadcasted_iota(jnp.int32, block.shape, 1)
    scaled = block * jnp.asarray(scale, block.dtype)
    zero = jnp.zeros_like(block)
    return jnp.concatenate(
        [jnp.where(lane < HEAD_DIM, scaled, zero), jnp.where(lane < HEAD_DIM, zero, scaled)]
    )


def own_lanes(both):
    rows = both.shape[1] // 2
    lane = lax.broadcasted_iota(jnp.int32, (both.shape[0], rows), 0)
    return jnp.where(lane < HEAD_DIM, both[:, :rows], both[:, rows:]).T


def fill_bias(bias, starts, rank):
    rows = bias.shape[1]
    key = lax.broadcasted_iota(jnp.int32, (rows, rows), 0)
    place = rank * rows + lax.broadcasted_iota(jnp.int32, (rows, rows), 1)
    begin = starts[...]
    for t in range(4):
        x, c = lax.div(rank, 2), lax.rem(rank, 2)
        owner = (1 - x if t >= 2 else x) * 2 + (1 - c if t % 2 else c)
        at = owner * rows + key
        bias[t] = jnp.where((at >= begin) & (at <= place), 0.0, masked_score)


NT = (((1,), (1,)), ((), ()))
TN = (((0,), (0,)), ((), ()))


def attend_step(rank, begin, starts, q, tiles, out, log_total, bias, scores, peak, total, acc):
    f32, bf16 = jnp.float32, jnp.bfloat16

    @pl.when(begin)
    def _():
        fill_bias(bias, starts, rank)

    high = rank >= 2
    stacked = two_heads(q, score_scale)

    def score(t):
        s = lax.dot_general(tiles[t][0][...], stacked, NT, preferred_element_type=f32)
        s = s + jnp.concatenate([bias[t], bias[t]], axis=1)
        scores[t] = s
        return jnp.max(s, axis=0, keepdims=True)

    def gather_values(t, top):
        e = jnp.exp(scores[t] - top)
        part = lax.dot_general(tiles[t][1][...], e.astype(bf16), TN, preferred_element_type=f32)
        return jnp.sum(e, axis=0, keepdims=True), part

    peak[...] = jnp.maximum(score(0), score(1))

    @pl.when(high)
    def _():
        peak[...] = jnp.maximum(peak[...], jnp.maximum(score(2), score(3)))

    top = peak[...]
    sum_a, acc_a = gather_values(0, top)
    sum_b, acc_b = gather_values(1, top)
    total[...] = sum_a + sum_b
    acc[...] = acc_a + acc_b

    @pl.when(high)
    def _():
        top = peak[...]
        sum_a, acc_a = gather_values(2, top)
        sum_b, acc_b = gather_values(3, top)
        total[...] += sum_a + sum_b
        acc[...] += acc_a + acc_b

    out[...] = own_lanes(acc[...] / total[...]).astype(bf16)
    log_total[...] = peak[...] + jnp.log(total[...])


def attend_scratch(rows):
    return [
        pltpu.VMEM((4, rows, rows), jnp.float32),
        pltpu.VMEM((4, rows, 2 * rows), jnp.float32),
        pltpu.VMEM((1, 2 * rows), jnp.float32),
        pltpu.VMEM((1, 2 * rows), jnp.float32),
        pltpu.VMEM((128, 2 * rows), jnp.float32),
    ]


def attend_back_step(
    rank, begin, starts, q, tiles, context, d_context, log_total, cos_t, sin_t, d_q, d_tiles, bias, acc
):
    f32, bf16 = jnp.float32, jnp.bfloat16

    @pl.when(begin)
    def _():
        fill_bias(bias, starts, rank)

    high = rank >= 2
    stacked = two_heads(q, score_scale)
    stacked_do = two_heads(d_context, 1.0)
    turned_product = (d_context.astype(f32) * context.astype(f32)).T
    delta = jnp.concatenate(
        [
            jnp.sum(turned_product[:HEAD_DIM], axis=0, keepdims=True),
            jnp.sum(turned_product[HEAD_DIM:], axis=0, keepdims=True),
        ],
        axis=1,
    )
    lse = log_total[...]

    def one(t):
        keys, values = tiles[t][0][...], tiles[t][1][...]
        s = lax.dot_general(keys, stacked, NT, preferred_element_type=f32)
        s = s + jnp.concatenate([bias[t], bias[t]], axis=1)
        p = jnp.exp(s - lse)
        dp = lax.dot_general(values, stacked_do, NT, preferred_element_type=f32)
        ds = (p * (dp - delta)).astype(bf16)
        d_tiles[t][1][...] = jnp.dot(p.astype(bf16), stacked_do, preferred_element_type=f32).astype(bf16)
        d_tiles[t][0][...] = jnp.dot(ds, stacked, preferred_element_type=f32).astype(bf16)
        return lax.dot_general(keys, ds, TN, preferred_element_type=f32)

    acc[...] = one(0) + one(1)

    @pl.when(high)
    def _():
        acc[...] += one(2) + one(3)

    d_q[...] = turned(own_lanes(acc[...]) * score_scale, cos_t[...], sin_t[...], -1.0).astype(bf16)


def attend_back_scratch(rows):
    return [pltpu.VMEM((4, rows, rows), jnp.float32), pltpu.VMEM((128, 2 * rows), jnp.float32)]


def position():
    dp = lax.axis_index("dp")
    ct = lax.axis_index("ctx")
    return lax.div(dp, 2), lax.rem(dp, 2), lax.div(ct, 2), lax.rem(ct, 2)


def visit(step, z, planes):
    back = planes - 1 - step
    high = back + jnp.where(back >= z, 1, 0)
    low = planes - 1 - back
    low = low - jnp.where(low <= z, 1, 0)
    other = jnp.where(z < planes // 2, low, high)
    return jnp.where(step == 0, z, other)


def device(z, y, x, c):
    return (z * 2 + y, x * 2 + c)


def halves(shape):
    if shape[0] % 2 == 0:
        cut = shape[0] // 2
        return (pl.ds(0, cut), slice(None), slice(None)), (pl.ds(cut, cut), slice(None), slice(None))
    cut = shape[2] // 2 // 128 * 128
    return (
        (slice(None), slice(None), pl.ds(0, cut)),
        (slice(None), slice(None), pl.ds(cut, shape[2] - cut)),
    )


def entry_barrier(z, y, x, c, planes):
    barrier = pltpu.get_barrier_semaphore()

    def hello(target):
        pl.semaphore_signal(barrier, inc=1, device_id=target, device_id_type=MESH_ID)

    hello(device(z, y, 1 - x, c))
    hello(device(z, 1 - y, x, c))
    hello(device(z, y, x, 1 - c))

    @pl.when(z > 0)
    def _():
        hello(device(z - 1, y, x, c))

    @pl.when(z < planes - 1)
    def _():
        hello(device(z + 1, y, x, c))

    pl.semaphore_wait(barrier, 3 + jnp.where(z > 0, 1, 0) + jnp.where(z < planes - 1, 1, 0))


def forward_kernel(planes, shapes, first_group, *refs):
    n = len(shapes)
    ins, refs = refs[:n], refs[n:]
    tok, first, starts, cos_table, sin_table = refs[:5]
    outs, refs = refs[5 : 5 + n], refs[5 + n :]
    normed, query, mine, near, chip, far, context, log_total = refs[:8]
    sems, refs = refs[8:19], refs[19:]
    own_sem, z_send, z_recv, x_send, x_recv, y_send, y_recv, d_send, d_recv, c_send, c_recv = sems
    tile_send, tile_recv, load_sem, gains, *weights = refs[: 4 + first_group - 1]
    scratch = refs[4 + first_group - 1 :]
    z, y, x, c = position()
    entry_barrier(z, y, x, c, planes)
    local = [
        pltpu.make_async_copy(ins[g], outs[g].at[:, z, y, x, c], own_sem.at[g]) for g in range(n)
    ]
    for copy in local:
        copy.start()

    def push(src, dst, send, recv, target):
        return pltpu.make_async_remote_copy(
            src_ref=src,
            dst_ref=dst,
            send_sem=send,
            recv_sem=recv,
            device_id=target,
            device_id_type=MESH_ID,
        )

    def spot(g, zz, yy, xx):
        return outs[g].at[:, zz, yy, xx, c]

    def z_copy(g, zz, up, own):
        side = 1 if up else 0
        return push(
            ins[g] if own else spot(g, zz, y, x),
            spot(g, zz, y, x),
            z_send.at[g, zz, side],
            z_recv.at[g, zz],
            device(z + 1 if up else z - 1, y, x, c),
        )

    def x_copy(g, zz, own):
        return push(
            ins[g] if own else spot(g, zz, y, x),
            spot(g, zz, y, x),
            x_send.at[g, zz],
            x_recv.at[g, zz],
            device(z, y, 1 - x, c),
        )

    def y_copy(g, zz, own):
        return push(
            ins[g] if own else spot(g, zz, y, x),
            spot(g, zz, y, x),
            y_send.at[g, zz],
            y_recv.at[g, zz],
            device(z, 1 - y, x, c),
        )

    def relay(g, zz, half, by_y):
        here = spot(g, zz, y, 1 - x) if by_y else spot(g, zz, 1 - y, x)
        here = here.at[halves(shapes[g])[half]]
        return push(
            here,
            here,
            d_send.at[g, zz, 2 * half if by_y else 1],
            d_recv.at[g, zz, half],
            device(z, 1 - y, x, c) if by_y else device(z, y, 1 - x, c),
        )

    def diag_arrival(g, zz, half):
        here = spot(g, zz, 1 - y, 1 - x).at[halves(shapes[g])[half]]
        return push(
            here, here, d_send.at[g, zz, half], d_recv.at[g, zz, half], device(z, y, x, 1 - c)
        )

    def core_copy(g, zz, mine):
        here = outs[g].at[:, zz, :, :, c if mine else 1 - c]
        return push(here, here, c_send.at[g, zz], c_recv.at[g, zz], device(z, y, x, 1 - c))

    def on_links(g, t, act):
        zz = visit(t, z, planes)

        def both(own):
            up = (z < planes - 1) if own else (zz < z) & (z < planes - 1)
            down = (z > 0) if own else (zz > z) & (z > 0)
            pl.when(down)(lambda: act(z_copy(g, zz, False, own)))
            pl.when(up)(lambda: act(z_copy(g, zz, True, own)))
            act(x_copy(g, zz, own))
            act(y_copy(g, zz, own))

        pl.when(t == 0)(lambda: both(True))
        pl.when(t > 0)(lambda: both(False))

    def on_relays(g, t, act, between=lambda: None):
        zz = visit(t, z, planes)
        act(relay(g, zz, 0, True))
        if g < first_group:
            between()
            act(relay(g, zz, 1, False))
            return
        lean = t < planes - 1
        pl.when(lean & (x == 1))(lambda: act(relay(g, zz, 1, True)))
        between()
        pl.when((x == 1) | jnp.logical_not(lean))(lambda: act(relay(g, zz, 1, False)))

    def start(copy):
        copy.start()

    def wait_send(copy):
        copy.wait_send()

    def stage_line(g, t):
        @pl.when(t > 0)
        def _():
            z_copy(g, visit(t, z, planes), True, False).wait_recv()

        on_links(g, t, start)

    def stage_plane(g, t):
        zz = visit(t, z, planes)
        x_copy(g, zz, False).wait_recv()
        on_relays(g, t, start, lambda: y_copy(g, zz, False).wait_recv())

    def stage_core(g, t):
        zz = visit(t, z, planes)
        pl.when(t == 0)(lambda: local[g].wait())
        diag_arrival(g, zz, 0).wait_recv()
        diag_arrival(g, zz, 1).wait_recv()
        core_copy(g, zz, True).start()

    seqs, rows, width = query.shape
    pairs = width // 128
    partner = device(z, y, x, 1 - c)

    def to_partner(s):
        return push(
            mine.at[:, s], near.at[:, s], tile_send.at[0, s], tile_recv.at[0, s], partner
        )

    def to_x(s):
        return push(
            mine.at[:, s],
            chip.at[:, s],
            tile_send.at[1, s],
            tile_recv.at[1, s],
            device(z, y, 1 - x, c),
        )

    def passed_on(s):
        return push(
            chip.at[:, s], far.at[:, s], tile_send.at[2, s], tile_recv.at[2, s], partner
        )

    def send_tiles(s):
        to_partner(s).start()
        pl.when(x == 0)(lambda: to_x(s).start())

    def projection():
        @pl.loop(0, planes)
        def _(t):
            for g in range(first_group):
                core_copy(g, visit(t, z, planes), False).wait_recv()

        loads = [
            pltpu.make_async_copy(outs[g].at[0], buf, load_sem.at[g])
            for g, buf in enumerate([gains, *weights])
        ]
        for copy in loads:
            copy.start()
        loads[0].wait()
        flat_gains = [gains[i, j, k, m] for i in range(planes) for j in (0, 1) for k in (0, 1) for m in (0, 1)]
        per = len(flat_gains) * 128 // width
        gain = jnp.concatenate(
            [
                sum(b[:1].astype(jnp.float32) for b in flat_gains[i * per : (i + 1) * per])
                for i in range(width // 128)
            ],
            axis=1,
        )
        normalise(tok, gain, normed)
        for copy in loads[1:]:
            copy.wait()
        as_blocks = lambda w: w.reshape((planes * 8, *w.shape[4:]))
        project(
            normed, first, *[as_blocks(w) for w in weights], cos_table, sin_table, query, mine
        )
        for s in range(seqs):
            send_tiles(s)

    def unit(s, p):
        lanes = pl.ds(pl.multiple_of(p * 128, 128), 128)
        attend_step(
            lax.axis_index("ctx"),
            p == 0,
            starts.at[s],
            query[s, :, lanes],
            [[w.at[0, s, :, lanes], w.at[1, s, :, lanes]] for w in (mine, near, chip, far)],
            context.at[s, :, lanes],
            log_total.at[s, p],
            *scratch,
        )

    def attention():
        @pl.loop(0, seqs)
        def _(s):
            to_partner(s).wait_recv()

            @pl.when(x == 1)
            def _():
                to_x(s).wait_recv()
                passed_on(s).start()
                passed_on(s).wait_recv()

            @pl.loop(0, pairs)
            def _(p):
                unit(s, p)

    groups = (range(first_group), range(first_group, n))

    @pl.loop(0, 2 * planes + 2)
    def _(r):
        for stage, lag in ((stage_line, 0), (stage_plane, 1), (stage_core, 2)):
            for k, group in enumerate(groups):
                t = r - k * planes - lag
                for g in group:
                    pl.when((t >= 0) & (t < planes))(lambda: stage(g, t))
            if lag == 0:
                pl.when(r == planes + 3)(attention)
        pl.when(r == planes + 1)(projection)

    @pl.loop(0, planes)
    def _(t):
        zz = visit(t, z, planes)
        for g in range(n):
            if g >= first_group:
                core_copy(g, zz, False).wait_recv()
            core_copy(g, zz, True).wait_send()
            on_links(g, t, wait_send)
            on_relays(g, t, wait_send)

    for s in range(seqs):
        to_partner(s).wait_send()
        pl.when(x == 0)(lambda: to_x(s).wait_send())
        pl.when(x == 1)(lambda: passed_on(s).wait_send())


def forward(planes, first_group, blocks, tok, first, starts, cos_table, sin_table):
    blocks = [b[None] for b in blocks]
    n = len(blocks)
    shapes = [b.shape for b in blocks]
    seqs, _, rows = starts.shape
    width = tok.shape[1]
    bf16 = jnp.bfloat16
    dma = pltpu.SemaphoreType.DMA
    anywhere = pl.BlockSpec(memory_space=pl.ANY)
    vmem = pl.BlockSpec(memory_space=pltpu.VMEM)
    local = jax.ShapeDtypeStruct((seqs, rows, width), bf16)
    tile = jax.ShapeDtypeStruct((2, seqs, rows, width), bf16)
    got = pl.pallas_call(
        functools.partial(forward_kernel, planes, shapes, first_group),
        out_shape=[
            jax.ShapeDtypeStruct((s[0], planes, 2, 2, 2, s[1], s[2]), b.dtype)
            for s, b in zip(shapes, blocks)
        ]
        + [jax.ShapeDtypeStruct(tok.shape, bf16), local, *[tile] * 4, local]
        + [jax.ShapeDtypeStruct((seqs, width // 128, 1, 2 * rows), jnp.float32)],
        in_specs=[anywhere] * n + [vmem] * 5,
        out_specs=[anywhere] * n + [vmem] * 8,
        scratch_shapes=[
            dma((n,)),
            dma((n, planes, 2)),
            dma((n, planes)),
            dma((n, planes)),
            dma((n, planes)),
            dma((n, planes)),
            dma((n, planes)),
            dma((n, planes, 3)),
            dma((n, planes, 2)),
            dma((n, planes)),
            dma((n, planes)),
            dma((3, seqs)),
            dma((3, seqs)),
            dma((first_group,)),
            *[pltpu.VMEM((planes, 2, 2, 2, *s[1:]), bf16) for s in shapes[:first_group]],
            *attend_scratch(rows),
        ],
        compiler_params=pltpu.CompilerParams(
            collective_id=0, has_side_effects=True, vmem_limit_bytes=67043328
        ),
        name="forward",
    )(*blocks, tok, first, starts, cos_table, sin_table)
    full = [g.reshape(planes * 8 * s[1], s[2]) for g, s in zip(got, shapes)]
    return full, got[n:]


def columns(shape, half):
    cut = shape[1] // 2 // 128 * 128
    return pl.ds(0, cut) if half == 0 else pl.ds(cut, shape[1] - cut)


class Reduction:
    def __init__(self, **steps):
        self.__dict__.update(steps)


def reduction(planes, shapes, routed, own_at, away_at, before_core, boxes, sems, outs):
    n = len(shapes)
    from_core, from_dx, from_dy, from_x, from_y, from_z = (
        boxes[k * n : (k + 1) * n] for k in range(6)
    )
    c_send, c_recv, d_send, d_recv, x_send, x_recv, y_send, y_recv, z_send, z_recv = sems
    z, y, x, c = position()

    def push(src, dst, send, recv, target):
        return pltpu.make_async_remote_copy(
            src_ref=src,
            dst_ref=dst,
            send_sem=send,
            recv_sem=recv,
            device_id=target,
            device_id_type=MESH_ID,
        )

    f32 = jnp.float32

    def add(dst, *srcs):
        total = dst[...].astype(f32)
        for src in srcs:
            total = total + src[...].astype(f32)
        dst[...] = total.astype(dst.dtype)

    def core_copy(g, zz):
        return push(
            away_at(g, zz),
            from_core[g].at[zz],
            c_send.at[g, zz],
            c_recv.at[g, zz],
            device(z, y, x, 1 - c),
        )

    def diag_x(g, zz):
        return push(
            own_at(g, zz, 1 - y, 1 - x).at[:, columns(shapes[g], 0)],
            from_dx[g].at[zz],
            d_send.at[g, zz, 0],
            d_recv.at[g, zz, 0],
            device(z, y, 1 - x, c),
        )

    def diag_y(g, zz, full):
        part = slice(None) if full else columns(shapes[g], 1)
        return push(
            own_at(g, zz, 1 - y, 1 - x).at[:, part],
            from_dy[g].at[zz, :, part],
            d_send.at[g, zz, 1],
            d_recv.at[g, zz, 1],
            device(z, 1 - y, x, c),
        )

    def x_copy(g, zz):
        return push(
            own_at(g, zz, y, 1 - x),
            from_x[g].at[zz],
            x_send.at[g, zz],
            x_recv.at[g, zz],
            device(z, y, 1 - x, c),
        )

    def y_copy(g, zz):
        return push(
            own_at(g, zz, 1 - y, x),
            from_y[g].at[zz],
            y_send.at[g, zz],
            y_recv.at[g, zz],
            device(z, 1 - y, x, c),
        )

    def z_copy(g, zz, up):
        slot = zz if up else jnp.where(zz == z - 1, planes, zz)
        return push(
            own_at(g, zz, y, x),
            from_z[g].at[slot],
            z_send.at[g, zz],
            z_recv.at[g, slot],
            device(z + 1 if up else z - 1, y, x, c),
        )

    def z_arrival(g, slot):
        return push(
            from_z[g].at[slot],
            from_z[g].at[slot],
            z_send.at[g, 0],
            z_recv.at[g, slot],
            device(z, y, x, 1 - c),
        )

    def lean_or_even(t, lean, even):
        if not routed:
            even()
            return
        is_lean = (x == 1) & (t < planes - 2)
        pl.when(jnp.logical_not(is_lean))(even)
        pl.when(is_lean)(lean)

    def stage_core(g, t):
        zz = visit(t, z, planes)
        before_core(g, zz)
        core_copy(g, zz).wait_recv()
        add(own_at(g, zz, 1 - y, 1 - x), from_core[g].at[zz, 1 - y, 1 - x])

        def even():
            diag_x(g, zz).start()
            diag_y(g, zz, False).start()

        lean_or_even(t, lambda: diag_y(g, zz, True).start(), even)
        add(own_at(g, zz, 1 - y, x), from_core[g].at[zz, 1 - y, x])
        if routed:

            @pl.when((x == 0) & (t < planes - 2))
            def _():
                y_copy(g, zz).start()

        add(own_at(g, zz, y, 1 - x), from_core[g].at[zz, y, 1 - x])
        add(own_at(g, zz, y, x), from_core[g].at[zz, y, x])

    def stage_plane(g, t):
        zz = visit(t, z, planes)

        def take_x():
            diag_x(g, zz).wait_recv()
            add(own_at(g, zz, 1 - y, x).at[:, columns(shapes[g], 0)], from_dx[g].at[zz])
            y_copy(g, zz).start()

        def take_y(full):
            part = slice(None) if full else columns(shapes[g], 1)
            diag_y(g, zz, full).wait_recv()
            add(own_at(g, zz, y, 1 - x).at[:, part], from_dy[g].at[zz, :, part])
            x_copy(g, zz).start()

        if not routed:
            take_x()
            take_y(False)
            return
        lean = t < planes - 2
        pl.when((x == 1) | jnp.logical_not(lean))(take_x)
        pl.when((x == 1) & lean)(lambda: take_y(True))
        pl.when((x == 0) | jnp.logical_not(lean))(lambda: take_y(False))

    def stage_line(g, t):
        zz = visit(t, z, planes)
        x_copy(g, zz).wait_recv()
        y_copy(g, zz).wait_recv()
        here = own_at(g, zz, y, x)

        @pl.when(t > 0)
        def _():
            add(here, from_x[g].at[zz], from_y[g].at[zz])
            farther = jnp.where(zz > z, z > 0, z < planes - 1)

            @pl.when(farther)
            def _():
                z_arrival(g, zz).wait_recv()
                add(here, from_z[g].at[zz])

            @pl.when(zz > z)
            def _():
                z_copy(g, zz, True).start()

            @pl.when(zz < z)
            def _():
                z_copy(g, zz, False).start()

        @pl.when(t == 0)
        def _():
            outs[g][...] = (
                here[...].astype(f32)
                + from_x[g][zz].astype(f32)
                + from_y[g][zz].astype(f32)
            )

            @pl.when(z > 0)
            def _():
                z_arrival(g, zz).wait_recv()
                outs[g][...] += from_z[g][zz].astype(f32)

            @pl.when(z < planes - 1)
            def _():
                z_arrival(g, planes).wait_recv()
                outs[g][...] += from_z[g][planes].astype(f32)

    def stage_end(g, t):
        zz = visit(t, z, planes)
        core_copy(g, zz).wait_send()

        def even():
            diag_x(g, zz).wait_send()
            diag_y(g, zz, False).wait_send()

        lean_or_even(t, lambda: diag_y(g, zz, True).wait_send(), even)
        x_copy(g, zz).wait_send()
        y_copy(g, zz).wait_send()

        @pl.when(t > 0)
        def _():
            z_copy(g, zz, True).wait_send()

    return Reduction(
        core_copy=core_copy, core=stage_core, plane=stage_plane, line=stage_line, end=stage_end
    )


def remote(src, dst, send, recv, target):
    return pltpu.make_async_remote_copy(
        src_ref=src,
        dst_ref=dst,
        send_sem=send,
        recv_sem=recv,
        device_id=target,
        device_id_type=MESH_ID,
    )


def scatter_kernel(planes, shapes, *refs):
    n = len(shapes)
    parts, refs = refs[:n], refs[n:]
    starts, query, *tiles, context, d_context, log_total, cos_table, sin_table = refs[:11]
    refs = refs[11:]
    outs, refs = refs[:n], refs[n:]
    d_query, d_key, d_value, first_grad = refs[:4]
    refs = refs[4:]
    mine, near, chip, far, from_b, from_d, tile_send, tile_recv, bias, acc = refs[-10:]
    own, boxes, own_sem, sems = refs[:n], refs[n : 7 * n], refs[7 * n], refs[7 * n + 1 : -10]
    z, y, x, c = position()
    entry_barrier(z, y, x, c, planes)
    f32 = jnp.float32
    push = remote

    def add(dst, src):
        dst[...] = (dst[...].astype(f32) + src[...].astype(f32)).astype(dst.dtype)

    def load(g, zz):
        return pltpu.make_async_copy(
            parts[g].at[zz, :, :, c], own[g].at[zz], own_sem.at[g, zz]
        )

    steps = reduction(
        planes,
        shapes,
        True,
        lambda g, zz, yy, xx: own[g].at[zz, yy, xx],
        lambda g, zz: parts[g].at[zz, :, :, 1 - c],
        lambda g, zz: load(g, zz).wait(),
        boxes,
        sems,
        outs,
    )

    partner = device(z, y, x, 1 - c)
    seqs, rows = mine.shape[1:3]
    pairs = mine.shape[3] // 128

    def send_b(s):
        return push(
            near.at[:, s], from_b.at[:, s], tile_send.at[0, s], tile_recv.at[0, s], partner
        )

    def send_d(s):
        return push(
            far.at[:, s], from_d.at[:, s], tile_send.at[1, s], tile_recv.at[1, s], partner
        )

    def send_back(s):
        return push(
            chip.at[:, s],
            chip.at[:, s],
            tile_send.at[2, s],
            tile_recv.at[2, s],
            device(z, y, 1 - x, c),
        )

    def unit(s, p):
        lanes = pl.ds(pl.multiple_of(p * 128, 128), 128)
        flat = pl.ds(pl.multiple_of(s * rows, rows), rows)
        two = lambda ref: [ref.at[0, s, :, lanes], ref.at[1, s, :, lanes]]
        attend_back_step(
            lax.axis_index("ctx"),
            p == 0,
            starts.at[s],
            query[s, :, lanes],
            [two(t) for t in tiles],
            context[s, :, lanes],
            d_context[s, :, lanes],
            log_total.at[s, p],
            cos_table.at[flat],
            sin_table.at[flat],
            d_query.at[s, :, lanes],
            [two(t) for t in (mine, near, chip, far)],
            bias,
            acc,
        )

    def work(i):
        @pl.when((i >= 2) & (i <= 2 * seqs) & (lax.rem(i, 2) == 0) & (x == 1))
        def _():
            s = lax.div(i, 2) - 1
            send_d(s).wait_recv()

            @pl.loop(0, 2 * rows // 32)
            def _(j):
                kind = lax.div(j, rows // 32)
                at = pl.ds(pl.multiple_of(lax.rem(j, rows // 32) * 32, 32), 32)
                add(chip.at[kind, s, at], from_d.at[kind, s, at])

            send_back(s).start()

        @pl.when((i >= 0) & (i < 2 * seqs))
        def _():
            s = lax.div(i, 2)

            @pl.loop(0, pairs // 2)
            def _(p):
                unit(s, lax.rem(i, 2) * (pairs // 2) + p)

            @pl.when(lax.rem(i, 2) == 1)
            def _():
                send_b(s).start()
                pl.when(x == 1)(lambda: send_d(s).start())

    def finish(s):
        send_b(s).wait_recv()
        pl.when(x == 0)(lambda: send_back(s).wait_recv())

        @pl.loop(0, rows // 32)
        def _(i):
            at = pl.ds(pl.multiple_of(i * 32, 32), 32)
            flat = pl.ds(pl.multiple_of(s * rows + i * 32, 32), 32)
            cos_rows, sin_rows = cos_table[flat, :], sin_table[flat, :]
            for k in range(pairs):
                lanes = pl.ds(k * 128, 128)

                def summed(kind):
                    return (
                        mine[kind, s, at, lanes].astype(f32)
                        + from_b[kind, s, at, lanes].astype(f32)
                        + jnp.where(x == 0, chip[kind, s, at, lanes].astype(f32), 0.0)
                    )

                d_key[flat, lanes] = turned(summed(0), cos_rows, sin_rows, -1.0).astype(jnp.bfloat16)
                half = 0.5 * summed(1)
                d_value[flat, lanes] = half.astype(jnp.bfloat16)
                first_grad[flat, lanes] = half

    @pl.loop(0, planes)
    def _(r):
        zz = visit(planes - 1 - r, z, planes)
        for g in range(n):
            steps.core_copy(g, zz).start()
            load(g, zz).start()

    @pl.loop(0, planes + 2)
    def _(r):
        t = planes - 1 - r
        for g in range(n):
            pl.when(r < planes)(lambda: steps.core(g, t))
        for g in range(n):
            if g == 0:
                work(2 * r - 2)
            pl.when((r >= 1) & (r < planes + 1))(lambda: steps.plane(g, t + 1))
        work(2 * r - 1)
        for g in range(n):
            pl.when(r >= 2)(lambda: steps.line(g, t + 2))
        pl.when((r >= planes) & (r < planes + seqs))(lambda: finish(r - planes))

    @pl.loop(0, planes)
    def _(t):
        for g in range(n):
            steps.end(g, t)

    for s in range(2, seqs):
        finish(s)
    for s in range(seqs):
        send_b(s).wait_send()

        @pl.when(x == 1)
        def _():
            send_d(s).wait_send()
            send_back(s).wait_send()


def boxes_of(planes, shapes, types):
    def boxes(lead, narrow=False):
        out = []
        for s, d in zip(shapes, types):
            width = s[1] // 2 // 128 * 128 if narrow else s[1]
            out.append(pltpu.VMEM((*lead, s[0], width), d))
        return out

    return [
        *boxes((planes, 2, 2)),
        *boxes((planes,), True),
        *boxes((planes,)),
        *boxes((planes,)),
        *boxes((planes,)),
        *boxes((planes + 1,)),
    ]


def sems_of(planes, n):
    dma = pltpu.SemaphoreType.DMA
    return [
        dma((n, planes)),
        dma((n, planes)),
        dma((n, planes, 2)),
        dma((n, planes, 2)),
        dma((n, planes)),
        dma((n, planes)),
        dma((n, planes)),
        dma((n, planes)),
        dma((n, planes)),
        dma((n, planes + 1)),
    ]


def scatter_sum(planes, partials, attention):
    n = len(partials)
    partials = [
        p.reshape(planes, 2, 2, 2, p.shape[0] // (planes * 8), p.shape[1]) for p in partials
    ]
    shapes = [p.shape[4:] for p in partials]
    bf16 = jnp.bfloat16
    dma = pltpu.SemaphoreType.DMA
    box = attention[2].shape
    seqs, rows, width = box[1:]
    flat = (seqs * rows, width)
    vmem = pl.BlockSpec(memory_space=pltpu.VMEM)
    return pl.pallas_call(
        functools.partial(scatter_kernel, planes, shapes),
        out_shape=[jax.ShapeDtypeStruct(s, jnp.float32) for s in shapes]
        + [
            jax.ShapeDtypeStruct(box[1:], bf16),
            jax.ShapeDtypeStruct(flat, bf16),
            jax.ShapeDtypeStruct(flat, bf16),
            jax.ShapeDtypeStruct(flat, jnp.float32),
        ],
        in_specs=[pl.BlockSpec(memory_space=pl.ANY)] * n + [vmem] * len(attention),
        out_specs=[vmem] * (n + 4),
        scratch_shapes=[
            *[pltpu.VMEM((planes, 2, 2, *s), bf16) for s in shapes],
            *boxes_of(planes, shapes, [bf16] * n),
            dma((n, planes)),
            *sems_of(planes, n),
            *[pltpu.VMEM(box, bf16)] * 6,
            dma((3, seqs)),
            dma((3, seqs)),
            *attend_back_scratch(rows),
        ],
        compiler_params=pltpu.CompilerParams(
            collective_id=1, has_side_effects=True, vmem_limit_bytes=67043328
        ),
        name="gradient_scatter",
    )(*partials, *attention)


def last_kernel(planes, shapes, *refs):
    f32, bf16 = jnp.float32, jnp.bfloat16
    n = len(shapes)
    normed, *d_proj = refs[:4]
    w_in, tok_in, d_residual_in, attn_gain, d_ffn_gain = refs[4:7], *refs[7:11]
    outs, token_grad = refs[11 : 11 + n], refs[11 + n]
    refs = refs[12 + n :]
    weights, tok, d_residual, gain_sum = refs[:3], *refs[3:6]
    parts, boxes, sems, load_sem = refs[6 : 6 + n], refs[6 + n : 6 + 7 * n], refs[6 + 7 * n : -1], refs[-1]
    z, y, x, c = position()
    loads = [
        pltpu.make_async_copy(src, dst, load_sem.at[i])
        for i, (src, dst) in enumerate(zip([*w_in, tok_in, d_residual_in], [*weights, tok, d_residual]))
    ]
    for copy in loads:
        copy.start()
    entry_barrier(z, y, x, c, planes)
    rows, width = tok.shape
    steps = reduction(
        planes,
        shapes,
        False,
        lambda g, zz, yy, xx: parts[g].at[zz, yy, xx, c],
        lambda g, zz: parts[g].at[zz, :, :, 1 - c],
        lambda g, zz: None,
        boxes,
        sems,
        outs,
    )
    at_once = planes * 256 // width

    def weight_grads(j):
        lanes = pl.ds(pl.multiple_of(j * 256, 256), 256)
        for g in range(3):
            part = lax.dot_general(normed[:, lanes], d_proj[g][...], TN, preferred_element_type=f32)
            shape = (at_once, 2, 2, 2, *shapes[g])
            parts[g][pl.ds(j * at_once, at_once)] = part.reshape(shape).astype(bf16)

    each = max(width // 256 // planes, 1)

    def normed_grad(r):
        @pl.when(r == 0)
        def _():
            for copy in loads:
                copy.wait()

        @pl.loop(r * each, r * each + each)
        def _(j):
            at = pl.ds(pl.multiple_of(j * 256, 256), 256)
            total = 0.0
            for g in range(3):
                total = total + lax.dot_general(
                    d_proj[g][...], weights[g][at, :], NT, preferred_element_type=f32
                )
            token_grad[:, at] = total

    def token_gradient():
        gain_sum[...] = jnp.zeros_like(gain_sum)

        @pl.loop(0, rows // 64)
        def _(i):
            at = pl.ds(pl.multiple_of(i * 64, 64), 64)
            values = tok[at, :].astype(f32)
            scale = inverse_rms(values)
            d_normed = token_grad[at, :]
            products = d_normed * values * scale
            gain_sum[...] += jnp.sum(products.reshape(8, 8, width), axis=0)
            weighted = d_normed * attn_gain[...]
            token_grad[at, :] = (
                d_residual[at, :]
                + scale * weighted
                - values * (scale * scale * scale) * jnp.mean(weighted * values, axis=-1, keepdims=True)
            )

        both = jnp.concatenate(
            [jnp.sum(gain_sum[...], axis=0, keepdims=True), d_ffn_gain[...], jnp.zeros((6, width), f32)]
        )
        per = planes * 8 * 256 // width
        for i in range(planes * 8):
            at = i // per * 256
            parts[3][i // 8, i // 4 % 2, i // 2 % 2, i % 2] = both[:, at : at + 256]

    def send_cores(g, t):
        steps.core_copy(g, visit(t, z, planes)).start()

    if at_once > 1:
        pl.loop(0, width // 256)(weight_grads)
    @pl.loop(0, planes + 4)
    def _(r):
        t = planes - 1 - r

        @pl.when(r < planes)
        def _():
            if at_once == 1:
                weight_grads(visit(t, z, planes))
            for g in range(3):
                send_cores(g, t)

        for behind, step in ((1, steps.core), (2, steps.plane), (3, steps.line)):
            for g in range(3):
                pl.when((r >= behind) & (r < planes + behind))(lambda: step(g, t + behind))

            @pl.when(r == planes + behind)
            def _():
                @pl.loop(0, planes)
                def _(i):
                    step(3, planes - 1 - i)

        @pl.when(r < width // 256 // each)
        def _():
            normed_grad(r)

        @pl.when(r == planes)
        def _():
            token_gradient()

            @pl.loop(0, planes)
            def _(i):
                send_cores(3, i)

    @pl.loop(0, planes)
    def _(t):
        for g in range(n):
            steps.end(g, t)


def last(planes, normed, d_proj, weights, tok, d_residual, attn_gain, d_ffn_gain):
    f32, bf16 = jnp.float32, jnp.bfloat16
    width = tok.shape[1]
    shapes = [(width // (planes * 8), width)] * 3 + [(8, 256)]
    types = [bf16] * 3 + [f32]
    n = len(shapes)
    vmem, anywhere = pl.BlockSpec(memory_space=pltpu.VMEM), pl.BlockSpec(memory_space=pl.ANY)
    return pl.pallas_call(
        functools.partial(last_kernel, planes, shapes),
        out_shape=[jax.ShapeDtypeStruct(s, f32) for s in [*shapes, tok.shape]],
        in_specs=[vmem] * 4 + [anywhere] * 5 + [vmem] * 2,
        out_specs=[vmem] * (n + 1),
        scratch_shapes=[
            *[pltpu.VMEM((width, width), bf16)] * 3,
            pltpu.VMEM(tok.shape, bf16),
            pltpu.VMEM(tok.shape, f32),
            pltpu.VMEM((8, width), f32),
            *[pltpu.VMEM((planes, 2, 2, 2, *s), d) for s, d in zip(shapes, types)],
            *boxes_of(planes, shapes, types),
            *sems_of(planes, n),
            pltpu.SemaphoreType.DMA((5,)),
        ],
        compiler_params=pltpu.CompilerParams(
            collective_id=2, has_side_effects=True, vmem_limit_bytes=67043328
        ),
        name="last",
    )(normed, *d_proj, *weights, tok, d_residual, attn_gain, d_ffn_gain)


def deliver(arrays):
    n = len(arrays)

    def kernel(*refs):
        for src, dst in zip(refs[:n], refs[n:]):
            dst[...] = src[...]

    specs = [pl.BlockSpec((a.shape[0], a.shape[1] // 2), lambda i: (0, i)) for a in arrays]
    return pl.pallas_call(
        kernel,
        grid=(2,),
        in_specs=specs,
        out_specs=specs,
        out_shape=[jax.ShapeDtypeStruct(a.shape, a.dtype) for a in arrays],
        name="deliver",
    )(*arrays)


def on_device(
    planes,
    tokens,
    first_values,
    cotangent,
    segment_ids,
    attn_gain,
    w_query,
    w_key,
    w_value,
    w_out,
    ffn_gain,
    gate_weight,
    up_weight,
    down_weight,
):
    f32, bf16 = jnp.float32, jnp.bfloat16
    seqs, rows, width = tokens.shape
    rank = lax.axis_index("ctx")
    share = attn_gain.shape[0]
    per = 128 // share
    index = lax.axis_index("dp") * lax.axis_size("ctx") + rank
    place = lax.rem(index, per)
    lane = jnp.arange(128, dtype=jnp.int32)[None, :] - place * share
    here = lane == jnp.arange(share, dtype=jnp.int32)[:, None]
    spread = lambda gain: jnp.sum(jnp.where(here, gain.astype(f32)[:, None], 0.0), axis=0)
    kind = jnp.arange(16, dtype=jnp.int32)[:, None]
    gains = jnp.where(kind == 0, spread(attn_gain), jnp.where(kind == 1, spread(ffn_gain), 0.0))
    gains = gains.astype(bf16)
    starts, cos_table, sin_table = tables(segment_ids, rank, rows)
    flat = (seqs * rows, width)
    local = (seqs, rows, width)
    tokens = tokens.reshape(flat)
    mm = functools.partial(jnp.dot, preferred_element_type=f32)
    by_rows = lambda a, b: lax.dot_general(a, b, TN, preferred_element_type=f32).astype(bf16)
    back = lambda a, b: lax.dot_general(a, b, NT, preferred_element_type=f32)
    (gains, w_query, w_key, w_value, w_out, gate_weight, up_weight, down_weight), (
        normed_one,
        query_rot,
        *tiles,
        context3,
        log_total,
    ) = forward(
        planes,
        4,
        [gains, w_query, w_key, w_value, w_out, gate_weight, up_weight, down_weight],
        tokens,
        first_values.reshape(flat),
        starts,
        cos_table,
        sin_table,
    )
    gains = jnp.sum(gains.reshape(width // 128, per, 16, 128), axis=1)
    attn_gain = gains[:, 0].reshape(1, width)
    ffn_gain = gains[:, 1].reshape(1, width)
    context = context3.reshape(flat)
    tokens_float = tokens.astype(f32)
    cotangent = cotangent.reshape(flat)
    residual = tokens_float + mm(context, w_out)
    scale_two = inverse_rms(residual)
    second_normed = (residual * scale_two * ffn_gain.astype(f32)).astype(bf16)
    gate = mm(second_normed, gate_weight)
    up = mm(second_normed, up_weight)
    hidden = (swish(gate) * up).astype(bf16)
    output = (residual + mm(hidden, down_weight)).astype(bf16)

    out_float = cotangent.astype(f32)
    d_down = by_rows(hidden, cotangent)
    d_hidden = back(cotangent, down_weight)
    sigmoid_gate = jax.nn.sigmoid(gate)
    d_gate = (d_hidden * up * sigmoid_gate * (1.0 + gate * (1.0 - sigmoid_gate))).astype(bf16)
    d_up = (d_hidden * (gate * sigmoid_gate)).astype(bf16)
    d_gate_weight = by_rows(second_normed, d_gate)
    d_up_weight = by_rows(second_normed, d_up)
    d_normed_two = back(d_gate, gate_weight) + back(d_up, up_weight)
    d_ffn_gain = jnp.sum(d_normed_two * residual * scale_two, axis=0)
    weighted_two = d_normed_two * ffn_gain.astype(f32)
    d_residual = (
        out_float
        + scale_two * weighted_two
        - residual
        * (scale_two * scale_two * scale_two)
        * jnp.mean(weighted_two * residual, axis=-1, keepdims=True)
    )
    d_residual_low = d_residual.astype(bf16)
    d_out = by_rows(context, d_residual_low)
    d_context = back(d_residual_low, w_out).astype(bf16).reshape(local)
    s_down, s_gate, s_up, s_out, d_query, d_key, d_value, first_grad = scatter_sum(
        planes,
        [d_down, d_gate_weight, d_up_weight, d_out],
        [starts, query_rot, *tiles, context3, d_context, log_total, cos_table, sin_table],
    )
    d_query = d_query.reshape(flat)
    s_wq, s_wk, s_wv, s_gains, token_grad = last(
        planes,
        normed_one,
        [d_query, d_key, d_value],
        [w_query, w_key, w_value],
        tokens,
        d_residual,
        attn_gain.astype(f32),
        d_ffn_gain[None],
    )
    token_grad, first_grad, s_wq, s_wk, s_wv, s_out, s_gate, s_up, s_down = deliver(
        [token_grad, first_grad, s_wq, s_wk, s_wv, s_out, s_gate, s_up, s_down]
    )
    slot = lax.rem(index, 256 // share) * share
    s_gains = lax.dynamic_slice_in_dim(s_gains[:2], slot, share, 1)
    return (
        output.reshape(local),
        token_grad.reshape(local),
        first_grad.reshape(local),
        s_gains[0],
        s_wq,
        s_wk,
        s_wv,
        s_out,
        s_gains[1],
        s_gate,
        s_up,
        s_down,
    )


def solution(mesh):
    token, weight, vector = P("dp", "ctx", None), P(("dp", "ctx"), None), P(("dp", "ctx"))
    return jax.shard_map(
        functools.partial(on_device, mesh.shape["dp"] // 2),
        mesh=mesh,
        in_specs=(
            token,
            token,
            token,
            P("dp", None),
            vector,
            weight,
            weight,
            weight,
            weight,
            vector,
            weight,
            weight,
            weight,
        ),
        out_specs=(
            token,
            token,
            token,
            vector,
            weight,
            weight,
            weight,
            weight,
            vector,
            weight,
            weight,
            weight,
        ),
        check_vma=False,
    )
```

```python
import functools
import jax
import jax.numpy as jnp
from jax import lax
from jax.experimental import pallas as pl
from jax.experimental.pallas import tpu as pltpu
from jax.sharding import PartitionSpec as P

HEADS = 16
HEAD_DIM = 64
MESH_ID = pl.DeviceIdType.MESH

epsilon = 1e-05
rope_base = 10000.0
score_scale = 0.125
masked_score = -1e30


def inverse_rms(values):
    return lax.rsqrt(jnp.mean(values * values, axis=-1, keepdims=True) + epsilon)


def swish(values):
    return values * jax.nn.sigmoid(values)


def first_half(shape):
    return lax.broadcasted_iota(jnp.int32, shape, len(shape) - 1) % HEAD_DIM < HEAD_DIM // 2


def swap_halves(values):
    return jnp.where(
        first_half(values.shape), pltpu.roll(values, 96, 1), pltpu.roll(values, 32, 1)
    )


def turned(values, cos_table, sin_table, sign):
    return values * cos_table + sign * (swap_halves(values) * sin_table)


def tables(segment_ids, rank, rows):
    seqs = segment_ids.shape[0]
    own_ids = lax.dynamic_slice_in_dim(segment_ids, rank * rows, rows, 1)
    earlier = segment_ids[:, :, None] < own_ids[:, None, :]
    starts = jnp.sum(earlier.astype(jnp.int32), axis=1)
    local = rank * rows + jnp.arange(rows, dtype=jnp.int32) - starts
    lane = jnp.arange(128, dtype=jnp.int32)
    half = HEAD_DIM // 2
    frequency = rope_base ** (-(lane % half).astype(jnp.float32) * 2.0 / HEAD_DIM)
    angles = local.astype(jnp.float32).reshape(seqs * rows, 1) * frequency
    sign = jnp.where(lane % HEAD_DIM < half, -1.0, 1.0)
    return starts.reshape(seqs, 1, rows), jnp.cos(angles), jnp.sin(angles) * sign


def normalise(tok, gain, normed):
    rows = tok.shape[0]

    @pl.loop(0, rows // 64)
    def _(i):
        at = pl.ds(pl.multiple_of(i * 64, 64), 64)
        values = tok[at, :].astype(jnp.float32)
        normed[at, :] = (values * inverse_rms(values) * gain).astype(jnp.bfloat16)


def columns_of(weight, lanes):
    block = weight[:, :, lanes]
    if block.shape[1] % 16:
        block = block.astype(jnp.float32)
    return block.reshape(block.shape[0] * block.shape[1], block.shape[2]).astype(jnp.bfloat16)


def project(normed, first, wq, wk, wv, cos_ref, sin_ref, query, pair):
    f32, bf16 = jnp.float32, jnp.bfloat16
    seqs, rows, width = query.shape

    @pl.loop(0, width // 256)
    def _(i):
        lanes = pl.ds(pl.multiple_of(i * 256, 256), 256)
        n1 = normed[...]
        cos_table, sin_table = cos_ref[...], sin_ref[...]
        queries = jnp.dot(n1, columns_of(wq, lanes), preferred_element_type=f32)
        keys = jnp.dot(n1, columns_of(wk, lanes), preferred_element_type=f32)
        values = jnp.dot(n1, columns_of(wv, lanes), preferred_element_type=f32)
        mixed = (0.5 * values + 0.5 * first[:, lanes].astype(f32)).astype(bf16)
        for half in range(2):
            part = slice(half * 128, half * 128 + 128)
            at = pl.ds(pl.multiple_of(i * 256 + half * 128, 128), 128)
            q = turned(queries[:, part], cos_table, sin_table, 1.0).astype(bf16)
            k = turned(keys[:, part], cos_table, sin_table, 1.0).astype(bf16)
            for s in range(seqs):
                query[s, :, at] = q[s * rows : (s + 1) * rows]
                pair[0, s, :, at] = k[s * rows : (s + 1) * rows]
                pair[1, s, :, at] = mixed[s * rows : (s + 1) * rows, part]


def two_heads(block, scale):
    lane = lax.broadcasted_iota(jnp.int32, block.shape, 1)
    scaled = block * jnp.asarray(scale, block.dtype)
    zero = jnp.zeros_like(block)
    return jnp.concatenate(
        [jnp.where(lane < HEAD_DIM, scaled, zero), jnp.where(lane < HEAD_DIM, zero, scaled)]
    )


def own_lanes(both):
    rows = both.shape[1] // 2
    lane = lax.broadcasted_iota(jnp.int32, (both.shape[0], rows), 0)
    return jnp.where(lane < HEAD_DIM, both[:, :rows], both[:, rows:]).T


def fill_bias(bias, starts, rank):
    rows = bias.shape[1]
    key = lax.broadcasted_iota(jnp.int32, (rows, rows), 0)
    place = rank * rows + lax.broadcasted_iota(jnp.int32, (rows, rows), 1)
    begin = starts[...]
    for t in range(4):
        x, c = lax.div(rank, 2), lax.rem(rank, 2)
        owner = (1 - x if t >= 2 else x) * 2 + (1 - c if t % 2 else c)
        at = owner * rows + key
        bias[t] = jnp.where((at >= begin) & (at <= place), 0.0, masked_score)


NT = (((1,), (1,)), ((), ()))
TN = (((0,), (0,)), ((), ()))


def attend_step(rank, begin, starts, q, tiles, out, log_total, bias, scores, peak, total, acc):
    f32, bf16 = jnp.float32, jnp.bfloat16

    @pl.when(begin)
    def _():
        fill_bias(bias, starts, rank)

    high = rank >= 2
    stacked = two_heads(q, score_scale)

    def score(t):
        s = lax.dot_general(tiles[t][0][...], stacked, NT, preferred_element_type=f32)
        s = s + jnp.concatenate([bias[t], bias[t]], axis=1)
        scores[t] = s
        return jnp.max(s, axis=0, keepdims=True)

    def gather_values(t, top):
        e = jnp.exp(scores[t] - top)
        part = lax.dot_general(tiles[t][1][...], e.astype(bf16), TN, preferred_element_type=f32)
        return jnp.sum(e, axis=0, keepdims=True), part

    peak[...] = jnp.maximum(score(0), score(1))

    @pl.when(high)
    def _():
        peak[...] = jnp.maximum(peak[...], jnp.maximum(score(2), score(3)))

    top = peak[...]
    sum_a, acc_a = gather_values(0, top)
    sum_b, acc_b = gather_values(1, top)
    total[...] = sum_a + sum_b
    acc[...] = acc_a + acc_b

    @pl.when(high)
    def _():
        top = peak[...]
        sum_a, acc_a = gather_values(2, top)
        sum_b, acc_b = gather_values(3, top)
        total[...] += sum_a + sum_b
        acc[...] += acc_a + acc_b

    out[...] = own_lanes(acc[...] / total[...]).astype(bf16)
    log_total[...] = peak[...] + jnp.log(total[...])


def attend_scratch(rows):
    return [
        pltpu.VMEM((4, rows, rows), jnp.float32),
        pltpu.VMEM((4, rows, 2 * rows), jnp.float32),
        pltpu.VMEM((1, 2 * rows), jnp.float32),
        pltpu.VMEM((1, 2 * rows), jnp.float32),
        pltpu.VMEM((128, 2 * rows), jnp.float32),
    ]


def attend_back_step(
    rank, begin, starts, q, tiles, context, d_context, log_total, cos_t, sin_t, d_q, d_tiles, bias, acc
):
    f32, bf16 = jnp.float32, jnp.bfloat16

    @pl.when(begin)
    def _():
        fill_bias(bias, starts, rank)

    high = rank >= 2
    stacked = two_heads(q, score_scale)
    stacked_do = two_heads(d_context, 1.0)
    turned_product = (d_context.astype(f32) * context.astype(f32)).T
    delta = jnp.concatenate(
        [
            jnp.sum(turned_product[:HEAD_DIM], axis=0, keepdims=True),
            jnp.sum(turned_product[HEAD_DIM:], axis=0, keepdims=True),
        ],
        axis=1,
    )
    lse = log_total[...]

    def one(t):
        keys, values = tiles[t][0][...], tiles[t][1][...]
        s = lax.dot_general(keys, stacked, NT, preferred_element_type=f32)
        s = s + jnp.concatenate([bias[t], bias[t]], axis=1)
        p = jnp.exp(s - lse)
        dp = lax.dot_general(values, stacked_do, NT, preferred_element_type=f32)
        ds = (p * (dp - delta)).astype(bf16)
        d_tiles[t][1][...] = jnp.dot(p.astype(bf16), stacked_do, preferred_element_type=f32).astype(bf16)
        d_tiles[t][0][...] = jnp.dot(ds, stacked, preferred_element_type=f32).astype(bf16)
        return lax.dot_general(keys, ds, TN, preferred_element_type=f32)

    acc[...] = one(0) + one(1)

    @pl.when(high)
    def _():
        acc[...] += one(2) + one(3)

    d_q[...] = turned(own_lanes(acc[...]) * score_scale, cos_t[...], sin_t[...], -1.0).astype(bf16)


def attend_back_scratch(rows):
    return [pltpu.VMEM((4, rows, rows), jnp.float32), pltpu.VMEM((128, 2 * rows), jnp.float32)]


def position():
    dp = lax.axis_index("dp")
    ct = lax.axis_index("ctx")
    return lax.div(dp, 2), lax.rem(dp, 2), lax.div(ct, 2), lax.rem(ct, 2)


def visit(step, z, planes):
    back = planes - 1 - step
    high = back + jnp.where(back >= z, 1, 0)
    low = planes - 1 - back
    low = low - jnp.where(low <= z, 1, 0)
    other = jnp.where(z < planes // 2, low, high)
    return jnp.where(step == 0, z, other)


def device(z, y, x, c):
    return (z * 2 + y, x * 2 + c)


def halves(shape):
    if shape[0] % 2 == 0:
        cut = shape[0] // 2
        return (pl.ds(0, cut), slice(None), slice(None)), (pl.ds(cut, cut), slice(None), slice(None))
    cut = shape[2] // 2 // 128 * 128
    return (
        (slice(None), slice(None), pl.ds(0, cut)),
        (slice(None), slice(None), pl.ds(cut, shape[2] - cut)),
    )


def entry_barrier(z, y, x, c, planes):
    barrier = pltpu.get_barrier_semaphore()

    def hello(target):
        pl.semaphore_signal(barrier, inc=1, device_id=target, device_id_type=MESH_ID)

    hello(device(z, y, 1 - x, c))
    hello(device(z, 1 - y, x, c))
    hello(device(z, y, x, 1 - c))

    @pl.when(z > 0)
    def _():
        hello(device(z - 1, y, x, c))

    @pl.when(z < planes - 1)
    def _():
        hello(device(z + 1, y, x, c))

    pl.semaphore_wait(barrier, 3 + jnp.where(z > 0, 1, 0) + jnp.where(z < planes - 1, 1, 0))


def forward_kernel(planes, shapes, first_group, *refs):
    n = len(shapes)
    ins, refs = refs[:n], refs[n:]
    tok, first, starts, cos_table, sin_table = refs[:5]
    outs, refs = refs[5 : 5 + n], refs[5 + n :]
    *results, log_total, attn_gain, ffn_gain = refs[:10]
    sems, refs = refs[10:21], refs[21:]
    normed, query, mine, near, chip, far, context = held = refs[:7]
    store_sem, refs = refs[7], refs[8:]
    stores = [
        pltpu.make_async_copy(src, dst, store_sem.at[i])
        for i, (src, dst) in enumerate(zip(held, results))
    ]
    own_sem, z_send, z_recv, x_send, x_recv, y_send, y_recv, d_send, d_recv, c_send, c_recv = sems
    tile_send, tile_recv, load_sem, gains, *weights = refs[: 4 + first_group - 1]
    scratch = refs[4 + first_group - 1 :]
    z, y, x, c = position()
    entry_barrier(z, y, x, c, planes)
    local = [
        pltpu.make_async_copy(ins[g], outs[g].at[:, z, y, x, c], own_sem.at[g]) for g in range(n)
    ]
    for copy in local:
        copy.start()

    def push(src, dst, send, recv, target):
        return pltpu.make_async_remote_copy(
            src_ref=src,
            dst_ref=dst,
            send_sem=send,
            recv_sem=recv,
            device_id=target,
            device_id_type=MESH_ID,
        )

    def spot(g, zz, yy, xx):
        return outs[g].at[:, zz, yy, xx, c]

    def z_copy(g, zz, up, own):
        side = 1 if up else 0
        return push(
            ins[g] if own else spot(g, zz, y, x),
            spot(g, zz, y, x),
            z_send.at[g, zz, side],
            z_recv.at[g, zz],
            device(z + 1 if up else z - 1, y, x, c),
        )

    def x_copy(g, zz, own):
        return push(
            ins[g] if own else spot(g, zz, y, x),
            spot(g, zz, y, x),
            x_send.at[g, zz],
            x_recv.at[g, zz],
            device(z, y, 1 - x, c),
        )

    def y_copy(g, zz, own):
        return push(
            ins[g] if own else spot(g, zz, y, x),
            spot(g, zz, y, x),
            y_send.at[g, zz],
            y_recv.at[g, zz],
            device(z, 1 - y, x, c),
        )

    def relay(g, zz, half, by_y):
        here = spot(g, zz, y, 1 - x) if by_y else spot(g, zz, 1 - y, x)
        here = here.at[halves(shapes[g])[half]]
        return push(
            here,
            here,
            d_send.at[g, zz, 2 * half if by_y else 1],
            d_recv.at[g, zz, half],
            device(z, 1 - y, x, c) if by_y else device(z, y, 1 - x, c),
        )

    def diag_arrival(g, zz, half):
        here = spot(g, zz, 1 - y, 1 - x).at[halves(shapes[g])[half]]
        return push(
            here, here, d_send.at[g, zz, half], d_recv.at[g, zz, half], device(z, y, x, 1 - c)
        )

    def core_copy(g, zz, mine):
        here = outs[g].at[:, zz, :, :, c if mine else 1 - c]
        return push(here, here, c_send.at[g, zz], c_recv.at[g, zz], device(z, y, x, 1 - c))

    def on_links(g, t, act):
        zz = visit(t, z, planes)

        def both(own):
            up = (z < planes - 1) if own else (zz < z) & (z < planes - 1)
            down = (z > 0) if own else (zz > z) & (z > 0)
            pl.when(down)(lambda: act(z_copy(g, zz, False, own)))
            pl.when(up)(lambda: act(z_copy(g, zz, True, own)))
            act(x_copy(g, zz, own))
            act(y_copy(g, zz, own))

        pl.when(t == 0)(lambda: both(True))
        pl.when(t > 0)(lambda: both(False))

    def on_relays(g, t, act, between=lambda: None):
        zz = visit(t, z, planes)
        act(relay(g, zz, 0, True))
        if g < first_group:
            between()
            act(relay(g, zz, 1, False))
            return
        lean = t < planes - 1
        pl.when(lean & (x == 1))(lambda: act(relay(g, zz, 1, True)))
        between()
        pl.when((x == 1) | jnp.logical_not(lean))(lambda: act(relay(g, zz, 1, False)))

    def start(copy):
        copy.start()

    def wait_send(copy):
        copy.wait_send()

    def stage_line(g, t):
        @pl.when(t > 0)
        def _():
            z_copy(g, visit(t, z, planes), True, False).wait_recv()

        on_links(g, t, start)

    def stage_plane(g, t):
        zz = visit(t, z, planes)
        x_copy(g, zz, False).wait_recv()
        on_relays(g, t, start, lambda: y_copy(g, zz, False).wait_recv())

    def stage_core(g, t):
        zz = visit(t, z, planes)
        pl.when(t == 0)(lambda: local[g].wait())
        diag_arrival(g, zz, 0).wait_recv()
        diag_arrival(g, zz, 1).wait_recv()
        core_copy(g, zz, True).start()

    seqs, rows, width = query.shape
    pairs = width // 128
    partner = device(z, y, x, 1 - c)

    def to_partner(s):
        return push(
            mine.at[:, s], near.at[:, s], tile_send.at[0, s], tile_recv.at[0, s], partner
        )

    def to_x(s):
        return push(
            mine.at[:, s],
            chip.at[:, s],
            tile_send.at[1, s],
            tile_recv.at[1, s],
            device(z, y, 1 - x, c),
        )

    def passed_on(s):
        return push(
            chip.at[:, s], far.at[:, s], tile_send.at[2, s], tile_recv.at[2, s], partner
        )

    def send_tiles(s):
        to_partner(s).start()
        pl.when(x == 0)(lambda: to_x(s).start())

    def projection():
        @pl.loop(0, planes)
        def _(t):
            for g in range(first_group):
                core_copy(g, visit(t, z, planes), False).wait_recv()

        loads = [
            pltpu.make_async_copy(outs[g].at[0], buf, load_sem.at[g])
            for g, buf in enumerate([gains, *weights])
        ]
        for copy in loads:
            copy.start()
        loads[0].wait()
        flat_gains = [gains[i, j, k, m] for i in range(planes) for j in (0, 1) for k in (0, 1) for m in (0, 1)]
        per = len(flat_gains) * 128 // width
        gain = jnp.concatenate(
            [
                sum(b[:2].astype(jnp.float32) for b in flat_gains[i * per : (i + 1) * per])
                for i in range(width // 128)
            ],
            axis=1,
        )
        attn_gain[...] = gain[:1]
        ffn_gain[...] = gain[1:]
        normalise(tok, gain[:1], normed)
        for copy in loads[1:]:
            copy.wait()
        as_blocks = lambda w: w.reshape((planes * 8, *w.shape[4:]))
        project(
            normed, first, *[as_blocks(w) for w in weights], cos_table, sin_table, query, mine
        )
        for s in range(seqs):
            send_tiles(s)
        for copy in stores[:3]:
            copy.start()

    def unit(s, p):
        lanes = pl.ds(pl.multiple_of(p * 128, 128), 128)
        attend_step(
            lax.axis_index("ctx"),
            p == 0,
            starts.at[s],
            query[s, :, lanes],
            [[w.at[0, s, :, lanes], w.at[1, s, :, lanes]] for w in (mine, near, chip, far)],
            context.at[s, :, lanes],
            log_total.at[s, p],
            *scratch,
        )

    def attention():
        @pl.loop(0, seqs)
        def _(s):
            to_partner(s).wait_recv()

            @pl.when(x == 1)
            def _():
                to_x(s).wait_recv()
                passed_on(s).start()
                passed_on(s).wait_recv()

            @pl.loop(0, pairs)
            def _(p):
                unit(s, p)

        for copy in (stores[3], stores[6]):
            copy.start()

        @pl.when(x == 1)
        def _():
            stores[4].start()
            stores[5].start()

    groups = (range(first_group), range(first_group, n))

    @pl.loop(0, 2 * planes + 2)
    def _(r):
        for stage, lag in ((stage_line, 0), (stage_plane, 1), (stage_core, 2)):
            for k, group in enumerate(groups):
                t = r - k * planes - lag
                for g in group:
                    pl.when((t >= 0) & (t < planes))(lambda: stage(g, t))
            if lag == 0:
                pl.when(r == planes + 3)(attention)
        pl.when(r == planes + 1)(projection)

    @pl.loop(0, planes)
    def _(t):
        zz = visit(t, z, planes)
        for g in range(n):
            if g >= first_group:
                core_copy(g, zz, False).wait_recv()
            core_copy(g, zz, True).wait_send()
            on_links(g, t, wait_send)
            on_relays(g, t, wait_send)

    for s in range(seqs):
        to_partner(s).wait_send()
        pl.when(x == 0)(lambda: to_x(s).wait_send())
        pl.when(x == 1)(lambda: passed_on(s).wait_send())
    for copy in (*stores[:4], stores[6]):
        copy.wait()

    @pl.when(x == 1)
    def _():
        stores[4].wait()
        stores[5].wait()


def forward(planes, first_group, blocks, tok, first, starts, cos_table, sin_table):
    blocks = [b[None] for b in blocks]
    n = len(blocks)
    shapes = [b.shape for b in blocks]
    seqs, _, rows = starts.shape
    width = tok.shape[1]
    bf16 = jnp.bfloat16
    dma = pltpu.SemaphoreType.DMA
    anywhere = pl.BlockSpec(memory_space=pl.ANY)
    vmem = pl.BlockSpec(memory_space=pltpu.VMEM)
    local = jax.ShapeDtypeStruct((seqs, rows, width), bf16)
    tile = jax.ShapeDtypeStruct((2, seqs, rows, width), bf16)
    got = pl.pallas_call(
        functools.partial(forward_kernel, planes, shapes, first_group),
        out_shape=[
            jax.ShapeDtypeStruct((s[0], planes, 2, 2, 2, s[1], s[2]), b.dtype)
            for s, b in zip(shapes, blocks)
        ]
        + [jax.ShapeDtypeStruct(tok.shape, bf16), local, *[tile] * 4, local]
        + [jax.ShapeDtypeStruct((seqs, width // 128, 1, 2 * rows), jnp.float32)]
        + [jax.ShapeDtypeStruct((1, width), jnp.float32)] * 2,
        in_specs=[anywhere] * n + [vmem] * 5,
        out_specs=[anywhere] * (n + 7) + [vmem] * 3,
        scratch_shapes=[
            dma((n,)),
            dma((n, planes, 2)),
            dma((n, planes)),
            dma((n, planes)),
            dma((n, planes)),
            dma((n, planes)),
            dma((n, planes)),
            dma((n, planes, 3)),
            dma((n, planes, 2)),
            dma((n, planes)),
            dma((n, planes)),
            *[pltpu.VMEM(h.shape, bf16) for h in [tok, local, *[tile] * 4, local]],
            dma((7,)),
            dma((3, seqs)),
            dma((3, seqs)),
            dma((first_group,)),
            *[pltpu.VMEM((planes, 2, 2, 2, *s[1:]), bf16) for s in shapes[:first_group]],
            *attend_scratch(rows),
        ],
        compiler_params=pltpu.CompilerParams(
            collective_id=0, has_side_effects=True, vmem_limit_bytes=67043328
        ),
        name="forward",
    )(*blocks, tok, first, starts, cos_table, sin_table)
    full = [g.reshape(planes * 8 * s[1], s[2]) for g, s in zip(got, shapes)]
    return full, got[n:]


def columns(shape, half):
    cut = shape[1] // 2 // 128 * 128
    return pl.ds(0, cut) if half == 0 else pl.ds(cut, shape[1] - cut)


class Reduction:
    def __init__(self, **steps):
        self.__dict__.update(steps)


def reduction(planes, shapes, routed, own_at, away_at, before_core, boxes, sems, outs):
    n = len(shapes)
    from_core, from_dx, from_dy, from_x, from_y, from_z = (
        boxes[k * n : (k + 1) * n] for k in range(6)
    )
    c_send, c_recv, d_send, d_recv, x_send, x_recv, y_send, y_recv, z_send, z_recv = sems
    z, y, x, c = position()

    def push(src, dst, send, recv, target):
        return pltpu.make_async_remote_copy(
            src_ref=src,
            dst_ref=dst,
            send_sem=send,
            recv_sem=recv,
            device_id=target,
            device_id_type=MESH_ID,
        )

    f32 = jnp.float32

    def add(dst, *srcs):
        total = dst[...].astype(f32)
        for src in srcs:
            total = total + src[...].astype(f32)
        dst[...] = total.astype(dst.dtype)

    def core_copy(g, zz):
        return push(
            away_at(g, zz),
            from_core[g].at[zz],
            c_send.at[g, zz],
            c_recv.at[g, zz],
            device(z, y, x, 1 - c),
        )

    def diag_x(g, zz):
        return push(
            own_at(g, zz, 1 - y, 1 - x).at[:, columns(shapes[g], 0)],
            from_dx[g].at[zz],
            d_send.at[g, zz, 0],
            d_recv.at[g, zz, 0],
            device(z, y, 1 - x, c),
        )

    def diag_y(g, zz, full):
        part = slice(None) if full else columns(shapes[g], 1)
        return push(
            own_at(g, zz, 1 - y, 1 - x).at[:, part],
            from_dy[g].at[zz, :, part],
            d_send.at[g, zz, 1],
            d_recv.at[g, zz, 1],
            device(z, 1 - y, x, c),
        )

    def x_copy(g, zz):
        return push(
            own_at(g, zz, y, 1 - x),
            from_x[g].at[zz],
            x_send.at[g, zz],
            x_recv.at[g, zz],
            device(z, y, 1 - x, c),
        )

    def y_copy(g, zz):
        return push(
            own_at(g, zz, 1 - y, x),
            from_y[g].at[zz],
            y_send.at[g, zz],
            y_recv.at[g, zz],
            device(z, 1 - y, x, c),
        )

    def z_copy(g, zz, up):
        slot = zz if up else jnp.where(zz == z - 1, planes, zz)
        return push(
            own_at(g, zz, y, x),
            from_z[g].at[slot],
            z_send.at[g, zz],
            z_recv.at[g, slot],
            device(z + 1 if up else z - 1, y, x, c),
        )

    def z_arrival(g, slot):
        return push(
            from_z[g].at[slot],
            from_z[g].at[slot],
            z_send.at[g, 0],
            z_recv.at[g, slot],
            device(z, y, x, 1 - c),
        )

    def lean_or_even(t, lean, even):
        if not routed:
            even()
            return
        is_lean = (x == 1) & (t < planes - 1)
        pl.when(jnp.logical_not(is_lean))(even)
        pl.when(is_lean)(lean)

    def stage_core(g, t):
        zz = visit(t, z, planes)
        before_core(g, zz)
        core_copy(g, zz).wait_recv()
        add(own_at(g, zz, 1 - y, 1 - x), from_core[g].at[zz, 1 - y, 1 - x])

        def even():
            diag_x(g, zz).start()
            diag_y(g, zz, False).start()

        lean_or_even(t, lambda: diag_y(g, zz, True).start(), even)
        add(own_at(g, zz, 1 - y, x), from_core[g].at[zz, 1 - y, x])
        if routed:

            @pl.when((x == 0) & (t < planes - 1))
            def _():
                y_copy(g, zz).start()

        add(own_at(g, zz, y, 1 - x), from_core[g].at[zz, y, 1 - x])
        add(own_at(g, zz, y, x), from_core[g].at[zz, y, x])

    def stage_plane(g, t):
        zz = visit(t, z, planes)

        def take_x():
            diag_x(g, zz).wait_recv()
            add(own_at(g, zz, 1 - y, x).at[:, columns(shapes[g], 0)], from_dx[g].at[zz])
            y_copy(g, zz).start()

        def take_y(full):
            part = slice(None) if full else columns(shapes[g], 1)
            diag_y(g, zz, full).wait_recv()
            add(own_at(g, zz, y, 1 - x).at[:, part], from_dy[g].at[zz, :, part])
            x_copy(g, zz).start()

        if not routed:
            take_x()
            take_y(False)
            return
        lean = t < planes - 1
        pl.when((x == 1) | jnp.logical_not(lean))(take_x)
        pl.when((x == 1) & lean)(lambda: take_y(True))
        pl.when((x == 0) | jnp.logical_not(lean))(lambda: take_y(False))

    def stage_line(g, t):
        zz = visit(t, z, planes)
        x_copy(g, zz).wait_recv()
        y_copy(g, zz).wait_recv()
        here = own_at(g, zz, y, x)

        @pl.when(t > 0)
        def _():
            add(here, from_x[g].at[zz], from_y[g].at[zz])
            farther = jnp.where(zz > z, z > 0, z < planes - 1)

            @pl.when(farther)
            def _():
                z_arrival(g, zz).wait_recv()
                add(here, from_z[g].at[zz])

            @pl.when(zz > z)
            def _():
                z_copy(g, zz, True).start()

            @pl.when(zz < z)
            def _():
                z_copy(g, zz, False).start()

        @pl.when(t == 0)
        def _():
            outs[g][...] = (
                here[...].astype(f32)
                + from_x[g][zz].astype(f32)
                + from_y[g][zz].astype(f32)
            )

            @pl.when(z > 0)
            def _():
                z_arrival(g, zz).wait_recv()
                outs[g][...] += from_z[g][zz].astype(f32)

            @pl.when(z < planes - 1)
            def _():
                z_arrival(g, planes).wait_recv()
                outs[g][...] += from_z[g][planes].astype(f32)

    def stage_end(g, t):
        zz = visit(t, z, planes)
        core_copy(g, zz).wait_send()

        def even():
            diag_x(g, zz).wait_send()
            diag_y(g, zz, False).wait_send()

        lean_or_even(t, lambda: diag_y(g, zz, True).wait_send(), even)
        x_copy(g, zz).wait_send()
        y_copy(g, zz).wait_send()

        @pl.when(t > 0)
        def _():
            z_copy(g, zz, True).wait_send()

    return Reduction(
        core_copy=core_copy, core=stage_core, plane=stage_plane, line=stage_line, end=stage_end
    )


def remote(src, dst, send, recv, target):
    return pltpu.make_async_remote_copy(
        src_ref=src,
        dst_ref=dst,
        send_sem=send,
        recv_sem=recv,
        device_id=target,
        device_id_type=MESH_ID,
    )


def scatter_kernel(planes, shapes, *refs):
    n = len(shapes)
    parts, refs = refs[:n], refs[n:]
    starts, log_total, cos_table, sin_table, *sources = refs[:11]
    refs = refs[11:]
    outs, refs = refs[:n], refs[n:]
    query, *tiles, context, d_context = held = refs[-8:-1]
    source_sem, refs = refs[-1], refs[:-8]
    d_query, d_key, d_value, first_grad = refs[:4]
    refs = refs[4:]
    mine, near, chip, far, from_b, from_d, tile_send, tile_recv, bias, acc = refs[-10:]
    own, boxes, own_sem, sems = refs[:n], refs[n : 7 * n], refs[7 * n], refs[7 * n + 1 : -10]
    z, y, x, c = position()
    entry_barrier(z, y, x, c, planes)
    f32 = jnp.float32
    push = remote

    def add(dst, src):
        dst[...] = (dst[...].astype(f32) + src[...].astype(f32)).astype(dst.dtype)

    def load(g, zz):
        return pltpu.make_async_copy(
            parts[g].at[zz, :, :, c], own[g].at[zz], own_sem.at[g, zz]
        )

    steps = reduction(
        planes,
        shapes,
        True,
        lambda g, zz, yy, xx: own[g].at[zz, yy, xx],
        lambda g, zz: parts[g].at[zz, :, :, 1 - c],
        lambda g, zz: load(g, zz).wait(),
        boxes,
        sems,
        outs,
    )

    partner = device(z, y, x, 1 - c)
    seqs, rows = mine.shape[1:3]
    pairs = mine.shape[3] // 128

    def send_b(s):
        return push(
            near.at[:, s], from_b.at[:, s], tile_send.at[0, s], tile_recv.at[0, s], partner
        )

    def send_d(s):
        return push(
            far.at[:, s], from_d.at[:, s], tile_send.at[1, s], tile_recv.at[1, s], partner
        )

    def send_back(s):
        return push(
            chip.at[:, s],
            chip.at[:, s],
            tile_send.at[2, s],
            tile_recv.at[2, s],
            device(z, y, 1 - x, c),
        )

    def unit(s, p):
        lanes = pl.ds(pl.multiple_of(p * 128, 128), 128)
        flat = pl.ds(pl.multiple_of(s * rows, rows), rows)
        two = lambda ref: [ref.at[0, s, :, lanes], ref.at[1, s, :, lanes]]
        attend_back_step(
            lax.axis_index("ctx"),
            p == 0,
            starts.at[s],
            query[s, :, lanes],
            [two(t) for t in tiles],
            context[s, :, lanes],
            d_context[s, :, lanes],
            log_total.at[s, p],
            cos_table.at[flat],
            sin_table.at[flat],
            d_query.at[s, :, lanes],
            [two(t) for t in (mine, near, chip, far)],
            bias,
            acc,
        )

    def work(i):
        @pl.when((i >= 2) & (i <= 2 * seqs) & (lax.rem(i, 2) == 0) & (x == 1))
        def _():
            s = lax.div(i, 2) - 1
            send_d(s).wait_recv()

            @pl.loop(0, 2 * rows // 32)
            def _(j):
                kind = lax.div(j, rows // 32)
                at = pl.ds(pl.multiple_of(lax.rem(j, rows // 32) * 32, 32), 32)
                add(chip.at[kind, s, at], from_d.at[kind, s, at])

            send_back(s).start()

        @pl.when(i == 0)
        def _():
            for copy in sources:
                copy.wait()

        @pl.when((i >= 0) & (i < 2 * seqs))
        def _():
            s = lax.div(i, 2)

            @pl.loop(0, pairs // 2)
            def _(p):
                unit(s, lax.rem(i, 2) * (pairs // 2) + p)

            @pl.when(lax.rem(i, 2) == 1)
            def _():
                send_b(s).start()
                pl.when(x == 1)(lambda: send_d(s).start())

    def finish(s):
        send_b(s).wait_recv()
        pl.when(x == 0)(lambda: send_back(s).wait_recv())

        @pl.loop(0, rows // 32)
        def _(i):
            at = pl.ds(pl.multiple_of(i * 32, 32), 32)
            flat = pl.ds(pl.multiple_of(s * rows + i * 32, 32), 32)
            cos_rows, sin_rows = cos_table[flat, :], sin_table[flat, :]
            for k in range(pairs):
                lanes = pl.ds(k * 128, 128)

                def summed(kind):
                    return (
                        mine[kind, s, at, lanes].astype(f32)
                        + from_b[kind, s, at, lanes].astype(f32)
                        + jnp.where(x == 0, chip[kind, s, at, lanes].astype(f32), 0.0)
                    )

                d_key[flat, lanes] = turned(summed(0), cos_rows, sin_rows, -1.0).astype(jnp.bfloat16)
                half = 0.5 * summed(1)
                d_value[flat, lanes] = half.astype(jnp.bfloat16)
                first_grad[flat, lanes] = half

    @pl.loop(0, planes)
    def _(r):
        zz = visit(planes - 1 - r, z, planes)
        for g in range(n):
            steps.core_copy(g, zz).start()
            load(g, zz).start()

    sources = [
        pltpu.make_async_copy(src, dst, source_sem.at[i])
        for i, (src, dst) in enumerate(zip(sources, held))
    ]
    for copy in sources:
        copy.start()

    @pl.loop(0, planes + 2)
    def _(r):
        t = planes - 1 - r
        for g in range(n):
            pl.when(r < planes)(lambda: steps.core(g, t))
        for g in range(n):
            if g == 0:
                work(2 * r - 2)
            pl.when((r >= 1) & (r < planes + 1))(lambda: steps.plane(g, t + 1))
        work(2 * r - 1)
        for g in range(n):
            pl.when(r >= 2)(lambda: steps.line(g, t + 2))
        pl.when((r >= planes) & (r < planes + seqs))(lambda: finish(r - planes))

    @pl.loop(0, planes)
    def _(t):
        for g in range(n):
            steps.end(g, t)

    for s in range(2, seqs):
        finish(s)
    for s in range(seqs):
        send_b(s).wait_send()

        @pl.when(x == 1)
        def _():
            send_d(s).wait_send()
            send_back(s).wait_send()


def boxes_of(planes, shapes, types):
    def boxes(lead, narrow=False):
        out = []
        for s, d in zip(shapes, types):
            width = s[1] // 2 // 128 * 128 if narrow else s[1]
            out.append(pltpu.VMEM((*lead, s[0], width), d))
        return out

    return [
        *boxes((planes, 2, 2)),
        *boxes((planes,), True),
        *boxes((planes,)),
        *boxes((planes,)),
        *boxes((planes,)),
        *boxes((planes + 1,)),
    ]


def sems_of(planes, n):
    dma = pltpu.SemaphoreType.DMA
    return [
        dma((n, planes)),
        dma((n, planes)),
        dma((n, planes, 2)),
        dma((n, planes, 2)),
        dma((n, planes)),
        dma((n, planes)),
        dma((n, planes)),
        dma((n, planes)),
        dma((n, planes)),
        dma((n, planes + 1)),
    ]


def scatter_sum(planes, partials, attention):
    n = len(partials)
    partials = [
        p.reshape(planes, 2, 2, 2, p.shape[0] // (planes * 8), p.shape[1]) for p in partials
    ]
    shapes = [p.shape[4:] for p in partials]
    bf16 = jnp.bfloat16
    dma = pltpu.SemaphoreType.DMA
    attention, held = attention[:4], attention[4:]
    box = held[1].shape
    seqs, rows, width = box[1:]
    flat = (seqs * rows, width)
    vmem, anywhere = pl.BlockSpec(memory_space=pltpu.VMEM), pl.BlockSpec(memory_space=pl.ANY)
    return pl.pallas_call(
        functools.partial(scatter_kernel, planes, shapes),
        out_shape=[jax.ShapeDtypeStruct(s, jnp.float32) for s in shapes]
        + [
            jax.ShapeDtypeStruct(box[1:], bf16),
            jax.ShapeDtypeStruct(flat, bf16),
            jax.ShapeDtypeStruct(flat, bf16),
            jax.ShapeDtypeStruct(flat, jnp.float32),
        ],
        in_specs=[anywhere] * n + [vmem] * len(attention) + [anywhere] * len(held),
        out_specs=[vmem] * (n + 4),
        scratch_shapes=[
            *[pltpu.VMEM((planes, 2, 2, *s), bf16) for s in shapes],
            *boxes_of(planes, shapes, [bf16] * n),
            dma((n, planes)),
            *sems_of(planes, n),
            *[pltpu.VMEM(box, bf16)] * 6,
            dma((3, seqs)),
            dma((3, seqs)),
            *attend_back_scratch(rows),
            *[pltpu.VMEM(h.shape, h.dtype) for h in held],
            dma((len(held),)),
        ],
        compiler_params=pltpu.CompilerParams(
            collective_id=1, has_side_effects=True, vmem_limit_bytes=67043328
        ),
        name="gradient_scatter",
    )(*partials, *attention, *held)


def last_kernel(planes, shapes, *refs):
    f32, bf16 = jnp.float32, jnp.bfloat16
    n = len(shapes)
    normed, *d_proj = refs[:4]
    w_in, tok_in, d_residual_in, attn_gain, d_ffn_gain = refs[4:7], *refs[7:11]
    outs, token_grad = refs[11 : 11 + n], refs[11 + n]
    refs = refs[12 + n :]
    weights, tok, d_residual, gain_sum = refs[:3], *refs[3:6]
    parts, boxes, sems, load_sem = refs[6 : 6 + n], refs[6 + n : 6 + 7 * n], refs[6 + 7 * n : -1], refs[-1]
    z, y, x, c = position()
    loads = [
        pltpu.make_async_copy(src, dst, load_sem.at[i])
        for i, (src, dst) in enumerate(zip([*w_in, tok_in, d_residual_in], [*weights, tok, d_residual]))
    ]
    for copy in loads:
        copy.start()
    entry_barrier(z, y, x, c, planes)
    rows, width = tok.shape
    steps = reduction(
        planes,
        shapes,
        False,
        lambda g, zz, yy, xx: parts[g].at[zz, yy, xx, c],
        lambda g, zz: parts[g].at[zz, :, :, 1 - c],
        lambda g, zz: None,
        boxes,
        sems,
        outs,
    )
    at_once = planes * 256 // width

    def weight_grads(j):
        lanes = pl.ds(pl.multiple_of(j * 256, 256), 256)
        block = normed[:, lanes].T
        for g in range(3):
            part = jnp.dot(block, d_proj[g][...], preferred_element_type=f32)
            shape = (at_once, 2, 2, 2, *shapes[g])
            parts[g][pl.ds(j * at_once, at_once)] = part.reshape(shape).astype(bf16)

    each = max(width // 256 // planes, 1)

    def normed_grad(r):
        @pl.when(r == 0)
        def _():
            for copy in loads:
                copy.wait()

        @pl.loop(r * each, r * each + each)
        def _(j):
            at = pl.ds(pl.multiple_of(j * 256, 256), 256)
            total = 0.0
            for g in range(3):
                total = total + lax.dot_general(
                    d_proj[g][...], weights[g][at, :], NT, preferred_element_type=f32
                )
            token_grad[:, at] = total

    def token_gradient():
        gain_sum[...] = jnp.zeros_like(gain_sum)

        @pl.loop(0, rows // 64)
        def _(i):
            at = pl.ds(pl.multiple_of(i * 64, 64), 64)
            values = tok[at, :].astype(f32)
            scale = inverse_rms(values)
            d_normed = token_grad[at, :]
            products = d_normed * values * scale
            gain_sum[...] += jnp.sum(products.reshape(8, 8, width), axis=0)
            weighted = d_normed * attn_gain[...]
            token_grad[at, :] = (
                d_residual[at, :]
                + scale * weighted
                - values * (scale * scale * scale) * jnp.mean(weighted * values, axis=-1, keepdims=True)
            )

        both = jnp.concatenate(
            [jnp.sum(gain_sum[...], axis=0, keepdims=True), d_ffn_gain[...], jnp.zeros((6, width), f32)]
        )
        per = planes * 8 * 256 // width
        for i in range(planes * 8):
            at = i // per * 256
            parts[3][i // 8, i // 4 % 2, i // 2 % 2, i % 2] = both[:, at : at + 256]

    def send_cores(g, t):
        steps.core_copy(g, visit(t, z, planes)).start()

    if at_once > 1:
        pl.loop(0, width // 256)(weight_grads)
    @pl.loop(0, planes + 4)
    def _(r):
        t = planes - 1 - r

        @pl.when(r < planes)
        def _():
            if at_once == 1:
                weight_grads(visit(t, z, planes))
            for g in range(3):
                send_cores(g, t)

        for behind, step in ((1, steps.core), (2, steps.plane), (3, steps.line)):
            for g in range(3):
                pl.when((r >= behind) & (r < planes + behind))(lambda: step(g, t + behind))

            @pl.when(r == planes + behind)
            def _():
                @pl.loop(0, planes)
                def _(i):
                    step(3, planes - 1 - i)

        @pl.when(r < width // 256 // each)
        def _():
            normed_grad(r)

        @pl.when(r == planes)
        def _():
            token_gradient()

            @pl.loop(0, planes)
            def _(i):
                send_cores(3, i)

    @pl.loop(0, planes)
    def _(t):
        for g in range(n):
            steps.end(g, t)


def last(planes, normed, d_proj, weights, tok, d_residual, attn_gain, d_ffn_gain):
    f32, bf16 = jnp.float32, jnp.bfloat16
    width = tok.shape[1]
    shapes = [(width // (planes * 8), width)] * 3 + [(8, 256)]
    types = [bf16] * 3 + [f32]
    n = len(shapes)
    vmem, anywhere = pl.BlockSpec(memory_space=pltpu.VMEM), pl.BlockSpec(memory_space=pl.ANY)
    return pl.pallas_call(
        functools.partial(last_kernel, planes, shapes),
        out_shape=[jax.ShapeDtypeStruct(s, f32) for s in [*shapes, tok.shape]],
        in_specs=[vmem] * 4 + [anywhere] * 5 + [vmem] * 2,
        out_specs=[vmem] * (n + 1),
        scratch_shapes=[
            *[pltpu.VMEM((width, width), bf16)] * 3,
            pltpu.VMEM(tok.shape, bf16),
            pltpu.VMEM(tok.shape, f32),
            pltpu.VMEM((8, width), f32),
            *[pltpu.VMEM((planes, 2, 2, 2, *s), d) for s, d in zip(shapes, types)],
            *boxes_of(planes, shapes, types),
            *sems_of(planes, n),
            pltpu.SemaphoreType.DMA((5,)),
        ],
        compiler_params=pltpu.CompilerParams(
            collective_id=2, has_side_effects=True, vmem_limit_bytes=67043328
        ),
        name="last",
    )(normed, *d_proj, *weights, tok, d_residual, attn_gain, d_ffn_gain)


def deliver(arrays):
    n = len(arrays)

    def kernel(*refs):
        for src, dst in zip(refs[:n], refs[n:]):
            dst[...] = src[...]

    specs = [pl.BlockSpec((a.shape[0], a.shape[1] // 2), lambda i: (0, i)) for a in arrays]
    return pl.pallas_call(
        kernel,
        grid=(2,),
        in_specs=specs,
        out_specs=specs,
        out_shape=[jax.ShapeDtypeStruct(a.shape, a.dtype) for a in arrays],
        name="deliver",
    )(*arrays)


def on_device(
    planes,
    tokens,
    first_values,
    cotangent,
    segment_ids,
    attn_gain,
    w_query,
    w_key,
    w_value,
    w_out,
    ffn_gain,
    gate_weight,
    up_weight,
    down_weight,
):
    f32, bf16 = jnp.float32, jnp.bfloat16
    seqs, rows, width = tokens.shape
    rank = lax.axis_index("ctx")
    share = attn_gain.shape[0]
    per = 128 // share
    index = lax.axis_index("dp") * lax.axis_size("ctx") + rank
    place = lax.rem(index, per)
    lane = jnp.arange(128, dtype=jnp.int32)[None, :] - place * share
    here = lane == jnp.arange(share, dtype=jnp.int32)[:, None]
    spread = lambda gain: jnp.sum(jnp.where(here, gain.astype(f32)[:, None], 0.0), axis=0)
    kind = jnp.arange(16, dtype=jnp.int32)[:, None]
    gains = jnp.where(kind == 0, spread(attn_gain), jnp.where(kind == 1, spread(ffn_gain), 0.0))
    gains = gains.astype(bf16)
    starts, cos_table, sin_table = tables(segment_ids, rank, rows)
    flat = (seqs * rows, width)
    local = (seqs, rows, width)
    tokens = tokens.reshape(flat)
    mm = functools.partial(jnp.dot, preferred_element_type=f32)
    by_rows = lambda a, b: lax.dot_general(a, b, TN, preferred_element_type=f32).astype(bf16)
    back = lambda a, b: lax.dot_general(a, b, NT, preferred_element_type=f32)
    (_, w_query, w_key, w_value, w_out, gate_weight, up_weight, down_weight), (
        normed_one,
        query_rot,
        *tiles,
        context3,
        log_total,
        attn_gain,
        ffn_gain,
    ) = forward(
        planes,
        4,
        [gains, w_query, w_key, w_value, w_out, gate_weight, up_weight, down_weight],
        tokens,
        first_values.reshape(flat),
        starts,
        cos_table,
        sin_table,
    )
    context = context3.reshape(flat)
    tokens_float = tokens.astype(f32)
    cotangent = cotangent.reshape(flat)
    residual = tokens_float + mm(context, w_out)
    scale_two = inverse_rms(residual)
    second_normed = (residual * scale_two * ffn_gain).astype(bf16)
    gate = mm(second_normed, gate_weight)
    up = mm(second_normed, up_weight)
    hidden = (swish(gate) * up).astype(bf16)
    output = (residual + mm(hidden, down_weight)).astype(bf16)

    out_float = cotangent.astype(f32)
    d_down = by_rows(hidden, cotangent)
    d_hidden = back(cotangent, down_weight)
    sigmoid_gate = jax.nn.sigmoid(gate)
    d_gate = (d_hidden * up * sigmoid_gate * (1.0 + gate * (1.0 - sigmoid_gate))).astype(bf16)
    d_up = (d_hidden * (gate * sigmoid_gate)).astype(bf16)
    d_gate_weight = by_rows(second_normed, d_gate)
    d_up_weight = by_rows(second_normed, d_up)
    d_normed_two = back(d_gate, gate_weight) + back(d_up, up_weight)
    d_ffn_gain = jnp.sum(d_normed_two * residual * scale_two, axis=0)
    weighted_two = d_normed_two * ffn_gain
    d_residual = (
        out_float
        + scale_two * weighted_two
        - residual
        * (scale_two * scale_two * scale_two)
        * jnp.mean(weighted_two * residual, axis=-1, keepdims=True)
    )
    d_residual_low = d_residual.astype(bf16)
    d_out = by_rows(context, d_residual_low)
    d_context = back(d_residual_low, w_out).astype(bf16).reshape(local)
    s_down, s_gate, s_up, s_out, d_query, d_key, d_value, first_grad = scatter_sum(
        planes,
        [d_down, d_gate_weight, d_up_weight, d_out],
        [starts, log_total, cos_table, sin_table, query_rot, *tiles, context3, d_context],
    )
    d_query = d_query.reshape(flat)
    s_wq, s_wk, s_wv, s_gains, token_grad = last(
        planes,
        normed_one,
        [d_query, d_key, d_value],
        [w_query, w_key, w_value],
        tokens,
        d_residual,
        attn_gain,
        d_ffn_gain[None],
    )
    token_grad, first_grad, s_wq, s_wk, s_wv, s_out, s_gate, s_up, s_down = deliver(
        [token_grad, first_grad, s_wq, s_wk, s_wv, s_out, s_gate, s_up, s_down]
    )
    slot = lax.rem(index, 256 // share) * share
    s_gains = lax.dynamic_slice_in_dim(s_gains[:2], slot, share, 1)
    return (
        output.reshape(local),
        token_grad.reshape(local),
        first_grad.reshape(local),
        s_gains[0],
        s_wq,
        s_wk,
        s_wv,
        s_out,
        s_gains[1],
        s_gate,
        s_up,
        s_down,
    )


def solution(mesh):
    token, weight, vector = P("dp", "ctx", None), P(("dp", "ctx"), None), P(("dp", "ctx"))
    return jax.shard_map(
        functools.partial(on_device, mesh.shape["dp"] // 2),
        mesh=mesh,
        in_specs=(
            token,
            token,
            token,
            P("dp", None),
            vector,
            weight,
            weight,
            weight,
            weight,
            vector,
            weight,
            weight,
            weight,
        ),
        out_specs=(
            token,
            token,
            token,
            vector,
            weight,
            weight,
            weight,
            weight,
            vector,
            weight,
            weight,
            weight,
        ),
        check_vma=False,
    )
```
